8 devices in a mesh: data: 2 (over z, y), tp: 4 (over x, core).
Axes of the slice: x: 2, y: 2, z: 1, core: 2. Of those that a mesh axis runs over, the one named last changes fastest.
Arguments:
- attn_out: bfloat16 [512, 8192], P('data', 'tp'), parts along dimension 0
- w_out: bfloat16 [8192, 8192], P('tp')
- residual: bfloat16 [512, 8192], P('data', 'tp'), parts along dimension 0
- norm_gain: float32 [8192], P('tp')
Outputs:
- output 1: bfloat16 [512, 8192], P('data', 'tp'), parts along dimension 0
- output 2: bfloat16 [512, 8192], P('data', 'tp'), parts along dimension 0
There are 2 independent parts. The reference program is written for one: setup_inputs(seed, part) draws one part's arguments, and reference() takes and returns one part's arrays. A program takes and returns all parts, laid end to end along the dimension named above; an argument that names none is the same for every part.
All inputs are finite; a program needn't handle non-finite values.
Results may differ from the reference program's by a relative error of at most 0.00645153.
Values are sent between devices in bfloat16 or wider.
A program may use at most 1 GiB of HBM per device.

```python
import jax
import jax.numpy as jnp
from jax import lax

D_MODEL = 8192
N_HEADS = 64
HEAD_DIM = 128
TOKENS = 256
EPS = 1e-5


def setup_inputs(seed: int = 0, part: int = 0) -> dict:
    proj_width = N_HEADS * HEAD_DIM
    part_key = jax.random.fold_in(jax.random.key(seed), part)
    key_attn, key_resid = jax.random.split(part_key, 2)
    key_weight, key_gain = jax.random.split(jax.random.key(seed + 1), 2)
    attn_out = jax.random.normal(key_attn, (TOKENS, proj_width), jnp.float32).astype(jnp.bfloat16)
    weight_vals = jax.random.normal(key_weight, (proj_width, D_MODEL), jnp.float32) * proj_width ** -0.5
    w_out = weight_vals.astype(jnp.bfloat16)
    residual = jax.random.normal(key_resid, (TOKENS, D_MODEL), jnp.float32).astype(jnp.bfloat16)
    norm_gain = jax.random.uniform(key_gain, (D_MODEL,), jnp.float32, 0.5, 1.5)
    return {"attn_out": attn_out, "w_out": w_out, "residual": residual, "norm_gain": norm_gain}


def reference(attn_out, w_out, residual, norm_gain):
    projected = jnp.dot(attn_out, w_out, preferred_element_type=jnp.float32)
    hidden = residual.astype(jnp.float32) + projected
    mean_sq = jnp.mean(hidden * hidden, axis=-1, keepdims=True)
    normed = hidden * lax.rsqrt(mean_sq + EPS) * norm_gain
    return (hidden.astype(jnp.bfloat16), normed.astype(jnp.bfloat16))
```

```python
import functools

import jax
import jax.numpy as jnp
from jax import lax
from jax.experimental import pallas as pl
from jax.experimental.pallas import tpu as pltpu
from jax.sharding import PartitionSpec as P

EPS = 1e-5
MESH = pl.DeviceIdType.MESH
F32, BF16 = jnp.float32, jnp.bfloat16

CW = 256
N_COL = 2
BIG, SMALL = 32, 16


def kernel(d_model, a_hbm, w_hbm, r_hbm, g_hbm, hid_hbm, nrm_hbm,
           a_v, w_v, r_v, g_v, part, recv, own, hid, nrm, st_tx, st_rx,
           a_sem, w_sem, r_sem, g_sem, col_tx, col_rx, row_tx, row_rx, sib_tx, sib_rx, stat_tx, stat_rx, out_sem):
    t = lax.axis_index("tp")
    rows, _ = a_v.shape
    d_loc = own.shape[1]
    per = d_loc // CW
    peers = ((t + 2) % 4, 3 - t, t + 1 - 2 * (t % 2))
    n_big = (rows - 2 * SMALL) // BIG
    blocks = [(n_big * BIG, SMALL), (n_big * BIG + SMALL, SMALL)]
    n_blk = n_big + 2
    c0 = N_COL * CW

    def w_copy(slot, col):
        return pltpu.make_async_copy(w_hbm.at[:, pl.ds(pl.multiple_of(col, CW), CW)], w_v.at[slot], w_sem.at[slot])

    def cross_col(i):
        k = i % 2
        return (peers[0] + (peers[1] - peers[0]) * k) * d_loc + (i // 2) * CW

    def near_col(i):
        return (peers[2] + (t - peers[2]) * (i // per)) * d_loc + (i % per) * CW

    def remote(src, dst, tx, rx, peer):
        return pltpu.make_async_remote_copy(src_ref=src, dst_ref=dst, send_sem=tx, recv_sem=rx,
                                            device_id={"tp": peer}, device_id_type=MESH)

    def col_copy(k, j):
        cols = pl.ds(j * CW, CW)
        return remote(part.at[k, :, cols], recv.at[k, :, cols], col_tx.at[k, j], col_rx.at[k, j], peers[k])

    def row_copy(k, b, row, n):
        sl = (k, pl.ds(row, n), pl.ds(c0, d_loc - c0))
        return remote(part.at[sl], recv.at[sl], row_tx.at[k, b], row_rx.at[k, b], peers[k])

    def sib_copy():
        return remote(part.at[2], recv.at[2], sib_tx, sib_rx, peers[2])

    def stat_copy(k, b):
        return remote(st_tx.at[b], st_rx.at[k, b], stat_tx.at[k, b], stat_rx.at[k, b], peers[k])

    a_copy = pltpu.make_async_copy(a_hbm, a_v, a_sem)
    r_copy = pltpu.make_async_copy(r_hbm, r_v, r_sem)
    g_copy = pltpu.make_async_copy(g_hbm, g_v, g_sem)
    a_copy.start()
    w_copy(0, cross_col(0)).start()
    w_copy(1, cross_col(1)).start()
    barrier = pltpu.get_barrier_semaphore()
    for p in peers:
        pl.semaphore_signal(barrier, inc=1, device_id={"tp": p}, device_id_type=MESH)
    for i in range(2, 2 * per):
        w_copy(i, cross_col(i)).start()
    pl.semaphore_wait(barrier, 3)
    a_copy.wait()

    def chunk(slot, col):
        w_copy(slot, col).wait()
        return jnp.dot(a_v[...], w_v[slot], preferred_element_type=F32)

    def cross(i, by_col):
        k, j = i % 2, i // 2
        part[k, :, pl.ds(pl.multiple_of(j * CW, CW), CW)] = chunk(i, cross_col(i)).astype(BF16)
        w_copy(2 * per + i, near_col(i)).start()

    for i in range(2 * N_COL):
        cross(i, True)
        col_copy(i % 2, i // 2).start()

    @pl.loop(2 * N_COL, 2 * per)
    def _(i):
        cross(i, False)

    @pl.loop(0, n_big)
    def _(b):
        row = pl.multiple_of(b * BIG, BIG)
        row_copy(0, b, row, BIG).start()
        row_copy(1, b, row, BIG).start()

    for q, (row, n) in enumerate(blocks):
        row_copy(0, n_big + q, row, n).start()
        row_copy(1, n_big + q, row, n).start()
    r_copy.start()
    g_copy.start()

    @pl.loop(0, per)
    def _(j):
        part[2, :, pl.ds(pl.multiple_of(j * CW, CW), CW)] = chunk(2 * per + j, near_col(j)).astype(BF16)

    sib_copy().start()

    @pl.loop(0, per)
    def _(j):
        own[:, pl.ds(pl.multiple_of(j * CW, CW), CW)] = chunk(3 * per + j, near_col(per + j))

    r_copy.wait()
    g_copy.wait()
    sib_copy().wait_recv()
    for j in range(N_COL):
        for k in range(2):
            col_copy(k, j).wait_recv()

    lane = lax.broadcasted_iota(jnp.int32, (8, 128), 1)
    sub = lax.broadcasted_iota(jnp.int32, (8, 128), 0)

    def reduce_block(b, row, n):
        row_copy(0, b, row, n).wait_recv()
        row_copy(1, b, row, n).wait_recv()
        sl = pl.ds(row, n)
        h = own[sl, :] + recv[0, sl, :].astype(F32) + recv[1, sl, :].astype(F32) + recv[2, sl, :].astype(F32)
        h = r_v[sl, :].astype(F32) + h
        own[sl, :] = h
        hid[sl, :] = h.astype(BF16)
        s = jnp.sum(h * h, axis=1, keepdims=True)
        line = jnp.zeros((8, 128), F32)
        for q in range(n // 8):
            line = line + jnp.where(lane == sub + 8 * q, s[8 * q:8 * q + 8, :], 0.0)
        st_tx[b] = jnp.sum(line, axis=0, keepdims=True)
        for k in range(3):
            stat_copy(k, b).start()
        pltpu.make_async_copy(hid.at[sl, :], hid_hbm.at[sl, :], out_sem.at[0, b]).start()

    def norm_block(b, row, n):
        for k in range(3):
            stat_copy(k, b).wait_recv()
        tot = (st_tx[b] + st_rx[2, b]) + (st_rx[0, b] + st_rx[1, b])
        scale = lax.rsqrt(tot / d_model + EPS)
        scale = jnp.broadcast_to(scale, (8, 128))
        for q in range(n // 8):
            sl = pl.ds(row + 8 * q, 8)
            col = jnp.sum(jnp.where(lane == sub + 8 * q, scale, 0.0), axis=1, keepdims=True)
            own[sl, :] = own[sl, :] * col * g_v[...]
        sl = pl.ds(row, n)
        nrm[sl, :] = own[sl, :].astype(BF16)
        pltpu.make_async_copy(nrm.at[sl, :], nrm_hbm.at[sl, :], out_sem.at[1, b]).start()

    reduce_block(0, 0, BIG)

    @pl.loop(1, n_big)
    def _(b):
        row = pl.multiple_of(b * BIG, BIG)
        reduce_block(b, row, BIG)
        norm_block(b - 1, pl.multiple_of(row - BIG, BIG), BIG)

    (row_s, n_s), (row_l, n_l) = blocks
    reduce_block(n_big, row_s, n_s)
    norm_block(n_big - 1, row_s - BIG, BIG)
    reduce_block(n_big + 1, row_l, n_l)
    norm_block(n_big, row_s, n_s)
    norm_block(n_big + 1, row_l, n_l)

    for j in range(N_COL):
        for k in range(2):
            col_copy(k, j).wait_send()
    sib_copy().wait_send()

    def drain(b, row, n):
        sl = pl.ds(row, n)
        row_copy(0, b, row, n).wait_send()
        row_copy(1, b, row, n).wait_send()
        for k in range(3):
            stat_copy(k, b).wait_send()
        pltpu.make_async_copy(hid.at[sl, :], hid_hbm.at[sl, :], out_sem.at[0, b]).wait()
        pltpu.make_async_copy(nrm.at[sl, :], nrm_hbm.at[sl, :], out_sem.at[1, b]).wait()

    @pl.loop(0, n_big)
    def _(b):
        drain(b, pl.multiple_of(b * BIG, BIG), BIG)

    drain(n_big, row_s, n_s)
    drain(n_big + 1, row_l, n_l)


def solution(mesh):
    tp = mesh.shape["tp"]

    def local_step(a, w, r, g):
        rows, depth = a.shape
        d_loc = r.shape[1]
        per = d_loc // CW
        n_blk = (rows - 2 * SMALL) // BIG + 2
        any_spec = pl.BlockSpec(memory_space=pl.ANY)
        dma = pltpu.SemaphoreType.DMA
        return pl.pallas_call(
            functools.partial(kernel, d_loc * tp),
            out_shape=(jax.ShapeDtypeStruct((rows, d_loc), BF16),) * 2,
            in_specs=[any_spec] * 4,
            out_specs=(any_spec,) * 2,
            scratch_shapes=[
                pltpu.VMEM((rows, depth), BF16),
                pltpu.VMEM((4 * per, depth, CW), BF16),
                pltpu.VMEM((rows, d_loc), BF16),
                pltpu.VMEM((1, d_loc), F32),
                pltpu.VMEM((3, rows, d_loc), BF16),
                pltpu.VMEM((3, rows, d_loc), BF16),
                pltpu.VMEM((rows, d_loc), F32),
                pltpu.VMEM((rows, d_loc), BF16),
                pltpu.VMEM((rows, d_loc), BF16),
                pltpu.VMEM((n_blk, 1, 128), F32),
                pltpu.VMEM((3, n_blk, 1, 128), F32),
                dma, dma((4 * per,)), dma, dma,
                dma((2, N_COL)), dma((2, N_COL)), dma((2, n_blk)), dma((2, n_blk)), dma, dma,
                dma((3, n_blk)), dma((3, n_blk)), dma((2, n_blk)),
            ],
            compiler_params=pltpu.CompilerParams(
                collective_id=0, has_side_effects=True, vmem_limit_bytes=56 * 1024 * 1024),
            cost_estimate=pl.CostEstimate(flops=2 * rows * depth * d_loc * tp, transcendentals=0,
                                          bytes_accessed=2 * depth * d_loc * tp),
        )(a, w, r, g.reshape(1, d_loc))

    return jax.shard_map(
        local_step,
        mesh=mesh,
        in_specs=(P("data", "tp"), P("tp", None), P("data", "tp"), P("tp")),
        out_specs=(P("data", "tp"), P("data", "tp")),
        check_vma=False,
    )
```

```python
import functools

import jax
import jax.numpy as jnp
from jax import lax
from jax.experimental import pallas as pl
from jax.experimental.pallas import tpu as pltpu
from jax.sharding import PartitionSpec as P

EPS = 1e-5
MESH = pl.DeviceIdType.MESH
F32, BF16 = jnp.float32, jnp.bfloat16

CW = 256
N_COL = 2
BIG, SMALL = 32, 16
AHEAD = 2


def kernel(d_model, a_hbm, w_hbm, r_hbm, g_hbm, hid_hbm, nrm_hbm,
           a_v, w_v, r_v, g_v, part, recv, own, hid, nrm, st_tx, st_rx,
           a_sem, w_sem, r_sem, g_sem, col_tx, col_rx, row_tx, row_rx, sib_tx, sib_rx, stat_tx, stat_rx, out_sem):
    t = lax.axis_index("tp")
    rows, _ = a_v.shape
    d_loc = own.shape[1]
    per = d_loc // CW
    peers = ((t + 2) % 4, 3 - t, t + 1 - 2 * (t % 2))
    n_big = (rows - 2 * SMALL) // BIG
    blocks = [(n_big * BIG, SMALL), (n_big * BIG + SMALL, SMALL)]
    n_blk = n_big + 2
    c0 = N_COL * CW

    def w_copy(slot, col):
        return pltpu.make_async_copy(w_hbm.at[:, pl.ds(pl.multiple_of(col, CW), CW)], w_v.at[slot], w_sem.at[slot])

    def cross_col(i):
        k = i % 2
        return (peers[0] + (peers[1] - peers[0]) * k) * d_loc + (i // 2) * CW

    def near_col(i):
        return (peers[2] + (t - peers[2]) * (i // per)) * d_loc + (i % per) * CW

    def remote(src, dst, tx, rx, peer):
        return pltpu.make_async_remote_copy(src_ref=src, dst_ref=dst, send_sem=tx, recv_sem=rx,
                                            device_id={"tp": peer}, device_id_type=MESH)

    def col_copy(k, j):
        cols = pl.ds(j * CW, CW)
        return remote(part.at[k, :, cols], recv.at[k, :, cols], col_tx.at[k, j], col_rx.at[k, j], peers[k])

    def row_copy(k, b, row, n):
        sl = (k, pl.ds(row, n), pl.ds(c0, d_loc - c0))
        return remote(part.at[sl], recv.at[sl], row_tx.at[k, b], row_rx.at[k, b], peers[k])

    def sib_copy():
        return remote(part.at[2], recv.at[2], sib_tx, sib_rx, peers[2])

    def stat_copy(k, b):
        return remote(st_tx.at[b], st_rx.at[k, b], stat_tx.at[k, b], stat_rx.at[k, b], peers[k])

    a_copy = pltpu.make_async_copy(a_hbm, a_v, a_sem)
    r_copy = pltpu.make_async_copy(r_hbm, r_v, r_sem)
    g_copy = pltpu.make_async_copy(g_hbm, g_v, g_sem)
    a_copy.start()
    w_copy(0, cross_col(0)).start()
    w_copy(1, cross_col(1)).start()
    barrier = pltpu.get_barrier_semaphore()
    for p in peers:
        pl.semaphore_signal(barrier, inc=1, device_id={"tp": p}, device_id_type=MESH)
    for i in range(2, 2 * per):
        w_copy(i, cross_col(i)).start()
    pl.semaphore_wait(barrier, 3)
    a_copy.wait()

    def chunk(slot, col):
        w_copy(slot, col).wait()
        return jnp.dot(a_v[...], w_v[slot], preferred_element_type=F32)

    def cross(i, by_col):
        k, j = i % 2, i // 2
        part[k, :, pl.ds(pl.multiple_of(j * CW, CW), CW)] = chunk(i, cross_col(i)).astype(BF16)
        w_copy(2 * per + i, near_col(i)).start()

    for i in range(2 * N_COL):
        cross(i, True)
        col_copy(i % 2, i // 2).start()

    @pl.loop(2 * N_COL, 2 * per)
    def _(i):
        cross(i, False)

    def send_block(b, row, n):
        row_copy(0, b, row, n).start()
        row_copy(1, b, row, n).start()

    def sent_block(b, row, n):
        row_copy(0, b, row, n).wait_send()
        row_copy(1, b, row, n).wait_send()

    for b in range(AHEAD):
        send_block(b, b * BIG, BIG)
    r_copy.start()
    g_copy.start()

    @pl.loop(0, per)
    def _(j):
        part[2, :, pl.ds(pl.multiple_of(j * CW, CW), CW)] = chunk(2 * per + j, near_col(j)).astype(BF16)

    sib_copy().start()

    @pl.loop(0, per)
    def _(j):
        own[:, pl.ds(pl.multiple_of(j * CW, CW), CW)] = chunk(3 * per + j, near_col(per + j))

    r_copy.wait()
    g_copy.wait()
    sib_copy().wait_recv()
    for j in range(N_COL):
        for k in range(2):
            col_copy(k, j).wait_recv()

    lane = lax.broadcasted_iota(jnp.int32, (8, 128), 1)
    sub = lax.broadcasted_iota(jnp.int32, (8, 128), 0)

    def reduce_block(b, row, n):
        row_copy(0, b, row, n).wait_recv()
        row_copy(1, b, row, n).wait_recv()
        sl = pl.ds(row, n)
        h = own[sl, :] + recv[0, sl, :].astype(F32) + recv[1, sl, :].astype(F32) + recv[2, sl, :].astype(F32)
        h = r_v[sl, :].astype(F32) + h
        own[sl, :] = h
        hid[sl, :] = h.astype(BF16)
        s = jnp.sum(h * h, axis=1, keepdims=True)
        line = jnp.zeros((8, 128), F32)
        for q in range(n // 8):
            line = line + jnp.where(lane == sub + 8 * q, s[8 * q:8 * q + 8, :], 0.0)
        st_tx[b] = jnp.sum(line, axis=0, keepdims=True)
        for k in range(3):
            stat_copy(k, b).start()
        pltpu.make_async_copy(hid.at[sl, :], hid_hbm.at[sl, :], out_sem.at[0, b]).start()

    def norm_block(b, row, n):
        for k in range(3):
            stat_copy(k, b).wait_recv()
        tot = (st_tx[b] + st_rx[2, b]) + (st_rx[0, b] + st_rx[1, b])
        scale = lax.rsqrt(tot / d_model + EPS)
        scale = jnp.broadcast_to(scale, (8, 128))
        for q in range(n // 8):
            sl = pl.ds(row + 8 * q, 8)
            col = jnp.sum(jnp.where(lane == sub + 8 * q, scale, 0.0), axis=1, keepdims=True)
            own[sl, :] = own[sl, :] * col * g_v[...]
        sl = pl.ds(row, n)
        nrm[sl, :] = own[sl, :].astype(BF16)
        pltpu.make_async_copy(nrm.at[sl, :], nrm_hbm.at[sl, :], out_sem.at[1, b]).start()

    (row_s, n_s), (row_l, n_l) = blocks

    sent_block(0, 0, BIG)
    send_block(AHEAD, AHEAD * BIG, BIG)
    reduce_block(0, 0, BIG)

    @pl.loop(1, n_big - AHEAD)
    def _(b):
        row = pl.multiple_of(b * BIG, BIG)
        sent_block(b, row, BIG)
        send_block(b + AHEAD, pl.multiple_of(row + AHEAD * BIG, BIG), BIG)
        reduce_block(b, row, BIG)
        norm_block(b - 1, pl.multiple_of(row - BIG, BIG), BIG)

    for q in range(2):
        b = n_big - 2 + q
        sent_block(b, b * BIG, BIG)
        send_block(n_big + q, *blocks[q])
        reduce_block(b, b * BIG, BIG)
        norm_block(b - 1, b * BIG - BIG, BIG)

    reduce_block(n_big, row_s, n_s)
    norm_block(n_big - 1, row_s - BIG, BIG)
    reduce_block(n_big + 1, row_l, n_l)
    norm_block(n_big, row_s, n_s)
    norm_block(n_big + 1, row_l, n_l)
    sent_block(n_big, row_s, n_s)
    sent_block(n_big + 1, row_l, n_l)

    for j in range(N_COL):
        for k in range(2):
            col_copy(k, j).wait_send()
    sib_copy().wait_send()

    def drain(b, row, n):
        sl = pl.ds(row, n)
        for k in range(3):
            stat_copy(k, b).wait_send()
        pltpu.make_async_copy(hid.at[sl, :], hid_hbm.at[sl, :], out_sem.at[0, b]).wait()
        pltpu.make_async_copy(nrm.at[sl, :], nrm_hbm.at[sl, :], out_sem.at[1, b]).wait()

    @pl.loop(0, n_big)
    def _(b):
        drain(b, pl.multiple_of(b * BIG, BIG), BIG)

    drain(n_big, row_s, n_s)
    drain(n_big + 1, row_l, n_l)


def solution(mesh):
    tp = mesh.shape["tp"]

    def local_step(a, w, r, g):
        rows, depth = a.shape
        d_loc = r.shape[1]
        per = d_loc // CW
        n_blk = (rows - 2 * SMALL) // BIG + 2
        any_spec = pl.BlockSpec(memory_space=pl.ANY)
        dma = pltpu.SemaphoreType.DMA
        return pl.pallas_call(
            functools.partial(kernel, d_loc * tp),
            out_shape=(jax.ShapeDtypeStruct((rows, d_loc), BF16),) * 2,
            in_specs=[any_spec] * 4,
            out_specs=(any_spec,) * 2,
            scratch_shapes=[
                pltpu.VMEM((rows, depth), BF16),
                pltpu.VMEM((4 * per, depth, CW), BF16),
                pltpu.VMEM((rows, d_loc), BF16),
                pltpu.VMEM((1, d_loc), F32),
                pltpu.VMEM((3, rows, d_loc), BF16),
                pltpu.VMEM((3, rows, d_loc), BF16),
                pltpu.VMEM((rows, d_loc), F32),
                pltpu.VMEM((rows, d_loc), BF16),
                pltpu.VMEM((rows, d_loc), BF16),
                pltpu.VMEM((n_blk, 1, 128), F32),
                pltpu.VMEM((3, n_blk, 1, 128), F32),
                dma, dma((4 * per,)), dma, dma,
                dma((2, N_COL)), dma((2, N_COL)), dma((2, n_blk)), dma((2, n_blk)), dma, dma,
                dma((3, n_blk)), dma((3, n_blk)), dma((2, n_blk)),
            ],
            compiler_params=pltpu.CompilerParams(
                collective_id=0, has_side_effects=True, vmem_limit_bytes=56 * 1024 * 1024),
            cost_estimate=pl.CostEstimate(flops=2 * rows * depth * d_loc * tp, transcendentals=0,
                                          bytes_accessed=2 * depth * d_loc * tp),
        )(a, w, r, g.reshape(1, d_loc))

    return jax.shard_map(
        local_step,
        mesh=mesh,
        in_specs=(P("data", "tp"), P("tp", None), P("data", "tp"), P("tp")),
        out_specs=(P("data", "tp"), P("data", "tp")),
        check_vma=False,
    )
```

```python
import functools

import jax
import jax.numpy as jnp
from jax import lax
from jax.experimental import pallas as pl
from jax.experimental.pallas import tpu as pltpu
from jax.sharding import PartitionSpec as P

EPS = 1e-5
MESH = pl.DeviceIdType.MESH
F32, BF16 = jnp.float32, jnp.bfloat16

CW = 256
N_COL = 2
BIG, SMALL = 32, 16
AHEAD = 2


def kernel(d_model, a_hbm, w_hbm, r_hbm, g_hbm, hid, nrm,
           a_v, w_v, r_v, g_v, part, recv, own, st_tx, st_rx,
           a_sem, w_sem, r_sem, g_sem, col_tx, col_rx, row_tx, row_rx, sib_tx, sib_rx, stat_tx, stat_rx):
    t = lax.axis_index("tp")
    rows, _ = a_v.shape
    d_loc = own.shape[1]
    per = d_loc // CW
    peers = ((t + 2) % 4, 3 - t, t + 1 - 2 * (t % 2))
    n_big = (rows - 2 * SMALL) // BIG
    blocks = [(n_big * BIG, SMALL), (n_big * BIG + SMALL, SMALL)]
    n_blk = n_big + 2
    c0 = N_COL * CW

    def w_copy(slot, col):
        return pltpu.make_async_copy(w_hbm.at[:, pl.ds(pl.multiple_of(col, CW), CW)], w_v.at[slot], w_sem.at[slot])

    def cross_col(i):
        k = i % 2
        return (peers[0] + (peers[1] - peers[0]) * k) * d_loc + (i // 2) * CW

    def near_col(i):
        return (peers[2] + (t - peers[2]) * (i // per)) * d_loc + (i % per) * CW

    def remote(src, dst, tx, rx, peer):
        return pltpu.make_async_remote_copy(src_ref=src, dst_ref=dst, send_sem=tx, recv_sem=rx,
                                            device_id={"tp": peer}, device_id_type=MESH)

    def col_copy(k, j):
        cols = pl.ds(j * CW, CW)
        return remote(part.at[k, :, cols], recv.at[k, :, cols], col_tx.at[k, j], col_rx.at[k, j], peers[k])

    def row_copy(k, b, row, n):
        sl = (k, pl.ds(row, n), pl.ds(c0, d_loc - c0))
        return remote(part.at[sl], recv.at[sl], row_tx.at[k, b], row_rx.at[k, b], peers[k])

    def sib_copy():
        return remote(part.at[2], recv.at[2], sib_tx, sib_rx, peers[2])

    def stat_copy(k, b):
        return remote(st_tx.at[b], st_rx.at[k, b], stat_tx.at[k, b], stat_rx.at[k, b], peers[k])

    a_copy = pltpu.make_async_copy(a_hbm, a_v, a_sem)
    r_copy = pltpu.make_async_copy(r_hbm, r_v, r_sem)
    g_copy = pltpu.make_async_copy(g_hbm, g_v, g_sem)
    a_copy.start()
    w_copy(0, cross_col(0)).start()
    w_copy(1, cross_col(1)).start()
    barrier = pltpu.get_barrier_semaphore()
    for p in peers:
        pl.semaphore_signal(barrier, inc=1, device_id={"tp": p}, device_id_type=MESH)
    for i in range(2, 2 * per):
        w_copy(i, cross_col(i)).start()
    pl.semaphore_wait(barrier, 3)
    a_copy.wait()

    def chunk(slot, col):
        w_copy(slot, col).wait()
        return jnp.dot(a_v[...], w_v[slot], preferred_element_type=F32)

    def cross(i, by_col):
        k, j = i % 2, i // 2
        part[k, :, pl.ds(pl.multiple_of(j * CW, CW), CW)] = chunk(i, cross_col(i)).astype(BF16)
        w_copy(2 * per + i, near_col(i)).start()

    for i in range(2 * N_COL):
        cross(i, True)
        col_copy(i % 2, i // 2).start()

    @pl.loop(2 * N_COL, 2 * per)
    def _(i):
        cross(i, False)

    def send_block(b, row, n):
        row_copy(0, b, row, n).start()
        row_copy(1, b, row, n).start()

    def sent_block(b, row, n):
        row_copy(0, b, row, n).wait_send()
        row_copy(1, b, row, n).wait_send()

    for b in range(AHEAD):
        send_block(b, b * BIG, BIG)
    r_copy.start()
    g_copy.start()

    @pl.loop(0, per)
    def _(j):
        part[2, :, pl.ds(pl.multiple_of(j * CW, CW), CW)] = chunk(2 * per + j, near_col(j)).astype(BF16)

    sib_copy().start()

    @pl.loop(0, per)
    def _(j):
        own[:, pl.ds(pl.multiple_of(j * CW, CW), CW)] = chunk(3 * per + j, near_col(per + j))

    r_copy.wait()
    g_copy.wait()
    sib_copy().wait_recv()
    for j in range(N_COL):
        for k in range(2):
            col_copy(k, j).wait_recv()

    lane = lax.broadcasted_iota(jnp.int32, (8, 128), 1)
    sub = lax.broadcasted_iota(jnp.int32, (8, 128), 0)

    def reduce_block(b, row, n):
        row_copy(0, b, row, n).wait_recv()
        row_copy(1, b, row, n).wait_recv()
        sl = pl.ds(row, n)
        h = own[sl, :] + recv[0, sl, :].astype(F32) + recv[1, sl, :].astype(F32) + recv[2, sl, :].astype(F32)
        h = r_v[sl, :].astype(F32) + h
        own[sl, :] = h
        hid[sl, :] = h.astype(BF16)
        s = jnp.sum(h * h, axis=1, keepdims=True)
        line = jnp.zeros((8, 128), F32)
        for q in range(n // 8):
            line = line + jnp.where(lane == sub + 8 * q, s[8 * q:8 * q + 8, :], 0.0)
        st_tx[b] = jnp.sum(line, axis=0, keepdims=True)
        for k in range(3):
            stat_copy(k, b).start()

    def norm_block(b, row, n):
        for k in range(3):
            stat_copy(k, b).wait_recv()
        tot = (st_tx[b] + st_rx[2, b]) + (st_rx[0, b] + st_rx[1, b])
        scale = lax.rsqrt(tot / d_model + EPS)
        scale = jnp.broadcast_to(scale, (8, 128))
        for q in range(n // 8):
            sl = pl.ds(row + 8 * q, 8)
            col = jnp.sum(jnp.where(lane == sub + 8 * q, scale, 0.0), axis=1, keepdims=True)
            own[sl, :] = own[sl, :] * col * g_v[...]
        sl = pl.ds(row, n)
        nrm[sl, :] = own[sl, :].astype(BF16)

    (row_s, n_s), (row_l, n_l) = blocks

    sent_block(0, 0, BIG)
    send_block(AHEAD, AHEAD * BIG, BIG)
    reduce_block(0, 0, BIG)

    @pl.loop(1, n_big - AHEAD)
    def _(b):
        row = pl.multiple_of(b * BIG, BIG)
        sent_block(b, row, BIG)
        send_block(b + AHEAD, pl.multiple_of(row + AHEAD * BIG, BIG), BIG)
        reduce_block(b, row, BIG)
        norm_block(b - 1, pl.multiple_of(row - BIG, BIG), BIG)

    for q in range(2):
        b = n_big - 2 + q
        sent_block(b, b * BIG, BIG)
        send_block(n_big + q, *blocks[q])
        reduce_block(b, b * BIG, BIG)
        norm_block(b - 1, b * BIG - BIG, BIG)

    reduce_block(n_big, row_s, n_s)
    norm_block(n_big - 1, row_s - BIG, BIG)
    reduce_block(n_big + 1, row_l, n_l)
    norm_block(n_big, row_s, n_s)
    norm_block(n_big + 1, row_l, n_l)
    sent_block(n_big, row_s, n_s)
    sent_block(n_big + 1, row_l, n_l)

    for j in range(N_COL):
        for k in range(2):
            col_copy(k, j).wait_send()
    sib_copy().wait_send()

    @pl.loop(0, n_big + 2)
    def _(b):
        for k in range(3):
            stat_copy(k, b).wait_send()


def put(hid, nrm, hid_hbm, nrm_hbm, sem):
    copies = (pltpu.make_async_copy(hid, hid_hbm, sem.at[0]), pltpu.make_async_copy(nrm, nrm_hbm, sem.at[1]))
    for c in copies:
        c.start()
    for c in copies:
        c.wait()


def solution(mesh):
    tp = mesh.shape["tp"]

    def local_step(a, w, r, g):
        rows, depth = a.shape
        d_loc = r.shape[1]
        per = d_loc // CW
        n_blk = (rows - 2 * SMALL) // BIG + 2
        hbm = pl.BlockSpec(memory_space=pltpu.HBM)
        vmem = pl.BlockSpec(memory_space=pltpu.VMEM)
        dma = pltpu.SemaphoreType.DMA
        hid, nrm = pl.pallas_call(
            functools.partial(kernel, d_loc * tp),
            out_shape=(pltpu.VMEM((rows, d_loc), BF16),) * 2,
            in_specs=[hbm] * 4,
            out_specs=(vmem,) * 2,
            scratch_shapes=[
                pltpu.VMEM((rows, depth), BF16),
                pltpu.VMEM((4 * per, depth, CW), BF16),
                pltpu.VMEM((rows, d_loc), BF16),
                pltpu.VMEM((1, d_loc), F32),
                pltpu.VMEM((3, rows, d_loc), BF16),
                pltpu.VMEM((3, rows, d_loc), BF16),
                pltpu.VMEM((rows, d_loc), F32),
                pltpu.VMEM((n_blk, 1, 128), F32),
                pltpu.VMEM((3, n_blk, 1, 128), F32),
                dma, dma((4 * per,)), dma, dma,
                dma((2, N_COL)), dma((2, N_COL)), dma((2, n_blk)), dma((2, n_blk)), dma, dma,
                dma((3, n_blk)), dma((3, n_blk)),
            ],
            compiler_params=pltpu.CompilerParams(
                collective_id=0, has_side_effects=True, vmem_limit_bytes=64946176),
            cost_estimate=pl.CostEstimate(flops=2 * rows * depth * d_loc * tp, transcendentals=0,
                                          bytes_accessed=2 * depth * d_loc * tp),
        )(a, w, r, g.reshape(1, d_loc))
        return pl.pallas_call(
            put,
            out_shape=(jax.ShapeDtypeStruct((rows, d_loc), BF16),) * 2,
            in_specs=[vmem] * 2,
            out_specs=(hbm,) * 2,
            scratch_shapes=[dma((2,))],
            compiler_params=pltpu.CompilerParams(vmem_limit_bytes=1024 * 1024),
        )(hid, nrm)

    return jax.shard_map(
        local_step,
        mesh=mesh,
        in_specs=(P("data", "tp"), P("tp", None), P("data", "tp"), P("tp")),
        out_specs=(P("data", "tp"), P("data", "tp")),
        check_vma=False,
    )
```

```python
import functools

import jax
import jax.numpy as jnp
from jax import lax
from jax.experimental import pallas as pl
from jax.experimental.pallas import tpu as pltpu
from jax.sharding import PartitionSpec as P

EPS = 1e-5
MESH = pl.DeviceIdType.MESH
F32, BF16 = jnp.float32, jnp.bfloat16

CW = 256
N_COL = 2
BIG, SMALL = 32, 16
DEPTH = 4
PUT = 4
AHEAD = 2


def kernel(d_model, a_hbm, w_hbm, r_hbm, g_hbm, hid, nrm,
           a_v, w_v, r_v, g_v, part, recv, own, st_tx, st_rx,
           a_sem, w0_sem, w_sem, r_sem, g_sem, first_tx, first_rx, col_tx, col_rx, row_tx, row_rx, sib_tx, sib_rx, stat_tx, stat_rx):
    t = lax.axis_index("tp")
    rows, _ = a_v.shape
    d_loc = own.shape[1]
    per = d_loc // CW
    peers = ((t + 2) % 4, 3 - t, t + 1 - 2 * (t % 2))
    n_big = (rows - 2 * SMALL) // BIG
    blocks = [(n_big * BIG, SMALL), (n_big * BIG + SMALL, SMALL)]
    n_blk = n_big + 2
    c0 = N_COL * CW

    def w_copy(slot, col):
        return pltpu.make_async_copy(w_hbm.at[:, pl.ds(pl.multiple_of(col, CW), CW)], w_v.at[slot], w_sem.at[slot])

    def cross_col(i):
        k = i % 2
        return (peers[0] + (peers[1] - peers[0]) * k) * d_loc + (i // 2) * CW

    def near_col(i):
        return (peers[2] + (t - peers[2]) * (i // per)) * d_loc + (i % per) * CW

    def remote(src, dst, tx, rx, peer):
        return pltpu.make_async_remote_copy(src_ref=src, dst_ref=dst, send_sem=tx, recv_sem=rx,
                                            device_id={"tp": peer}, device_id_type=MESH)

    def col_copy(k, j):
        cols = pl.ds(j * CW, CW)
        return remote(part.at[k, :, cols], recv.at[k, :, cols], col_tx.at[k, j], col_rx.at[k, j], peers[k])

    def row_copy(k, b, row, n):
        sl = (k, pl.ds(row, n), pl.ds(c0, d_loc - c0))
        return remote(part.at[sl], recv.at[sl], row_tx.at[k, b], row_rx.at[k, b], peers[k])

    def sib_copy():
        return remote(part.at[2], recv.at[2], sib_tx, sib_rx, peers[2])

    def stat_copy(k, b):
        return remote(st_tx.at[b], st_rx.at[k, b], stat_tx.at[k, b], stat_rx.at[k, b], peers[k])

    half, lanes = rows // 2, 128

    def a_copy(q):
        sl = pl.ds(q * half, half)
        return pltpu.make_async_copy(a_hbm.at[sl, :], a_v.at[sl, :], a_sem.at[q])

    def w0_copy(q, first, n):
        src = w_hbm.at[:, pl.ds(pl.multiple_of(cross_col(0) + first, lanes), n)]
        return pltpu.make_async_copy(src, w_v.at[0, :, pl.ds(first, n)], w0_sem.at[q])

    def w_start(i):
        if isinstance(i, int):
            w_copy(i, cross_col(i) if i < 2 * per else near_col(i - 2 * per)).start()
            return

        @pl.when(i < 2 * per)
        def _():
            w_copy(i, cross_col(i)).start()

        @pl.when((i >= 2 * per) & (i < 4 * per))
        def _():
            w_copy(i, near_col(i - 2 * per)).start()

    r_copy = pltpu.make_async_copy(r_hbm, r_v, r_sem)
    g_copy = pltpu.make_async_copy(g_hbm, g_v, g_sem)
    a_copy(0).start()
    w0_copy(0, 0, lanes).start()
    a_copy(1).start()
    w0_copy(1, lanes, CW - lanes).start()
    barrier = pltpu.get_barrier_semaphore()
    for p in peers:
        pl.semaphore_signal(barrier, inc=1, device_id={"tp": p}, device_id_type=MESH)

    def dot(lhs, rhs):
        return jnp.dot(lhs, rhs, preferred_element_type=F32)

    pieces = ((pl.ds(0, half), pl.ds(0, lanes)), (pl.ds(half, half), pl.ds(0, lanes)),
              (pl.ds(0, rows), pl.ds(lanes, CW - lanes)))

    def piece_copy(q):
        sl = (0, *pieces[q])
        return remote(part.at[sl], recv.at[sl], first_tx.at[q], first_rx.at[q], peers[0])

    for q, (r_sl, c_sl) in enumerate(pieces):
        if q == 0:
            a_copy(0).wait()
            w0_copy(0, 0, lanes).wait()
            for i in range(1, DEPTH):
                w_start(i)
        elif q == 1:
            a_copy(1).wait()
        else:
            w0_copy(1, lanes, CW - lanes).wait()
            w_start(DEPTH)
        part[0, r_sl, c_sl] = dot(a_v[r_sl, :], w_v[0, :, c_sl]).astype(BF16)
        if q == 0:
            pl.semaphore_wait(barrier, 3)
        piece_copy(q).start()

    def chunk(i, col):
        w_copy(i, col).wait()
        w_start(i + DEPTH)
        return dot(a_v[...], w_v[i])

    def cross(i):
        part[i % 2, :, pl.ds(pl.multiple_of((i // 2) * CW, CW), CW)] = chunk(i, cross_col(i)).astype(BF16)

    for i in range(1, 2 * N_COL):
        cross(i)
        col_copy(i % 2, i // 2).start()

    @pl.loop(2 * N_COL, 2 * per)
    def _(i):
        cross(i)

    def send_block(b, row, n):
        row_copy(0, b, row, n).start()
        row_copy(1, b, row, n).start()

    def sent_block(b, row, n):
        row_copy(0, b, row, n).wait_send()
        row_copy(1, b, row, n).wait_send()

    for b in range(AHEAD):
        send_block(b, b * BIG, BIG)
    r_copy.start()
    g_copy.start()

    @pl.loop(0, per)
    def _(j):
        part[2, :, pl.ds(pl.multiple_of(j * CW, CW), CW)] = chunk(2 * per + j, near_col(j)).astype(BF16)

    sib_copy().start()

    @pl.loop(0, per)
    def _(j):
        own[:, pl.ds(pl.multiple_of(j * CW, CW), CW)] = chunk(3 * per + j, near_col(per + j))

    r_copy.wait()
    g_copy.wait()
    sib_copy().wait_recv()
    for q in range(len(pieces)):
        piece_copy(q).wait_recv()
    for i in range(1, 2 * N_COL):
        col_copy(i % 2, i // 2).wait_recv()

    lane = lax.broadcasted_iota(jnp.int32, (8, 128), 1)
    sub = lax.broadcasted_iota(jnp.int32, (8, 128), 0)

    def reduce_block(b, row, n):
        row_copy(0, b, row, n).wait_recv()
        row_copy(1, b, row, n).wait_recv()
        sl = pl.ds(row, n)
        h = own[sl, :] + recv[0, sl, :].astype(F32) + recv[1, sl, :].astype(F32) + recv[2, sl, :].astype(F32)
        h = r_v[sl, :].astype(F32) + h
        own[sl, :] = h
        hid[sl, :] = h.astype(BF16)
        s = jnp.sum(h * h, axis=1, keepdims=True)
        line = jnp.zeros((8, 128), F32)
        for q in range(n // 8):
            line = line + jnp.where(lane == sub + 8 * q, s[8 * q:8 * q + 8, :], 0.0)
        st_tx[b] = jnp.sum(line, axis=0, keepdims=True)
        for k in range(3):
            stat_copy(k, b).start()

    def norm_block(b, row, n):
        for k in range(3):
            stat_copy(k, b).wait_recv()
        tot = (st_tx[b] + st_rx[2, b]) + (st_rx[0, b] + st_rx[1, b])
        scale = lax.rsqrt(tot / d_model + EPS)
        scale = jnp.broadcast_to(scale, (8, 128))
        for q in range(n // 8):
            sl = pl.ds(row + 8 * q, 8)
            col = jnp.sum(jnp.where(lane == sub + 8 * q, scale, 0.0), axis=1, keepdims=True)
            own[sl, :] = own[sl, :] * col * g_v[...]
        sl = pl.ds(row, n)
        nrm[sl, :] = own[sl, :].astype(BF16)

    (row_s, n_s), (row_l, n_l) = blocks

    sent_block(0, 0, BIG)
    send_block(AHEAD, AHEAD * BIG, BIG)
    reduce_block(0, 0, BIG)

    @pl.loop(1, n_big - AHEAD)
    def _(b):
        row = pl.multiple_of(b * BIG, BIG)
        sent_block(b, row, BIG)
        send_block(b + AHEAD, pl.multiple_of(row + AHEAD * BIG, BIG), BIG)
        reduce_block(b, row, BIG)
        norm_block(b - 1, pl.multiple_of(row - BIG, BIG), BIG)

    for q in range(2):
        b = n_big - 2 + q
        sent_block(b, b * BIG, BIG)
        send_block(n_big + q, *blocks[q])
        reduce_block(b, b * BIG, BIG)
        norm_block(b - 1, b * BIG - BIG, BIG)

    reduce_block(n_big, row_s, n_s)
    norm_block(n_big - 1, row_s - BIG, BIG)
    reduce_block(n_big + 1, row_l, n_l)
    norm_block(n_big, row_s, n_s)
    norm_block(n_big + 1, row_l, n_l)
    sent_block(n_big, row_s, n_s)
    sent_block(n_big + 1, row_l, n_l)

    for q in range(len(pieces)):
        piece_copy(q).wait_send()
    for i in range(1, 2 * N_COL):
        col_copy(i % 2, i // 2).wait_send()
    sib_copy().wait_send()

    @pl.loop(0, n_big + 2)
    def _(b):
        for k in range(3):
            stat_copy(k, b).wait_send()


def put(hid, nrm, hid_hbm, nrm_hbm, sem):
    n = hid.shape[0] // PUT
    copies = []
    for q in range(PUT):
        sl = pl.ds(q * n, n)
        copies.append(pltpu.make_async_copy(hid.at[sl, :], hid_hbm.at[sl, :], sem.at[0, q]))
        copies.append(pltpu.make_async_copy(nrm.at[sl, :], nrm_hbm.at[sl, :], sem.at[1, q]))
    for c in copies:
        c.start()
    for c in copies:
        c.wait()


def solution(mesh):
    tp = mesh.shape["tp"]

    def local_step(a, w, r, g):
        rows, depth = a.shape
        d_loc = r.shape[1]
        per = d_loc // CW
        n_blk = (rows - 2 * SMALL) // BIG + 2
        hbm = pl.BlockSpec(memory_space=pltpu.HBM)
        vmem = pl.BlockSpec(memory_space=pltpu.VMEM)
        dma = pltpu.SemaphoreType.DMA
        hid, nrm = pl.pallas_call(
            functools.partial(kernel, d_loc * tp),
            out_shape=(pltpu.VMEM((rows, d_loc), BF16),) * 2,
            in_specs=[hbm] * 4,
            out_specs=(vmem,) * 2,
            scratch_shapes=[
                pltpu.VMEM((rows, depth), BF16),
                pltpu.VMEM((4 * per, depth, CW), BF16),
                pltpu.VMEM((rows, d_loc), BF16),
                pltpu.VMEM((1, d_loc), F32),
                pltpu.VMEM((3, rows, d_loc), BF16),
                pltpu.VMEM((3, rows, d_loc), BF16),
                pltpu.VMEM((rows, d_loc), F32),
                pltpu.VMEM((n_blk, 1, 128), F32),
                pltpu.VMEM((3, n_blk, 1, 128), F32),
                dma((2,)), dma((2,)), dma((4 * per,)), dma, dma, dma((3,)), dma((3,)),
                dma((2, N_COL)), dma((2, N_COL)), dma((2, n_blk)), dma((2, n_blk)), dma, dma,
                dma((3, n_blk)), dma((3, n_blk)),
            ],
            compiler_params=pltpu.CompilerParams(
                collective_id=0, has_side_effects=True, vmem_limit_bytes=64946176),
            cost_estimate=pl.CostEstimate(flops=2 * rows * depth * d_loc * tp, transcendentals=0,
                                          bytes_accessed=2 * depth * d_loc * tp),
        )(a, w, r, g.reshape(1, d_loc))
        return pl.pallas_call(
            put,
            out_shape=(jax.ShapeDtypeStruct((rows, d_loc), BF16),) * 2,
            in_specs=[vmem] * 2,
            out_specs=(hbm,) * 2,
            scratch_shapes=[dma((2, PUT))],
            compiler_params=pltpu.CompilerParams(vmem_limit_bytes=1024 * 1024),
        )(hid, nrm)

    return jax.shard_map(
        local_step,
        mesh=mesh,
        in_specs=(P("data", "tp"), P("tp", None), P("data", "tp"), P("tp")),
        out_specs=(P("data", "tp"), P("data", "tp")),
        check_vma=False,
    )
```

```python
import functools

import jax
import jax.numpy as jnp
from jax import lax
from jax.experimental import pallas as pl
from jax.experimental.pallas import tpu as pltpu
from jax.sharding import PartitionSpec as P

EPS = 1e-5
MESH = pl.DeviceIdType.MESH
F32, BF16 = jnp.float32, jnp.bfloat16

CW = 256
N_COL = 2
BIG, SMALL = 32, 16
DEPTH = 4
PUT = 1
AHEAD = 2


def kernel(d_model, a_hbm, w_hbm, r_hbm, g_hbm, hid, nrm,
           a_v, w_v, r_v, g_v, part, recv, own, st_tx, st_rx,
           a_sem, w0_sem, w_sem, r_sem, g_sem, first_tx, first_rx, col_tx, col_rx, row_tx, row_rx, sib_tx, sib_rx, stat_tx, stat_rx):
    t = lax.axis_index("tp")
    rows, _ = a_v.shape
    d_loc = own.shape[1]
    per = d_loc // CW
    peers = ((t + 2) % 4, 3 - t, t + 1 - 2 * (t % 2))
    n_big = (rows - 2 * SMALL) // BIG
    blocks = [(n_big * BIG, SMALL), (n_big * BIG + SMALL, SMALL)]
    n_blk = n_big + 2
    c0 = N_COL * CW

    def w_copy(slot, col):
        return pltpu.make_async_copy(w_hbm.at[:, pl.ds(pl.multiple_of(col, CW), CW)], w_v.at[slot], w_sem.at[slot])

    def cross_col(i):
        k = i % 2
        return (peers[0] + (peers[1] - peers[0]) * k) * d_loc + (i // 2) * CW

    def near_col(i):
        return (peers[2] + (t - peers[2]) * (i // per)) * d_loc + (i % per) * CW

    def remote(src, dst, tx, rx, peer):
        return pltpu.make_async_remote_copy(src_ref=src, dst_ref=dst, send_sem=tx, recv_sem=rx,
                                            device_id={"tp": peer}, device_id_type=MESH)

    def col_copy(k, j):
        cols = pl.ds(j * CW, CW)
        return remote(part.at[k, :, cols], recv.at[k, :, cols], col_tx.at[k, j], col_rx.at[k, j], peers[k])

    def row_copy(k, b, row, n):
        sl = (k, pl.ds(row, n), pl.ds(c0, d_loc - c0))
        return remote(part.at[sl], recv.at[sl], row_tx.at[k, b], row_rx.at[k, b], peers[k])

    def sib_copy():
        return remote(part.at[2], recv.at[2], sib_tx, sib_rx, peers[2])

    def stat_copy(k, b):
        return remote(st_tx.at[b], st_rx.at[k, b], stat_tx.at[k, b], stat_rx.at[k, b], peers[k])

    half, lanes = rows // 2, 128

    def a_copy(q):
        sl = pl.ds(q * half, half)
        return pltpu.make_async_copy(a_hbm.at[sl, :], a_v.at[sl, :], a_sem.at[q])

    def w0_copy(q, first, n):
        src = w_hbm.at[:, pl.ds(pl.multiple_of(cross_col(0) + first, lanes), n)]
        return pltpu.make_async_copy(src, w_v.at[0, :, pl.ds(first, n)], w0_sem.at[q])

    def w_start(i):
        if isinstance(i, int):
            w_copy(i, cross_col(i) if i < 2 * per else near_col(i - 2 * per)).start()
            return

        @pl.when(i < 2 * per)
        def _():
            w_copy(i, cross_col(i)).start()

        @pl.when((i >= 2 * per) & (i < 4 * per))
        def _():
            w_copy(i, near_col(i - 2 * per)).start()

    r_copy = pltpu.make_async_copy(r_hbm, r_v, r_sem)
    g_copy = pltpu.make_async_copy(g_hbm, g_v, g_sem)
    a_copy(0).start()
    w0_copy(0, 0, lanes).start()
    a_copy(1).start()
    w0_copy(1, lanes, CW - lanes).start()
    barrier = pltpu.get_barrier_semaphore()
    for p in peers:
        pl.semaphore_signal(barrier, inc=1, device_id={"tp": p}, device_id_type=MESH)

    def dot(lhs, rhs):
        return jnp.dot(lhs, rhs, preferred_element_type=F32)

    pieces = ((pl.ds(0, half), pl.ds(0, lanes)), (pl.ds(half, half), pl.ds(0, lanes)),
              (pl.ds(0, rows), pl.ds(lanes, CW - lanes)))

    def piece_copy(q):
        sl = (0, *pieces[q])
        return remote(part.at[sl], recv.at[sl], first_tx.at[q], first_rx.at[q], peers[0])

    for q, (r_sl, c_sl) in enumerate(pieces):
        if q == 0:
            a_copy(0).wait()
            w0_copy(0, 0, lanes).wait()
            for i in range(1, DEPTH):
                w_start(i)
        elif q == 1:
            a_copy(1).wait()
        else:
            w0_copy(1, lanes, CW - lanes).wait()
            w_start(DEPTH)
        part[0, r_sl, c_sl] = dot(a_v[r_sl, :], w_v[0, :, c_sl]).astype(BF16)
        if q == 0:
            pl.semaphore_wait(barrier, 3)
        piece_copy(q).start()

    def chunk(i, col):
        w_copy(i, col).wait()
        w_start(i + DEPTH)
        return dot(a_v[...], w_v[i])

    def cross(i):
        part[i % 2, :, pl.ds(pl.multiple_of((i // 2) * CW, CW), CW)] = chunk(i, cross_col(i)).astype(BF16)

    for i in range(1, 2 * N_COL):
        cross(i)
        col_copy(i % 2, i // 2).start()

    @pl.loop(2 * N_COL, 2 * per)
    def _(i):
        cross(i)

    def send_block(b, row, n):
        row_copy(0, b, row, n).start()
        row_copy(1, b, row, n).start()

    def sent_block(b, row, n):
        row_copy(0, b, row, n).wait_send()
        row_copy(1, b, row, n).wait_send()

    for b in range(AHEAD):
        send_block(b, b * BIG, BIG)
    r_copy.start()
    g_copy.start()

    @pl.loop(0, per)
    def _(j):
        part[2, :, pl.ds(pl.multiple_of(j * CW, CW), CW)] = chunk(2 * per + j, near_col(j)).astype(BF16)

    sib_copy().start()

    @pl.loop(0, per)
    def _(j):
        own[:, pl.ds(pl.multiple_of(j * CW, CW), CW)] = chunk(3 * per + j, near_col(per + j))

    r_copy.wait()
    g_copy.wait()
    sib_copy().wait_recv()
    for q in range(len(pieces)):
        piece_copy(q).wait_recv()
    for i in range(1, 2 * N_COL):
        col_copy(i % 2, i // 2).wait_recv()

    lane = lax.broadcasted_iota(jnp.int32, (8, 128), 1)
    sub = lax.broadcasted_iota(jnp.int32, (8, 128), 0)

    def reduce_block(b, row, n):
        row_copy(0, b, row, n).wait_recv()
        row_copy(1, b, row, n).wait_recv()
        sl = pl.ds(row, n)
        h = own[sl, :] + recv[0, sl, :].astype(F32) + recv[1, sl, :].astype(F32) + recv[2, sl, :].astype(F32)
        h = r_v[sl, :].astype(F32) + h
        own[sl, :] = h
        hid[sl, :] = h.astype(BF16)
        s = jnp.sum(h * h, axis=1, keepdims=True)
        line = jnp.zeros((8, 128), F32)
        for q in range(n // 8):
            line = line + jnp.where(lane == sub + 8 * q, s[8 * q:8 * q + 8, :], 0.0)
        st_tx[b] = jnp.sum(line, axis=0, keepdims=True)
        for k in range(3):
            stat_copy(k, b).start()

    def norm_block(b, row, n):
        for k in range(3):
            stat_copy(k, b).wait_recv()
        tot = (st_tx[b] + st_rx[2, b]) + (st_rx[0, b] + st_rx[1, b])
        scale = lax.rsqrt(tot / d_model + EPS)
        scale = jnp.broadcast_to(scale, (8, 128))
        for q in range(n // 8):
            sl = pl.ds(row + 8 * q, 8)
            col = jnp.sum(jnp.where(lane == sub + 8 * q, scale, 0.0), axis=1, keepdims=True)
            own[sl, :] = own[sl, :] * col * g_v[...]
        sl = pl.ds(row, n)
        nrm[sl, :] = own[sl, :].astype(BF16)

    (row_s, n_s), (row_l, n_l) = blocks

    sent_block(0, 0, BIG)
    send_block(AHEAD, AHEAD * BIG, BIG)
    reduce_block(0, 0, BIG)

    @pl.loop(1, n_big - AHEAD)
    def _(b):
        row = pl.multiple_of(b * BIG, BIG)
        sent_block(b, row, BIG)
        send_block(b + AHEAD, pl.multiple_of(row + AHEAD * BIG, BIG), BIG)
        reduce_block(b, row, BIG)
        norm_block(b - 1, pl.multiple_of(row - BIG, BIG), BIG)

    for q in range(2):
        b = n_big - 2 + q
        sent_block(b, b * BIG, BIG)
        send_block(n_big + q, *blocks[q])
        reduce_block(b, b * BIG, BIG)
        norm_block(b - 1, b * BIG - BIG, BIG)

    reduce_block(n_big, row_s, n_s)
    reduce_block(n_big + 1, row_l, n_l)
    norm_block(n_big - 1, row_s - BIG, BIG)
    norm_block(n_big, row_s, n_s)
    norm_block(n_big + 1, row_l, n_l)
    sent_block(n_big, row_s, n_s)
    sent_block(n_big + 1, row_l, n_l)

    for q in range(len(pieces)):
        piece_copy(q).wait_send()
    for i in range(1, 2 * N_COL):
        col_copy(i % 2, i // 2).wait_send()
    sib_copy().wait_send()

    @pl.loop(0, n_big + 2)
    def _(b):
        for k in range(3):
            stat_copy(k, b).wait_send()


def put(hid, nrm, hid_hbm, nrm_hbm, sem):
    n = hid.shape[0] // PUT
    copies = []
    for q in range(PUT):
        sl = pl.ds(q * n, n)
        copies.append(pltpu.make_async_copy(hid.at[sl, :], hid_hbm.at[sl, :], sem.at[0, q]))
        copies.append(pltpu.make_async_copy(nrm.at[sl, :], nrm_hbm.at[sl, :], sem.at[1, q]))
    for c in copies:
        c.start()
    for c in copies:
        c.wait()


def solution(mesh):
    tp = mesh.shape["tp"]

    def local_step(a, w, r, g):
        rows, depth = a.shape
        d_loc = r.shape[1]
        per = d_loc // CW
        n_blk = (rows - 2 * SMALL) // BIG + 2
        hbm = pl.BlockSpec(memory_space=pltpu.HBM)
        vmem = pl.BlockSpec(memory_space=pltpu.VMEM)
        dma = pltpu.SemaphoreType.DMA
        hid, nrm = pl.pallas_call(
            functools.partial(kernel, d_loc * tp),
            out_shape=(pltpu.VMEM((rows, d_loc), BF16),) * 2,
            in_specs=[hbm] * 4,
            out_specs=(vmem,) * 2,
            scratch_shapes=[
                pltpu.VMEM((rows, depth), BF16),
                pltpu.VMEM((4 * per, depth, CW), BF16),
                pltpu.VMEM((rows, d_loc), BF16),
                pltpu.VMEM((1, d_loc), F32),
                pltpu.VMEM((3, rows, d_loc), BF16),
                pltpu.VMEM((3, rows, d_loc), BF16),
                pltpu.VMEM((rows, d_loc), F32),
                pltpu.VMEM((n_blk, 1, 128), F32),
                pltpu.VMEM((3, n_blk, 1, 128), F32),
                dma((2,)), dma((2,)), dma((4 * per,)), dma, dma, dma((3,)), dma((3,)),
                dma((2, N_COL)), dma((2, N_COL)), dma((2, n_blk)), dma((2, n_blk)), dma, dma,
                dma((3, n_blk)), dma((3, n_blk)),
            ],
            compiler_params=pltpu.CompilerParams(
                collective_id=0, has_side_effects=True, vmem_limit_bytes=64946176),
            cost_estimate=pl.CostEstimate(flops=2 * rows * depth * d_loc * tp, transcendentals=0,
                                          bytes_accessed=2 * depth * d_loc * tp),
        )(a, w, r, g.reshape(1, d_loc))
        return pl.pallas_call(
            put,
            out_shape=(jax.ShapeDtypeStruct((rows, d_loc), BF16),) * 2,
            in_specs=[vmem] * 2,
            out_specs=(hbm,) * 2,
            scratch_shapes=[dma((2, PUT))],
            compiler_params=pltpu.CompilerParams(vmem_limit_bytes=1024 * 1024),
        )(hid, nrm)

    return jax.shard_map(
        local_step,
        mesh=mesh,
        in_specs=(P("data", "tp"), P("tp", None), P("data", "tp"), P("tp")),
        out_specs=(P("data", "tp"), P("data", "tp")),
        check_vma=False,
    )
```

```python
import functools

import jax
import jax.numpy as jnp
from jax import lax
from jax.experimental import pallas as pl
from jax.experimental.pallas import tpu as pltpu
from jax.sharding import PartitionSpec as P

EPS = 1e-5
MESH = pl.DeviceIdType.MESH
F32, BF16 = jnp.float32, jnp.bfloat16

CW = 256
N_COL = 2
BLOCKS = (64, 64, 64, 32, 16, 16)
SUB = 16
DEPTH = 4
PUT = 1
AHEAD = 2


def kernel(d_model, a_hbm, w_hbm, r_hbm, g_hbm, hid, nrm,
           a_v, w_v, r_v, g_v, part, recv, own, st_tx, st_rx,
           a_sem, w0_sem, w_sem, r_sem, g_sem, first_tx, first_rx, col_tx, col_rx, row_tx, row_rx, sib_tx, sib_rx, stat_tx, stat_rx):
    t = lax.axis_index("tp")
    rows, _ = a_v.shape
    d_loc = own.shape[1]
    per = d_loc // CW
    peers = ((t + 2) % 4, 3 - t, t + 1 - 2 * (t % 2))
    n_blk = len(BLOCKS)
    blocks = [(sum(BLOCKS[:b]), BLOCKS[b]) for b in range(n_blk)]
    c0 = N_COL * CW

    def w_copy(slot, col):
        return pltpu.make_async_copy(w_hbm.at[:, pl.ds(pl.multiple_of(col, CW), CW)], w_v.at[slot], w_sem.at[slot])

    def cross_col(i):
        k = i % 2
        return (peers[0] + (peers[1] - peers[0]) * k) * d_loc + (i // 2) * CW

    def near_col(i):
        return (peers[2] + (t - peers[2]) * (i // per)) * d_loc + (i % per) * CW

    def remote(src, dst, tx, rx, peer):
        return pltpu.make_async_remote_copy(src_ref=src, dst_ref=dst, send_sem=tx, recv_sem=rx,
                                            device_id={"tp": peer}, device_id_type=MESH)

    def col_copy(k, j):
        cols = pl.ds(j * CW, CW)
        return remote(part.at[k, :, cols], recv.at[k, :, cols], col_tx.at[k, j], col_rx.at[k, j], peers[k])

    def row_copy(k, b):
        sl = (k, pl.ds(*blocks[b]), pl.ds(c0, d_loc - c0))
        return remote(part.at[sl], recv.at[sl], row_tx.at[k, b], row_rx.at[k, b], peers[k])

    def sib_copy():
        return remote(part.at[2], recv.at[2], sib_tx, sib_rx, peers[2])

    def stat_copy(k, b):
        return remote(st_tx.at[b], st_rx.at[k, b], stat_tx.at[k, b], stat_rx.at[k, b], peers[k])

    half, lanes = rows // 2, 128

    def a_copy(q):
        sl = pl.ds(q * half, half)
        return pltpu.make_async_copy(a_hbm.at[sl, :], a_v.at[sl, :], a_sem.at[q])

    def w0_copy(q, first, n):
        src = w_hbm.at[:, pl.ds(pl.multiple_of(cross_col(0) + first, lanes), n)]
        return pltpu.make_async_copy(src, w_v.at[0, :, pl.ds(first, n)], w0_sem.at[q])

    def w_start(i):
        if isinstance(i, int):
            w_copy(i, cross_col(i) if i < 2 * per else near_col(i - 2 * per)).start()
            return

        @pl.when(i < 2 * per)
        def _():
            w_copy(i, cross_col(i)).start()

        @pl.when((i >= 2 * per) & (i < 4 * per))
        def _():
            w_copy(i, near_col(i - 2 * per)).start()

    r_copy = pltpu.make_async_copy(r_hbm, r_v, r_sem)
    g_copy = pltpu.make_async_copy(g_hbm, g_v, g_sem)
    a_copy(0).start()
    w0_copy(0, 0, lanes).start()
    a_copy(1).start()
    w0_copy(1, lanes, CW - lanes).start()
    barrier = pltpu.get_barrier_semaphore()
    for p in peers:
        pl.semaphore_signal(barrier, inc=1, device_id={"tp": p}, device_id_type=MESH)

    def dot(lhs, rhs):
        return jnp.dot(lhs, rhs, preferred_element_type=F32)

    pieces = ((pl.ds(0, half), pl.ds(0, lanes)), (pl.ds(half, half), pl.ds(0, lanes)),
              (pl.ds(0, rows), pl.ds(lanes, CW - lanes)))

    def piece_copy(q):
        sl = (0, *pieces[q])
        return remote(part.at[sl], recv.at[sl], first_tx.at[q], first_rx.at[q], peers[0])

    for q, (r_sl, c_sl) in enumerate(pieces):
        if q == 0:
            a_copy(0).wait()
            w0_copy(0, 0, lanes).wait()
            for i in range(1, DEPTH):
                w_start(i)
        elif q == 1:
            a_copy(1).wait()
        else:
            w0_copy(1, lanes, CW - lanes).wait()
            w_start(DEPTH)
        part[0, r_sl, c_sl] = dot(a_v[r_sl, :], w_v[0, :, c_sl]).astype(BF16)
        if q == 0:
            pl.semaphore_wait(barrier, 3)
        piece_copy(q).start()

    def chunk(i, col):
        w_copy(i, col).wait()
        w_start(i + DEPTH)
        return dot(a_v[...], w_v[i])

    def cross(i):
        part[i % 2, :, pl.ds(pl.multiple_of((i // 2) * CW, CW), CW)] = chunk(i, cross_col(i)).astype(BF16)

    for i in range(1, 2 * N_COL):
        cross(i)
        col_copy(i % 2, i // 2).start()

    @pl.loop(2 * N_COL, 2 * per)
    def _(i):
        cross(i)

    def send_block(b):
        row_copy(0, b).start()
        row_copy(1, b).start()

    for b in range(AHEAD):
        send_block(b)
    r_copy.start()
    g_copy.start()

    @pl.loop(0, per)
    def _(j):
        part[2, :, pl.ds(pl.multiple_of(j * CW, CW), CW)] = chunk(2 * per + j, near_col(j)).astype(BF16)

    sib_copy().start()

    @pl.loop(0, per)
    def _(j):
        own[:, pl.ds(pl.multiple_of(j * CW, CW), CW)] = chunk(3 * per + j, near_col(per + j))

    r_copy.wait()
    g_copy.wait()
    sib_copy().wait_recv()
    for q in range(len(pieces)):
        piece_copy(q).wait_recv()
    for i in range(1, 2 * N_COL):
        col_copy(i % 2, i // 2).wait_recv()

    lane = lax.broadcasted_iota(jnp.int32, (8, 128), 1)
    sub = lax.broadcasted_iota(jnp.int32, (8, 128), 0)

    def reduce_block(b):
        row_copy(0, b).wait_recv()
        row_copy(1, b).wait_recv()
        row, n = blocks[b]
        line = jnp.zeros((8, 128), F32)
        for first in range(0, n, SUB):
            sl = pl.ds(row + first, SUB)
            h = own[sl, :] + recv[0, sl, :].astype(F32) + recv[1, sl, :].astype(F32) + recv[2, sl, :].astype(F32)
            h = r_v[sl, :].astype(F32) + h
            own[sl, :] = h
            hid[sl, :] = h.astype(BF16)
            s = jnp.sum(h * h, axis=1, keepdims=True)
            for q in range(0, SUB, 8):
                line = line + jnp.where(lane == sub + (first + q), s[q:q + 8, :], 0.0)
        st_tx[b] = jnp.sum(line, axis=0, keepdims=True)
        for k in range(3):
            stat_copy(k, b).start()

    def norm_block(b):
        for k in range(3):
            stat_copy(k, b).wait_recv()
        row, n = blocks[b]
        tot = (st_tx[b] + st_rx[2, b]) + (st_rx[0, b] + st_rx[1, b])
        scale = jnp.broadcast_to(lax.rsqrt(tot / d_model + EPS), (8, 128))
        for first in range(0, n, SUB):
            for q in range(first, first + SUB, 8):
                sl = pl.ds(row + q, 8)
                col = jnp.sum(jnp.where(lane == sub + q, scale, 0.0), axis=1, keepdims=True)
                own[sl, :] = own[sl, :] * col * g_v[...]
            sl = pl.ds(row + first, SUB)
            nrm[sl, :] = own[sl, :].astype(BF16)

    for b in range(n_blk - 2):
        row_copy(0, b).wait_send()
        row_copy(1, b).wait_send()
        if b + AHEAD < n_blk:
            send_block(b + AHEAD)
        reduce_block(b)
        if b:
            norm_block(b - 1)

    reduce_block(n_blk - 2)
    reduce_block(n_blk - 1)
    for b in range(n_blk - 3, n_blk):
        norm_block(b)

    for b in range(n_blk - 2, n_blk):
        row_copy(0, b).wait_send()
        row_copy(1, b).wait_send()

    for q in range(len(pieces)):
        piece_copy(q).wait_send()
    for i in range(1, 2 * N_COL):
        col_copy(i % 2, i // 2).wait_send()
    sib_copy().wait_send()

    @pl.loop(0, n_blk)
    def _(b):
        for k in range(3):
            stat_copy(k, b).wait_send()


def put(hid, nrm, hid_hbm, nrm_hbm, sem):
    n = hid.shape[0] // PUT
    copies = []
    for q in range(PUT):
        sl = pl.ds(q * n, n)
        copies.append(pltpu.make_async_copy(hid.at[sl, :], hid_hbm.at[sl, :], sem.at[0, q]))
        copies.append(pltpu.make_async_copy(nrm.at[sl, :], nrm_hbm.at[sl, :], sem.at[1, q]))
    for c in copies:
        c.start()
    for c in copies:
        c.wait()


def solution(mesh):
    tp = mesh.shape["tp"]

    def local_step(a, w, r, g):
        rows, depth = a.shape
        d_loc = r.shape[1]
        per = d_loc // CW
        n_blk = len(BLOCKS)
        hbm = pl.BlockSpec(memory_space=pltpu.HBM)
        vmem = pl.BlockSpec(memory_space=pltpu.VMEM)
        dma = pltpu.SemaphoreType.DMA
        hid, nrm = pl.pallas_call(
            functools.partial(kernel, d_loc * tp),
            out_shape=(pltpu.VMEM((rows, d_loc), BF16),) * 2,
            in_specs=[hbm] * 4,
            out_specs=(vmem,) * 2,
            scratch_shapes=[
                pltpu.VMEM((rows, depth), BF16),
                pltpu.VMEM((4 * per, depth, CW), BF16),
                pltpu.VMEM((rows, d_loc), BF16),
                pltpu.VMEM((1, d_loc), F32),
                pltpu.VMEM((3, rows, d_loc), BF16),
                pltpu.VMEM((3, rows, d_loc), BF16),
                pltpu.VMEM((rows, d_loc), F32),
                pltpu.VMEM((n_blk, 1, 128), F32),
                pltpu.VMEM((3, n_blk, 1, 128), F32),
                dma((2,)), dma((2,)), dma((4 * per,)), dma, dma, dma((3,)), dma((3,)),
                dma((2, N_COL)), dma((2, N_COL)), dma((2, n_blk)), dma((2, n_blk)), dma, dma,
                dma((3, n_blk)), dma((3, n_blk)),
            ],
            compiler_params=pltpu.CompilerParams(
                collective_id=0, has_side_effects=True, vmem_limit_bytes=64946176),
            cost_estimate=pl.CostEstimate(flops=2 * rows * depth * d_loc * tp, transcendentals=0,
                                          bytes_accessed=2 * depth * d_loc * tp),
        )(a, w, r, g.reshape(1, d_loc))
        return pl.pallas_call(
            put,
            out_shape=(jax.ShapeDtypeStruct((rows, d_loc), BF16),) * 2,
            in_specs=[vmem] * 2,
            out_specs=(hbm,) * 2,
            scratch_shapes=[dma((2, PUT))],
            compiler_params=pltpu.CompilerParams(vmem_limit_bytes=1024 * 1024),
        )(hid, nrm)

    return jax.shard_map(
        local_step,
        mesh=mesh,
        in_specs=(P("data", "tp"), P("tp", None), P("data", "tp"), P("tp")),
        out_specs=(P("data", "tp"), P("data", "tp")),
        check_vma=False,
    )
```

```python
import functools

import jax
import jax.numpy as jnp
from jax import lax
from jax.experimental import pallas as pl
from jax.experimental.pallas import tpu as pltpu
from jax.sharding import PartitionSpec as P

EPS = 1e-5
MESH = pl.DeviceIdType.MESH
F32, BF16 = jnp.float32, jnp.bfloat16

CW = 256
N_COL = 2
BLOCKS = (64, 64, 64, 32, 16, 16)
SUB = 16
DEPTH = 4
PUT = 1
LAG = 2
AHEAD = 2


def kernel(d_model, a_hbm, w_hbm, r_hbm, g_hbm, hid, nrm,
           a_v, w_v, r_v, g_v, part, recv, own, st_tx, st_rx,
           a_sem, w0_sem, w_sem, r_sem, g_sem, first_tx, first_rx, col_tx, col_rx, row_tx, row_rx, sib_tx, sib_rx, stat_tx, stat_rx):
    t = lax.axis_index("tp")
    rows, _ = a_v.shape
    d_loc = own.shape[1]
    per = d_loc // CW
    peers = ((t + 2) % 4, 3 - t, t + 1 - 2 * (t % 2))
    n_blk = len(BLOCKS)
    blocks = [(sum(BLOCKS[:b]), BLOCKS[b]) for b in range(n_blk)]
    c0 = N_COL * CW

    def w_copy(slot, col):
        return pltpu.make_async_copy(w_hbm.at[:, pl.ds(pl.multiple_of(col, CW), CW)], w_v.at[slot], w_sem.at[slot])

    def cross_col(i):
        k = i % 2
        return (peers[0] + (peers[1] - peers[0]) * k) * d_loc + (i // 2) * CW

    def near_col(i):
        return (peers[2] + (t - peers[2]) * (i // per)) * d_loc + (i % per) * CW

    def remote(src, dst, tx, rx, peer):
        return pltpu.make_async_remote_copy(src_ref=src, dst_ref=dst, send_sem=tx, recv_sem=rx,
                                            device_id={"tp": peer}, device_id_type=MESH)

    def col_copy(k, j):
        cols = pl.ds(j * CW, CW)
        return remote(part.at[k, :, cols], recv.at[k, :, cols], col_tx.at[k, j], col_rx.at[k, j], peers[k])

    def row_copy(k, b):
        sl = (k, pl.ds(*blocks[b]), pl.ds(c0, d_loc - c0))
        return remote(part.at[sl], recv.at[sl], row_tx.at[k, b], row_rx.at[k, b], peers[k])

    def sib_copy():
        return remote(part.at[2], recv.at[2], sib_tx, sib_rx, peers[2])

    def stat_copy(k, b):
        return remote(st_tx.at[b], st_rx.at[k, b], stat_tx.at[k, b], stat_rx.at[k, b], peers[k])

    half, lanes = rows // 2, 128

    def a_copy(q):
        sl = pl.ds(q * half, half)
        return pltpu.make_async_copy(a_hbm.at[sl, :], a_v.at[sl, :], a_sem.at[q])

    def w0_copy(q, first, n):
        src = w_hbm.at[:, pl.ds(pl.multiple_of(cross_col(0) + first, lanes), n)]
        return pltpu.make_async_copy(src, w_v.at[0, :, pl.ds(first, n)], w0_sem.at[q])

    def w_start(i):
        if isinstance(i, int):
            w_copy(i, cross_col(i) if i < 2 * per else near_col(i - 2 * per)).start()
            return

        @pl.when(i < 2 * per)
        def _():
            w_copy(i, cross_col(i)).start()

        @pl.when((i >= 2 * per) & (i < 4 * per))
        def _():
            w_copy(i, near_col(i - 2 * per)).start()

    r_copy = pltpu.make_async_copy(r_hbm, r_v, r_sem)
    g_copy = pltpu.make_async_copy(g_hbm, g_v, g_sem)
    a_copy(0).start()
    w0_copy(0, 0, lanes).start()
    a_copy(1).start()
    w0_copy(1, lanes, CW - lanes).start()
    barrier = pltpu.get_barrier_semaphore()
    for p in peers:
        pl.semaphore_signal(barrier, inc=1, device_id={"tp": p}, device_id_type=MESH)

    def dot(lhs, rhs):
        return jnp.dot(lhs, rhs, preferred_element_type=F32)

    pieces = ((pl.ds(0, half), pl.ds(0, lanes)), (pl.ds(half, half), pl.ds(0, lanes)),
              (pl.ds(0, rows), pl.ds(lanes, CW - lanes)))

    def piece_copy(q):
        sl = (0, *pieces[q])
        return remote(part.at[sl], recv.at[sl], first_tx.at[q], first_rx.at[q], peers[0])

    for q, (r_sl, c_sl) in enumerate(pieces):
        if q == 0:
            a_copy(0).wait()
            w0_copy(0, 0, lanes).wait()
            for i in range(1, DEPTH):
                w_start(i)
        elif q == 1:
            a_copy(1).wait()
        else:
            w0_copy(1, lanes, CW - lanes).wait()
            w_start(DEPTH)
        part[0, r_sl, c_sl] = dot(a_v[r_sl, :], w_v[0, :, c_sl]).astype(BF16)
        if q == 0:
            pl.semaphore_wait(barrier, 3)
        piece_copy(q).start()

    def chunk(i, col):
        w_copy(i, col).wait()
        w_start(i + DEPTH)
        return dot(a_v[...], w_v[i])

    def cross(i):
        part[i % 2, :, pl.ds(pl.multiple_of((i // 2) * CW, CW), CW)] = chunk(i, cross_col(i)).astype(BF16)

    for i in range(1, 2 * N_COL):
        cross(i)
        col_copy(i % 2, i // 2).start()

    @pl.loop(2 * N_COL, 2 * per)
    def _(i):
        cross(i)

    def send_block(b):
        row_copy(0, b).start()
        row_copy(1, b).start()

    for b in range(AHEAD):
        send_block(b)
    r_copy.start()
    g_copy.start()

    @pl.loop(0, per)
    def _(j):
        part[2, :, pl.ds(pl.multiple_of(j * CW, CW), CW)] = chunk(2 * per + j, near_col(j)).astype(BF16)

    sib_copy().start()

    @pl.loop(0, per)
    def _(j):
        own[:, pl.ds(pl.multiple_of(j * CW, CW), CW)] = chunk(3 * per + j, near_col(per + j))

    r_copy.wait()
    g_copy.wait()
    sib_copy().wait_recv()
    for q in range(len(pieces)):
        piece_copy(q).wait_recv()
    for i in range(1, 2 * N_COL):
        col_copy(i % 2, i // 2).wait_recv()

    lane = lax.broadcasted_iota(jnp.int32, (8, 128), 1)
    sub = lax.broadcasted_iota(jnp.int32, (8, 128), 0)

    def reduce_block(b):
        row_copy(0, b).wait_recv()
        row_copy(1, b).wait_recv()
        row, n = blocks[b]
        line = jnp.zeros((8, 128), F32)
        for first in range(0, n, SUB):
            sl = pl.ds(row + first, SUB)
            h = own[sl, :] + recv[0, sl, :].astype(F32) + recv[1, sl, :].astype(F32) + recv[2, sl, :].astype(F32)
            h = r_v[sl, :].astype(F32) + h
            own[sl, :] = h
            hid[sl, :] = h.astype(BF16)
            s = jnp.sum(h * h, axis=1, keepdims=True)
            for q in range(0, SUB, 8):
                line = line + jnp.where(lane == sub + (first + q), s[q:q + 8, :], 0.0)
        st_tx[b] = jnp.sum(line, axis=0, keepdims=True)
        for k in range(3):
            stat_copy(k, b).start()

    def norm_block(b):
        for k in range(3):
            stat_copy(k, b).wait_recv()
        row, n = blocks[b]
        tot = (st_tx[b] + st_rx[2, b]) + (st_rx[0, b] + st_rx[1, b])
        scale = jnp.broadcast_to(lax.rsqrt(tot / d_model + EPS), (8, 128))
        for first in range(0, n, SUB):
            for q in range(first, first + SUB, 8):
                sl = pl.ds(row + q, 8)
                col = jnp.sum(jnp.where(lane == sub + q, scale, 0.0), axis=1, keepdims=True)
                own[sl, :] = own[sl, :] * col * g_v[...]
            sl = pl.ds(row + first, SUB)
            nrm[sl, :] = own[sl, :].astype(BF16)

    for b in range(n_blk - 2):
        row_copy(0, b).wait_send()
        row_copy(1, b).wait_send()
        if b + AHEAD < n_blk:
            send_block(b + AHEAD)
        reduce_block(b)
        if b >= LAG:
            norm_block(b - LAG)

    reduce_block(n_blk - 2)
    reduce_block(n_blk - 1)
    for b in range(n_blk - 2 - LAG, n_blk):
        norm_block(b)

    for b in range(n_blk - 2, n_blk):
        row_copy(0, b).wait_send()
        row_copy(1, b).wait_send()

    for q in range(len(pieces)):
        piece_copy(q).wait_send()
    for i in range(1, 2 * N_COL):
        col_copy(i % 2, i // 2).wait_send()
    sib_copy().wait_send()

    @pl.loop(0, n_blk)
    def _(b):
        for k in range(3):
            stat_copy(k, b).wait_send()


def put(hid, nrm, hid_hbm, nrm_hbm, sem):
    n = hid.shape[0] // PUT
    copies = []
    for q in range(PUT):
        sl = pl.ds(q * n, n)
        copies.append(pltpu.make_async_copy(hid.at[sl, :], hid_hbm.at[sl, :], sem.at[0, q]))
        copies.append(pltpu.make_async_copy(nrm.at[sl, :], nrm_hbm.at[sl, :], sem.at[1, q]))
    for c in copies:
        c.start()
    for c in copies:
        c.wait()


def solution(mesh):
    tp = mesh.shape["tp"]

    def local_step(a, w, r, g):
        rows, depth = a.shape
        d_loc = r.shape[1]
        per = d_loc // CW
        n_blk = len(BLOCKS)
        hbm = pl.BlockSpec(memory_space=pltpu.HBM)
        vmem = pl.BlockSpec(memory_space=pltpu.VMEM)
        dma = pltpu.SemaphoreType.DMA
        hid, nrm = pl.pallas_call(
            functools.partial(kernel, d_loc * tp),
            out_shape=(pltpu.VMEM((rows, d_loc), BF16),) * 2,
            in_specs=[hbm] * 4,
            out_specs=(vmem,) * 2,
            scratch_shapes=[
                pltpu.VMEM((rows, depth), BF16),
                pltpu.VMEM((4 * per, depth, CW), BF16),
                pltpu.VMEM((rows, d_loc), BF16),
                pltpu.VMEM((1, d_loc), F32),
                pltpu.VMEM((3, rows, d_loc), BF16),
                pltpu.VMEM((3, rows, d_loc), BF16),
                pltpu.VMEM((rows, d_loc), F32),
                pltpu.VMEM((n_blk, 1, 128), F32),
                pltpu.VMEM((3, n_blk, 1, 128), F32),
                dma((2,)), dma((2,)), dma((4 * per,)), dma, dma, dma((3,)), dma((3,)),
                dma((2, N_COL)), dma((2, N_COL)), dma((2, n_blk)), dma((2, n_blk)), dma, dma,
                dma((3, n_blk)), dma((3, n_blk)),
            ],
            compiler_params=pltpu.CompilerParams(
                collective_id=0, has_side_effects=True, vmem_limit_bytes=64946176),
            cost_estimate=pl.CostEstimate(flops=2 * rows * depth * d_loc * tp, transcendentals=0,
                                          bytes_accessed=2 * depth * d_loc * tp),
        )(a, w, r, g.reshape(1, d_loc))
        return pl.pallas_call(
            put,
            out_shape=(jax.ShapeDtypeStruct((rows, d_loc), BF16),) * 2,
            in_specs=[vmem] * 2,
            out_specs=(hbm,) * 2,
            scratch_shapes=[dma((2, PUT))],
            compiler_params=pltpu.CompilerParams(vmem_limit_bytes=1024 * 1024),
        )(hid, nrm)

    return jax.shard_map(
        local_step,
        mesh=mesh,
        in_specs=(P("data", "tp"), P("tp", None), P("data", "tp"), P("tp")),
        out_specs=(P("data", "tp"), P("data", "tp")),
        check_vma=False,
    )
```

```python
import functools

import jax
import jax.numpy as jnp
from jax import lax
from jax.experimental import pallas as pl
from jax.experimental.pallas import tpu as pltpu
from jax.sharding import PartitionSpec as P

EPS = 1e-5
MESH = pl.DeviceIdType.MESH
F32, BF16 = jnp.float32, jnp.bfloat16

CW = 256
N_COL = 2
BLOCKS = (128, 112, 16)
SUB = 16
DEPTH = 4
PUT = 1
AHEAD = 2


def kernel(d_model, a_hbm, w_hbm, r_hbm, g_hbm, hid, nrm,
           a_v, w_v, r_v, g_v, part, recv, own, st_tx, st_rx,
           a_sem, w0_sem, w_sem, r_sem, g_sem, first_tx, first_rx, col_tx, col_rx, row_tx, row_rx, sib_tx, sib_rx, stat_tx, stat_rx):
    t = lax.axis_index("tp")
    rows, _ = a_v.shape
    d_loc = own.shape[1]
    per = d_loc // CW
    peers = ((t + 2) % 4, 3 - t, t + 1 - 2 * (t % 2))
    n_blk = len(BLOCKS)
    blocks = [(sum(BLOCKS[:b]), BLOCKS[b]) for b in range(n_blk)]
    c0 = N_COL * CW

    def w_copy(slot, col):
        return pltpu.make_async_copy(w_hbm.at[:, pl.ds(pl.multiple_of(col, CW), CW)], w_v.at[slot], w_sem.at[slot])

    def cross_col(i):
        k = i % 2
        return (peers[0] + (peers[1] - peers[0]) * k) * d_loc + (i // 2) * CW

    def near_col(i):
        return (peers[2] + (t - peers[2]) * (i // per)) * d_loc + (i % per) * CW

    def remote(src, dst, tx, rx, peer):
        return pltpu.make_async_remote_copy(src_ref=src, dst_ref=dst, send_sem=tx, recv_sem=rx,
                                            device_id={"tp": peer}, device_id_type=MESH)

    def col_copy(k, j):
        cols = pl.ds(j * CW, CW)
        return remote(part.at[k, :, cols], recv.at[k, :, cols], col_tx.at[k, j], col_rx.at[k, j], peers[k])

    def row_copy(k, b):
        sl = (k, pl.ds(*blocks[b]), pl.ds(c0, d_loc - c0))
        return remote(part.at[sl], recv.at[sl], row_tx.at[k, b], row_rx.at[k, b],
                      peers[0] + (peers[1] - peers[0]) * k)

    def sib_copy():
        return remote(part.at[2], recv.at[2], sib_tx, sib_rx, peers[2])

    def stat_copy(k, b):
        return remote(st_tx.at[b], st_rx.at[k, b], stat_tx.at[k, b], stat_rx.at[k, b], peers[k])

    half, lanes = rows // 2, 128

    def a_copy(q):
        sl = pl.ds(q * half, half)
        return pltpu.make_async_copy(a_hbm.at[sl, :], a_v.at[sl, :], a_sem.at[q])

    def w0_copy(q, first, n):
        src = w_hbm.at[:, pl.ds(pl.multiple_of(cross_col(0) + first, lanes), n)]
        return pltpu.make_async_copy(src, w_v.at[0, :, pl.ds(first, n)], w0_sem.at[q])

    def w_start(i):
        if isinstance(i, int):
            w_copy(i, cross_col(i) if i < 2 * per else near_col(i - 2 * per)).start()
            return

        @pl.when(i < 2 * per)
        def _():
            w_copy(i, cross_col(i)).start()

        @pl.when((i >= 2 * per) & (i < 4 * per))
        def _():
            w_copy(i, near_col(i - 2 * per)).start()

    r_copy = pltpu.make_async_copy(r_hbm, r_v, r_sem)
    g_copy = pltpu.make_async_copy(g_hbm, g_v, g_sem)
    a_copy(0).start()
    w0_copy(0, 0, lanes).start()
    a_copy(1).start()
    w0_copy(1, lanes, CW - lanes).start()
    barrier = pltpu.get_barrier_semaphore()
    for p in peers:
        pl.semaphore_signal(barrier, inc=1, device_id={"tp": p}, device_id_type=MESH)

    def dot(lhs, rhs):
        return jnp.dot(lhs, rhs, preferred_element_type=F32)

    pieces = ((pl.ds(0, half), pl.ds(0, lanes)), (pl.ds(half, half), pl.ds(0, lanes)),
              (pl.ds(0, rows), pl.ds(lanes, CW - lanes)))

    def piece_copy(q):
        sl = (0, *pieces[q])
        return remote(part.at[sl], recv.at[sl], first_tx.at[q], first_rx.at[q], peers[0])

    for q, (r_sl, c_sl) in enumerate(pieces):
        if q == 0:
            a_copy(0).wait()
            w0_copy(0, 0, lanes).wait()
            for i in range(1, DEPTH):
                w_start(i)
        elif q == 1:
            a_copy(1).wait()
        else:
            w0_copy(1, lanes, CW - lanes).wait()
            w_start(DEPTH)
        part[0, r_sl, c_sl] = dot(a_v[r_sl, :], w_v[0, :, c_sl]).astype(BF16)
        if q == 0:
            pl.semaphore_wait(barrier, 3)
        piece_copy(q).start()

    def chunk(i, col):
        w_copy(i, col).wait()
        w_start(i + DEPTH)
        return dot(a_v[...], w_v[i])

    def cross(i):
        part[i % 2, :, pl.ds(pl.multiple_of((i // 2) * CW, CW), CW)] = chunk(i, cross_col(i)).astype(BF16)

    for i in range(1, 2 * N_COL):
        cross(i)
        col_copy(i % 2, i // 2).start()

    @pl.loop(2 * N_COL, 2 * per)
    def _(i):
        cross(i)

    def send_block(b):
        row_copy(t % 2, b).start()
        row_copy(1 - t % 2, b).start()

    for b in range(AHEAD):
        send_block(b)
    r_copy.start()
    g_copy.start()

    @pl.loop(0, per)
    def _(j):
        part[2, :, pl.ds(pl.multiple_of(j * CW, CW), CW)] = chunk(2 * per + j, near_col(j)).astype(BF16)

    sib_copy().start()

    @pl.loop(0, per)
    def _(j):
        own[:, pl.ds(pl.multiple_of(j * CW, CW), CW)] = chunk(3 * per + j, near_col(per + j))

    r_copy.wait()
    g_copy.wait()
    sib_copy().wait_recv()
    for q in range(len(pieces)):
        piece_copy(q).wait_recv()
    for i in range(1, 2 * N_COL):
        col_copy(i % 2, i // 2).wait_recv()

    lane = lax.broadcasted_iota(jnp.int32, (8, 128), 1)
    sub = lax.broadcasted_iota(jnp.int32, (8, 128), 0)

    def reduce_block(b):
        row_copy(0, b).wait_recv()
        row_copy(1, b).wait_recv()
        row, n = blocks[b]
        line = jnp.zeros((8, 128), F32)
        for first in range(0, n, SUB):
            sl = pl.ds(row + first, SUB)
            h = own[sl, :] + recv[0, sl, :].astype(F32) + recv[1, sl, :].astype(F32) + recv[2, sl, :].astype(F32)
            h = r_v[sl, :].astype(F32) + h
            own[sl, :] = h
            hid[sl, :] = h.astype(BF16)
            s = jnp.sum(h * h, axis=1, keepdims=True)
            for q in range(0, SUB, 8):
                line = line + jnp.where(lane == sub + (first + q), s[q:q + 8, :], 0.0)
        st_tx[b] = jnp.sum(line, axis=0, keepdims=True)
        for k in range(3):
            stat_copy(k, b).start()

    def norm_block(b):
        for k in range(3):
            stat_copy(k, b).wait_recv()
        row, n = blocks[b]
        tot = (st_tx[b] + st_rx[2, b]) + (st_rx[0, b] + st_rx[1, b])
        scale = jnp.broadcast_to(lax.rsqrt(tot / d_model + EPS), (8, 128))
        for first in range(0, n, SUB):
            for q in range(first, first + SUB, 8):
                sl = pl.ds(row + q, 8)
                col = jnp.sum(jnp.where(lane == sub + q, scale, 0.0), axis=1, keepdims=True)
                own[sl, :] = own[sl, :] * col * g_v[...]
            sl = pl.ds(row + first, SUB)
            nrm[sl, :] = own[sl, :].astype(BF16)

    for b in range(n_blk):
        if b + AHEAD < n_blk:
            row_copy(0, b).wait_send()
            row_copy(1, b).wait_send()
            send_block(b + AHEAD)
        reduce_block(b)

    for b in range(n_blk):
        norm_block(b)

    for q in range(len(pieces)):
        piece_copy(q).wait_send()
    for i in range(1, 2 * N_COL):
        col_copy(i % 2, i // 2).wait_send()
    sib_copy().wait_send()

    for b in range(n_blk - AHEAD, n_blk):
        row_copy(0, b).wait_send()
        row_copy(1, b).wait_send()

    @pl.loop(0, n_blk)
    def _(b):
        for k in range(3):
            stat_copy(k, b).wait_send()


def put(hid, nrm, hid_hbm, nrm_hbm, sem):
    n = hid.shape[0] // PUT
    copies = []
    for q in range(PUT):
        sl = pl.ds(q * n, n)
        copies.append(pltpu.make_async_copy(hid.at[sl, :], hid_hbm.at[sl, :], sem.at[0, q]))
        copies.append(pltpu.make_async_copy(nrm.at[sl, :], nrm_hbm.at[sl, :], sem.at[1, q]))
    for c in copies:
        c.start()
    for c in copies:
        c.wait()


def solution(mesh):
    tp = mesh.shape["tp"]

    def local_step(a, w, r, g):
        rows, depth = a.shape
        d_loc = r.shape[1]
        per = d_loc // CW
        n_blk = len(BLOCKS)
        hbm = pl.BlockSpec(memory_space=pltpu.HBM)
        vmem = pl.BlockSpec(memory_space=pltpu.VMEM)
        dma = pltpu.SemaphoreType.DMA
        hid, nrm = pl.pallas_call(
            functools.partial(kernel, d_loc * tp),
            out_shape=(pltpu.VMEM((rows, d_loc), BF16),) * 2,
            in_specs=[hbm] * 4,
            out_specs=(vmem,) * 2,
            scratch_shapes=[
                pltpu.VMEM((rows, depth), BF16),
                pltpu.VMEM((4 * per, depth, CW), BF16),
                pltpu.VMEM((rows, d_loc), BF16),
                pltpu.VMEM((1, d_loc), F32),
                pltpu.VMEM((3, rows, d_loc), BF16),
                pltpu.VMEM((3, rows, d_loc), BF16),
                pltpu.VMEM((rows, d_loc), F32),
                pltpu.VMEM((n_blk, 1, 128), F32),
                pltpu.VMEM((3, n_blk, 1, 128), F32),
                dma((2,)), dma((2,)), dma((4 * per,)), dma, dma, dma((3,)), dma((3,)),
                dma((2, N_COL)), dma((2, N_COL)), dma((2, n_blk)), dma((2, n_blk)), dma, dma,
                dma((3, n_blk)), dma((3, n_blk)),
            ],
            compiler_params=pltpu.CompilerParams(
                collective_id=0, has_side_effects=True, vmem_limit_bytes=64946176),
            cost_estimate=pl.CostEstimate(flops=2 * rows * depth * d_loc * tp, transcendentals=0,
                                          bytes_accessed=2 * depth * d_loc * tp),
        )(a, w, r, g.reshape(1, d_loc))
        return pl.pallas_call(
            put,
            out_shape=(jax.ShapeDtypeStruct((rows, d_loc), BF16),) * 2,
            in_specs=[vmem] * 2,
            out_specs=(hbm,) * 2,
            scratch_shapes=[dma((2, PUT))],
            compiler_params=pltpu.CompilerParams(vmem_limit_bytes=1024 * 1024),
        )(hid, nrm)

    return jax.shard_map(
        local_step,
        mesh=mesh,
        in_specs=(P("data", "tp"), P("tp", None), P("data", "tp"), P("tp")),
        out_specs=(P("data", "tp"), P("data", "tp")),
        check_vma=False,
    )
```

```python
import functools

import jax
import jax.numpy as jnp
from jax import lax
from jax.experimental import pallas as pl
from jax.experimental.pallas import tpu as pltpu
from jax.sharding import PartitionSpec as P

EPS = 1e-5
MESH = pl.DeviceIdType.MESH
F32, BF16 = jnp.float32, jnp.bfloat16

CW = 256
N_COL = 2
BLOCKS = (128, 112, 16)
SUB = 16
DEPTH = 4
PUT = 1
AHEAD = 3


def kernel(d_model, a_hbm, w_hbm, r_hbm, g_hbm, hid, nrm,
           a_v, w_v, r_v, g_v, part, recv, own, st_tx, st_rx,
           a_sem, w0_sem, w_sem, r_sem, g_sem, first_tx, first_rx, col_tx, col_rx, row_tx, row_rx, sib_tx, sib_rx, stat_tx, stat_rx):
    t = lax.axis_index("tp")
    rows, _ = a_v.shape
    d_loc = own.shape[1]
    per = d_loc // CW
    peers = ((t + 2) % 4, 3 - t, t + 1 - 2 * (t % 2))
    n_blk = len(BLOCKS)
    blocks = [(sum(BLOCKS[:b]), BLOCKS[b]) for b in range(n_blk)]
    c0 = N_COL * CW

    def w_copy(slot, col):
        return pltpu.make_async_copy(w_hbm.at[:, pl.ds(pl.multiple_of(col, CW), CW)], w_v.at[slot], w_sem.at[slot])

    def cross_col(i):
        k = i % 2
        return (peers[0] + (peers[1] - peers[0]) * k) * d_loc + (i // 2) * CW

    def near_col(i):
        return (peers[2] + (t - peers[2]) * (i // per)) * d_loc + (i % per) * CW

    def remote(src, dst, tx, rx, peer):
        return pltpu.make_async_remote_copy(src_ref=src, dst_ref=dst, send_sem=tx, recv_sem=rx,
                                            device_id={"tp": peer}, device_id_type=MESH)

    def col_copy(k, j):
        cols = pl.ds(j * CW, CW)
        return remote(part.at[k, :, cols], recv.at[k, :, cols], col_tx.at[k, j], col_rx.at[k, j], peers[k])

    def row_copy(k, b):
        sl = (k, pl.ds(*blocks[b]), pl.ds(c0, d_loc - c0))
        return remote(part.at[sl], recv.at[sl], row_tx.at[k, b], row_rx.at[k, b],
                      peers[0] + (peers[1] - peers[0]) * k)

    def sib_copy():
        return remote(part.at[2], recv.at[2], sib_tx, sib_rx, peers[2])

    def stat_copy(k, b):
        return remote(st_tx.at[b], st_rx.at[k, b], stat_tx.at[k, b], stat_rx.at[k, b], peers[k])

    half, lanes = rows // 2, 128

    def a_copy(q):
        sl = pl.ds(q * half, half)
        return pltpu.make_async_copy(a_hbm.at[sl, :], a_v.at[sl, :], a_sem.at[q])

    def w0_copy(q, first, n):
        src = w_hbm.at[:, pl.ds(pl.multiple_of(cross_col(0) + first, lanes), n)]
        return pltpu.make_async_copy(src, w_v.at[0, :, pl.ds(first, n)], w0_sem.at[q])

    def w_start(i):
        if isinstance(i, int):
            w_copy(i, cross_col(i) if i < 2 * per else near_col(i - 2 * per)).start()
            return

        @pl.when(i < 2 * per)
        def _():
            w_copy(i, cross_col(i)).start()

        @pl.when((i >= 2 * per) & (i < 4 * per))
        def _():
            w_copy(i, near_col(i - 2 * per)).start()

    r_copy = pltpu.make_async_copy(r_hbm, r_v, r_sem)
    g_copy = pltpu.make_async_copy(g_hbm, g_v, g_sem)
    a_copy(0).start()
    w0_copy(0, 0, lanes).start()
    a_copy(1).start()
    w0_copy(1, lanes, CW - lanes).start()
    barrier = pltpu.get_barrier_semaphore()
    for p in peers:
        pl.semaphore_signal(barrier, inc=1, device_id={"tp": p}, device_id_type=MESH)

    def dot(lhs, rhs):
        return jnp.dot(lhs, rhs, preferred_element_type=F32)

    pieces = ((pl.ds(0, half), pl.ds(0, lanes)), (pl.ds(half, half), pl.ds(0, lanes)),
              (pl.ds(0, rows), pl.ds(lanes, CW - lanes)))

    def piece_copy(q):
        sl = (0, *pieces[q])
        return remote(part.at[sl], recv.at[sl], first_tx.at[q], first_rx.at[q], peers[0])

    for q, (r_sl, c_sl) in enumerate(pieces):
        if q == 0:
            a_copy(0).wait()
            w0_copy(0, 0, lanes).wait()
            for i in range(1, DEPTH):
                w_start(i)
        elif q == 1:
            a_copy(1).wait()
        else:
            w0_copy(1, lanes, CW - lanes).wait()
            w_start(DEPTH)
        part[0, r_sl, c_sl] = dot(a_v[r_sl, :], w_v[0, :, c_sl]).astype(BF16)
        if q == 0:
            pl.semaphore_wait(barrier, 3)
        piece_copy(q).start()

    def chunk(i, col):
        w_copy(i, col).wait()
        w_start(i + DEPTH)
        return dot(a_v[...], w_v[i])

    def cross(i):
        part[i % 2, :, pl.ds(pl.multiple_of((i // 2) * CW, CW), CW)] = chunk(i, cross_col(i)).astype(BF16)

    for i in range(1, 2 * N_COL):
        cross(i)
        col_copy(i % 2, i // 2).start()

    @pl.loop(2 * N_COL, 2 * per)
    def _(i):
        cross(i)

    def send_block(b):
        row_copy(t % 2, b).start()
        row_copy(1 - t % 2, b).start()

    for b in range(AHEAD):
        send_block(b)
    r_copy.start()
    g_copy.start()

    @pl.loop(0, per)
    def _(j):
        part[2, :, pl.ds(pl.multiple_of(j * CW, CW), CW)] = chunk(2 * per + j, near_col(j)).astype(BF16)

    sib_copy().start()

    @pl.loop(0, per)
    def _(j):
        own[:, pl.ds(pl.multiple_of(j * CW, CW), CW)] = chunk(3 * per + j, near_col(per + j))

    r_copy.wait()
    g_copy.wait()
    sib_copy().wait_recv()
    for q in range(len(pieces)):
        piece_copy(q).wait_recv()
    for i in range(1, 2 * N_COL):
        col_copy(i % 2, i // 2).wait_recv()

    lane = lax.broadcasted_iota(jnp.int32, (8, 128), 1)
    sub = lax.broadcasted_iota(jnp.int32, (8, 128), 0)

    def reduce_block(b):
        row_copy(0, b).wait_recv()
        row_copy(1, b).wait_recv()
        row, n = blocks[b]
        line = jnp.zeros((8, 128), F32)
        for first in range(0, n, SUB):
            sl = pl.ds(row + first, SUB)
            h = own[sl, :] + recv[0, sl, :].astype(F32) + recv[1, sl, :].astype(F32) + recv[2, sl, :].astype(F32)
            h = r_v[sl, :].astype(F32) + h
            own[sl, :] = h
            hid[sl, :] = h.astype(BF16)
            s = jnp.sum(h * h, axis=1, keepdims=True)
            for q in range(0, SUB, 8):
                line = line + jnp.where(lane == sub + (first + q), s[q:q + 8, :], 0.0)
        st_tx[b] = jnp.sum(line, axis=0, keepdims=True)
        for k in range(3):
            stat_copy(k, b).start()

    def norm_block(b):
        for k in range(3):
            stat_copy(k, b).wait_recv()
        row, n = blocks[b]
        tot = (st_tx[b] + st_rx[2, b]) + (st_rx[0, b] + st_rx[1, b])
        scale = jnp.broadcast_to(lax.rsqrt(tot / d_model + EPS), (8, 128))
        for first in range(0, n, SUB):
            for q in range(first, first + SUB, 8):
                sl = pl.ds(row + q, 8)
                col = jnp.sum(jnp.where(lane == sub + q, scale, 0.0), axis=1, keepdims=True)
                own[sl, :] = own[sl, :] * col * g_v[...]
            sl = pl.ds(row + first, SUB)
            nrm[sl, :] = own[sl, :].astype(BF16)

    for b in range(n_blk):
        if b + AHEAD < n_blk:
            row_copy(0, b).wait_send()
            row_copy(1, b).wait_send()
            send_block(b + AHEAD)
        reduce_block(b)

    for b in range(n_blk):
        norm_block(b)

    for q in range(len(pieces)):
        piece_copy(q).wait_send()
    for i in range(1, 2 * N_COL):
        col_copy(i % 2, i // 2).wait_send()
    sib_copy().wait_send()

    for b in range(n_blk - AHEAD, n_blk):
        row_copy(0, b).wait_send()
        row_copy(1, b).wait_send()

    @pl.loop(0, n_blk)
    def _(b):
        for k in range(3):
            stat_copy(k, b).wait_send()


def put(hid, nrm, hid_hbm, nrm_hbm, sem):
    n = hid.shape[0] // PUT
    copies = []
    for q in range(PUT):
        sl = pl.ds(q * n, n)
        copies.append(pltpu.make_async_copy(hid.at[sl, :], hid_hbm.at[sl, :], sem.at[0, q]))
        copies.append(pltpu.make_async_copy(nrm.at[sl, :], nrm_hbm.at[sl, :], sem.at[1, q]))
    for c in copies:
        c.start()
    for c in copies:
        c.wait()


def solution(mesh):
    tp = mesh.shape["tp"]

    def local_step(a, w, r, g):
        rows, depth = a.shape
        d_loc = r.shape[1]
        per = d_loc // CW
        n_blk = len(BLOCKS)
        hbm = pl.BlockSpec(memory_space=pltpu.HBM)
        vmem = pl.BlockSpec(memory_space=pltpu.VMEM)
        dma = pltpu.SemaphoreType.DMA
        hid, nrm = pl.pallas_call(
            functools.partial(kernel, d_loc * tp),
            out_shape=(pltpu.VMEM((rows, d_loc), BF16),) * 2,
            in_specs=[hbm] * 4,
            out_specs=(vmem,) * 2,
            scratch_shapes=[
                pltpu.VMEM((rows, depth), BF16),
                pltpu.VMEM((4 * per, depth, CW), BF16),
                pltpu.VMEM((rows, d_loc), BF16),
                pltpu.VMEM((1, d_loc), F32),
                pltpu.VMEM((3, rows, d_loc), BF16),
                pltpu.VMEM((3, rows, d_loc), BF16),
                pltpu.VMEM((rows, d_loc), F32),
                pltpu.VMEM((n_blk, 1, 128), F32),
                pltpu.VMEM((3, n_blk, 1, 128), F32),
                dma((2,)), dma((2,)), dma((4 * per,)), dma, dma, dma((3,)), dma((3,)),
                dma((2, N_COL)), dma((2, N_COL)), dma((2, n_blk)), dma((2, n_blk)), dma, dma,
                dma((3, n_blk)), dma((3, n_blk)),
            ],
            compiler_params=pltpu.CompilerParams(
                collective_id=0, has_side_effects=True, vmem_limit_bytes=64946176),
            cost_estimate=pl.CostEstimate(flops=2 * rows * depth * d_loc * tp, transcendentals=0,
                                          bytes_accessed=2 * depth * d_loc * tp),
        )(a, w, r, g.reshape(1, d_loc))
        return pl.pallas_call(
            put,
            out_shape=(jax.ShapeDtypeStruct((rows, d_loc), BF16),) * 2,
            in_specs=[vmem] * 2,
            out_specs=(hbm,) * 2,
            scratch_shapes=[dma((2, PUT))],
            compiler_params=pltpu.CompilerParams(vmem_limit_bytes=1024 * 1024),
        )(hid, nrm)

    return jax.shard_map(
        local_step,
        mesh=mesh,
        in_specs=(P("data", "tp"), P("tp", None), P("data", "tp"), P("tp")),
        out_specs=(P("data", "tp"), P("data", "tp")),
        check_vma=False,
    )
```

```python
import functools

import jax
import jax.numpy as jnp
from jax import lax
from jax.experimental import pallas as pl
from jax.experimental.pallas import tpu as pltpu
from jax.sharding import PartitionSpec as P

EPS = 1e-5
MESH = pl.DeviceIdType.MESH
F32, BF16 = jnp.float32, jnp.bfloat16

CW = 256
N_COL = 2
BLOCKS = (128, 112, 16)
SUB = 16
DEPTH = 4
PUT = 1


def kernel(d_model, a_hbm, w_hbm, r_hbm, g_hbm, hid, nrm,
           a_v, w_v, r_v, g_v, part, recv, own, st_tx, st_rx,
           a_sem, w0_sem, w_sem, r_sem, g_sem, first_tx, first_rx, col_tx, col_rx, row_tx, row_rx, sib_tx, sib_rx, stat_tx, stat_rx):
    t = lax.axis_index("tp")
    rows, _ = a_v.shape
    d_loc = own.shape[1]
    per = d_loc // CW
    peers = ((t + 2) % 4, 3 - t, t + 1 - 2 * (t % 2))
    n_blk = len(BLOCKS)
    blocks = [(sum(BLOCKS[:b]), BLOCKS[b]) for b in range(n_blk)]
    c0 = N_COL * CW

    def w_copy(slot, col):
        return pltpu.make_async_copy(w_hbm.at[:, pl.ds(pl.multiple_of(col, CW), CW)], w_v.at[slot], w_sem.at[slot])

    def cross_col(i):
        k = i % 2
        return (peers[0] + (peers[1] - peers[0]) * k) * d_loc + (i // 2) * CW

    def near_col(i):
        return (peers[2] + (t - peers[2]) * (i // per)) * d_loc + (i % per) * CW

    def remote(src, dst, tx, rx, peer):
        return pltpu.make_async_remote_copy(src_ref=src, dst_ref=dst, send_sem=tx, recv_sem=rx,
                                            device_id={"tp": peer}, device_id_type=MESH)

    def col_copy(k, j):
        cols = pl.ds(j * CW, CW)
        return remote(part.at[k, :, cols], recv.at[k, :, cols], col_tx.at[k, j], col_rx.at[k, j], peers[k])

    def row_copy(k, b):
        sl = (k, pl.ds(*blocks[b]), pl.ds(c0, d_loc - c0))
        return remote(part.at[sl], recv.at[sl], row_tx.at[k, b], row_rx.at[k, b],
                      peers[0] + (peers[1] - peers[0]) * k)

    def sib_copy():
        return remote(part.at[2], recv.at[2], sib_tx, sib_rx, peers[2])

    def stat_copy(k, b):
        return remote(st_tx.at[b], st_rx.at[k, b], stat_tx.at[k, b], stat_rx.at[k, b], peers[k])

    half, lanes = rows // 2, 128

    def a_copy(q):
        sl = pl.ds(q * half, half)
        return pltpu.make_async_copy(a_hbm.at[sl, :], a_v.at[sl, :], a_sem.at[q])

    def w0_copy(q, first, n):
        src = w_hbm.at[:, pl.ds(pl.multiple_of(cross_col(0) + first, lanes), n)]
        return pltpu.make_async_copy(src, w_v.at[0, :, pl.ds(first, n)], w0_sem.at[q])

    def w_start(i):
        if isinstance(i, int):
            w_copy(i, cross_col(i) if i < 2 * per else near_col(i - 2 * per)).start()
            return

        @pl.when(i < 2 * per)
        def _():
            w_copy(i, cross_col(i)).start()

        @pl.when((i >= 2 * per) & (i < 4 * per))
        def _():
            w_copy(i, near_col(i - 2 * per)).start()

    r_copy = pltpu.make_async_copy(r_hbm, r_v, r_sem)
    g_copy = pltpu.make_async_copy(g_hbm, g_v, g_sem)
    a_copy(0).start()
    w0_copy(0, 0, lanes).start()
    a_copy(1).start()
    w0_copy(1, lanes, CW - lanes).start()
    barrier = pltpu.get_barrier_semaphore()
    for p in peers:
        pl.semaphore_signal(barrier, inc=1, device_id={"tp": p}, device_id_type=MESH)

    def dot(lhs, rhs):
        return jnp.dot(lhs, rhs, preferred_element_type=F32)

    pieces = ((pl.ds(0, half), pl.ds(0, lanes)), (pl.ds(half, half), pl.ds(0, lanes)),
              (pl.ds(0, rows), pl.ds(lanes, CW - lanes)))

    def piece_copy(q):
        sl = (0, *pieces[q])
        return remote(part.at[sl], recv.at[sl], first_tx.at[q], first_rx.at[q], peers[0])

    for q, (r_sl, c_sl) in enumerate(pieces):
        if q == 0:
            a_copy(0).wait()
            w0_copy(0, 0, lanes).wait()
            for i in range(1, DEPTH):
                w_start(i)
        elif q == 1:
            a_copy(1).wait()
        else:
            w0_copy(1, lanes, CW - lanes).wait()
            w_start(DEPTH)
        part[0, r_sl, c_sl] = dot(a_v[r_sl, :], w_v[0, :, c_sl]).astype(BF16)
        if q == 0:
            pl.semaphore_wait(barrier, 3)
        if q == 1:
            @pl.when(t % 2 == 0)
            def _():
                piece_copy(1).start()
            continue
        if q == 2:
            @pl.when(t % 2 == 1)
            def _():
                piece_copy(1).start()
        piece_copy(q).start()

    def chunk(i, col):
        w_copy(i, col).wait()
        w_start(i + DEPTH)
        return dot(a_v[...], w_v[i])

    def cross(i):
        part[i % 2, :, pl.ds(pl.multiple_of((i // 2) * CW, CW), CW)] = chunk(i, cross_col(i)).astype(BF16)

    for i in range(1, 2 * N_COL):
        cross(i)
        col_copy(i % 2, i // 2).start()

    @pl.loop(2 * N_COL, 2 * per)
    def _(i):
        cross(i)

    far, near = t % 2, 1 - t % 2
    order = ([(k, b) for b in range(n_blk - 2) for k in (far, near)]
             + [(k, b) for k in (far, near) for b in (n_blk - 2, n_blk - 1)])
    for k, b in order:
        row_copy(k, b).start()
    r_copy.start()
    g_copy.start()

    @pl.loop(0, per)
    def _(j):
        part[2, :, pl.ds(pl.multiple_of(j * CW, CW), CW)] = chunk(2 * per + j, near_col(j)).astype(BF16)

    sib_copy().start()

    @pl.loop(0, per)
    def _(j):
        own[:, pl.ds(pl.multiple_of(j * CW, CW), CW)] = chunk(3 * per + j, near_col(per + j))

    r_copy.wait()
    g_copy.wait()
    sib_copy().wait_recv()
    for q in range(len(pieces)):
        piece_copy(q).wait_recv()
    for i in range(1, 2 * N_COL):
        col_copy(i % 2, i // 2).wait_recv()

    lane = lax.broadcasted_iota(jnp.int32, (8, 128), 1)
    sub = lax.broadcasted_iota(jnp.int32, (8, 128), 0)

    def reduce_block(b):
        row_copy(0, b).wait_recv()
        row_copy(1, b).wait_recv()
        row, n = blocks[b]
        line = jnp.zeros((8, 128), F32)
        for first in range(0, n, SUB):
            sl = pl.ds(row + first, SUB)
            h = own[sl, :] + recv[0, sl, :].astype(F32) + recv[1, sl, :].astype(F32) + recv[2, sl, :].astype(F32)
            h = r_v[sl, :].astype(F32) + h
            own[sl, :] = h
            hid[sl, :] = h.astype(BF16)
            s = jnp.sum(h * h, axis=1, keepdims=True)
            for q in range(0, SUB, 8):
                line = line + jnp.where(lane == sub + (first + q), s[q:q + 8, :], 0.0)
        st_tx[b] = jnp.sum(line, axis=0, keepdims=True)
        for k in range(3):
            stat_copy(k, b).start()

    def norm_block(b):
        for k in range(3):
            stat_copy(k, b).wait_recv()
        row, n = blocks[b]
        tot = (st_tx[b] + st_rx[2, b]) + (st_rx[0, b] + st_rx[1, b])
        scale = jnp.broadcast_to(lax.rsqrt(tot / d_model + EPS), (8, 128))
        for first in range(0, n, SUB):
            for q in range(first, first + SUB, 8):
                sl = pl.ds(row + q, 8)
                col = jnp.sum(jnp.where(lane == sub + q, scale, 0.0), axis=1, keepdims=True)
                own[sl, :] = own[sl, :] * col * g_v[...]
            sl = pl.ds(row + first, SUB)
            nrm[sl, :] = own[sl, :].astype(BF16)

    for b in range(n_blk):
        reduce_block(b)

    for b in range(n_blk):
        norm_block(b)

    for q in range(len(pieces)):
        piece_copy(q).wait_send()
    for i in range(1, 2 * N_COL):
        col_copy(i % 2, i // 2).wait_send()
    sib_copy().wait_send()

    for b in range(n_blk):
        row_copy(0, b).wait_send()
        row_copy(1, b).wait_send()

    @pl.loop(0, n_blk)
    def _(b):
        for k in range(3):
            stat_copy(k, b).wait_send()


def put(hid, nrm, hid_hbm, nrm_hbm, sem):
    n = hid.shape[0] // PUT
    copies = []
    for q in range(PUT):
        sl = pl.ds(q * n, n)
        copies.append(pltpu.make_async_copy(hid.at[sl, :], hid_hbm.at[sl, :], sem.at[0, q]))
        copies.append(pltpu.make_async_copy(nrm.at[sl, :], nrm_hbm.at[sl, :], sem.at[1, q]))
    for c in copies:
        c.start()
    for c in copies:
        c.wait()


def solution(mesh):
    tp = mesh.shape["tp"]

    def local_step(a, w, r, g):
        rows, depth = a.shape
        d_loc = r.shape[1]
        per = d_loc // CW
        n_blk = len(BLOCKS)
        hbm = pl.BlockSpec(memory_space=pltpu.HBM)
        vmem = pl.BlockSpec(memory_space=pltpu.VMEM)
        dma = pltpu.SemaphoreType.DMA
        hid, nrm = pl.pallas_call(
            functools.partial(kernel, d_loc * tp),
            out_shape=(pltpu.VMEM((rows, d_loc), BF16),) * 2,
            in_specs=[hbm] * 4,
            out_specs=(vmem,) * 2,
            scratch_shapes=[
                pltpu.VMEM((rows, depth), BF16),
                pltpu.VMEM((4 * per, depth, CW), BF16),
                pltpu.VMEM((rows, d_loc), BF16),
                pltpu.VMEM((1, d_loc), F32),
                pltpu.VMEM((3, rows, d_loc), BF16),
                pltpu.VMEM((3, rows, d_loc), BF16),
                pltpu.VMEM((rows, d_loc), F32),
                pltpu.VMEM((n_blk, 1, 128), F32),
                pltpu.VMEM((3, n_blk, 1, 128), F32),
                dma((2,)), dma((2,)), dma((4 * per,)), dma, dma, dma((3,)), dma((3,)),
                dma((2, N_COL)), dma((2, N_COL)), dma((2, n_blk)), dma((2, n_blk)), dma, dma,
                dma((3, n_blk)), dma((3, n_blk)),
            ],
            compiler_params=pltpu.CompilerParams(
                collective_id=0, has_side_effects=True, vmem_limit_bytes=64946176),
            cost_estimate=pl.CostEstimate(flops=2 * rows * depth * d_loc * tp, transcendentals=0,
                                          bytes_accessed=2 * depth * d_loc * tp),
        )(a, w, r, g.reshape(1, d_loc))
        return pl.pallas_call(
            put,
            out_shape=(jax.ShapeDtypeStruct((rows, d_loc), BF16),) * 2,
            in_specs=[vmem] * 2,
            out_specs=(hbm,) * 2,
            scratch_shapes=[dma((2, PUT))],
            compiler_params=pltpu.CompilerParams(vmem_limit_bytes=1024 * 1024),
        )(hid, nrm)

    return jax.shard_map(
        local_step,
        mesh=mesh,
        in_specs=(P("data", "tp"), P("tp", None), P("data", "tp"), P("tp")),
        out_specs=(P("data", "tp"), P("data", "tp")),
        check_vma=False,
    )
```

```python
import functools

import jax
import jax.numpy as jnp
from jax import lax
from jax.experimental import pallas as pl
from jax.experimental.pallas import tpu as pltpu
from jax.sharding import PartitionSpec as P

EPS = 1e-5
MESH = pl.DeviceIdType.MESH
F32, BF16 = jnp.float32, jnp.bfloat16

CW = 256
N_COL = 2
BLOCKS = (128, 112, 16)
SUB = 16
DEPTH = 4
PUT = 1


def kernel(d_model, a_hbm, w_hbm, r_hbm, g_hbm, hid, nrm,
           a_v, w_v, r_v, g_v, part, recv, own, st_tx, st_rx,
           a_sem, w0_sem, w_sem, r_sem, g_sem, first_tx, first_rx, col_tx, col_rx, row_tx, row_rx, sib_tx, sib_rx, stat_tx, stat_rx):
    t = lax.axis_index("tp")
    rows, _ = a_v.shape
    d_loc = own.shape[1]
    per = d_loc // CW
    peers = ((t + 2) % 4, 3 - t, t + 1 - 2 * (t % 2))
    n_blk = len(BLOCKS)
    blocks = [(sum(BLOCKS[:b]), BLOCKS[b]) for b in range(n_blk)]
    c0 = N_COL * CW

    def w_copy(slot, col):
        return pltpu.make_async_copy(w_hbm.at[:, pl.ds(pl.multiple_of(col, CW), CW)], w_v.at[slot], w_sem.at[slot])

    def cross_col(i):
        k = i % 2
        return (peers[0] + (peers[1] - peers[0]) * k) * d_loc + (i // 2) * CW

    def near_col(i):
        return (peers[2] + (t - peers[2]) * (i // per)) * d_loc + (i % per) * CW

    def remote(src, dst, tx, rx, peer):
        return pltpu.make_async_remote_copy(src_ref=src, dst_ref=dst, send_sem=tx, recv_sem=rx,
                                            device_id={"tp": peer}, device_id_type=MESH)

    def col_copy(k, j):
        cols = pl.ds(j * CW, CW)
        return remote(part.at[k, :, cols], recv.at[k, :, cols], col_tx.at[k, j], col_rx.at[k, j], peers[k])

    def row_copy(k, b):
        sl = (k, pl.ds(*blocks[b]), pl.ds(c0, d_loc - c0))
        return remote(part.at[sl], recv.at[sl], row_tx.at[k, b], row_rx.at[k, b],
                      peers[0] + (peers[1] - peers[0]) * k)

    def sib_copy():
        return remote(part.at[2], recv.at[2], sib_tx, sib_rx, peers[2])

    def stat_copy(k, b):
        return remote(st_tx.at[b], st_rx.at[k, b], stat_tx.at[k, b], stat_rx.at[k, b], peers[k])

    half, lanes = rows // 2, 128

    def a_copy(q):
        sl = pl.ds(q * half, half)
        return pltpu.make_async_copy(a_hbm.at[sl, :], a_v.at[sl, :], a_sem.at[q])

    def w0_copy(q, first, n):
        src = w_hbm.at[:, pl.ds(pl.multiple_of(cross_col(0) + first, lanes), n)]
        return pltpu.make_async_copy(src, w_v.at[0, :, pl.ds(first, n)], w0_sem.at[q])

    def w_start(i):
        if isinstance(i, int):
            w_copy(i, cross_col(i) if i < 2 * per else near_col(i - 2 * per)).start()
            return

        @pl.when(i < 2 * per)
        def _():
            w_copy(i, cross_col(i)).start()

        @pl.when((i >= 2 * per) & (i < 4 * per))
        def _():
            w_copy(i, near_col(i - 2 * per)).start()

    r_copy = pltpu.make_async_copy(r_hbm, r_v, r_sem)
    g_copy = pltpu.make_async_copy(g_hbm, g_v, g_sem)
    a_copy(0).start()
    w0_copy(0, 0, lanes).start()
    a_copy(1).start()
    w0_copy(1, lanes, CW - lanes).start()
    barrier = pltpu.get_barrier_semaphore()
    for p in peers:
        pl.semaphore_signal(barrier, inc=1, device_id={"tp": p}, device_id_type=MESH)

    def dot(lhs, rhs):
        return jnp.dot(lhs, rhs, preferred_element_type=F32)

    pieces = ((pl.ds(0, half), pl.ds(0, lanes)), (pl.ds(half, half), pl.ds(0, lanes)),
              (pl.ds(0, rows), pl.ds(lanes, CW - lanes)))

    def piece_copy(q):
        sl = (0, *pieces[q])
        return remote(part.at[sl], recv.at[sl], first_tx.at[q], first_rx.at[q], peers[0])

    for q, (r_sl, c_sl) in enumerate(pieces):
        if q == 0:
            a_copy(0).wait()
            w0_copy(0, 0, lanes).wait()
            for i in range(1, DEPTH):
                w_start(i)
        elif q == 1:
            a_copy(1).wait()
        else:
            w0_copy(1, lanes, CW - lanes).wait()
            w_start(DEPTH)
        part[0, r_sl, c_sl] = dot(a_v[r_sl, :], w_v[0, :, c_sl]).astype(BF16)
        if q == 0:
            pl.semaphore_wait(barrier, 3)
        piece_copy(q).start()

    def chunk(i, col):
        w_copy(i, col).wait()
        w_start(i + DEPTH)
        return dot(a_v[...], w_v[i])

    def cross(i):
        part[i % 2, :, pl.ds(pl.multiple_of((i // 2) * CW, CW), CW)] = chunk(i, cross_col(i)).astype(BF16)

    for i in range(1, 2 * N_COL):
        cross(i)
        col_copy(i % 2, i // 2).start()

    @pl.loop(2 * N_COL, 2 * per)
    def _(i):
        cross(i)

    far, near = t % 2, 1 - t % 2
    order = [(k, b) for b in range(n_blk) for k in (near, far)]
    for k, b in order:
        row_copy(k, b).start()
    r_copy.start()
    g_copy.start()

    @pl.loop(0, per)
    def _(j):
        part[2, :, pl.ds(pl.multiple_of(j * CW, CW), CW)] = chunk(2 * per + j, near_col(j)).astype(BF16)

    sib_copy().start()

    @pl.loop(0, per)
    def _(j):
        own[:, pl.ds(pl.multiple_of(j * CW, CW), CW)] = chunk(3 * per + j, near_col(per + j))

    r_copy.wait()
    g_copy.wait()
    sib_copy().wait_recv()
    for q in range(len(pieces)):
        piece_copy(q).wait_recv()
    for i in range(1, 2 * N_COL):
        col_copy(i % 2, i // 2).wait_recv()

    lane = lax.broadcasted_iota(jnp.int32, (8, 128), 1)
    sub = lax.broadcasted_iota(jnp.int32, (8, 128), 0)

    def reduce_block(b):
        row_copy(0, b).wait_recv()
        row_copy(1, b).wait_recv()
        row, n = blocks[b]
        line = jnp.zeros((8, 128), F32)
        for first in range(0, n, SUB):
            sl = pl.ds(row + first, SUB)
            h = own[sl, :] + recv[0, sl, :].astype(F32) + recv[1, sl, :].astype(F32) + recv[2, sl, :].astype(F32)
            h = r_v[sl, :].astype(F32) + h
            own[sl, :] = h
            hid[sl, :] = h.astype(BF16)
            s = jnp.sum(h * h, axis=1, keepdims=True)
            for q in range(0, SUB, 8):
                line = line + jnp.where(lane == sub + (first + q), s[q:q + 8, :], 0.0)
        st_tx[b] = jnp.sum(line, axis=0, keepdims=True)
        for k in range(3):
            stat_copy(k, b).start()

    def norm_block(b):
        for k in range(3):
            stat_copy(k, b).wait_recv()
        row, n = blocks[b]
        tot = (st_tx[b] + st_rx[2, b]) + (st_rx[0, b] + st_rx[1, b])
        scale = jnp.broadcast_to(lax.rsqrt(tot / d_model + EPS), (8, 128))
        for first in range(0, n, SUB):
            for q in range(first, first + SUB, 8):
                sl = pl.ds(row + q, 8)
                col = jnp.sum(jnp.where(lane == sub + q, scale, 0.0), axis=1, keepdims=True)
                own[sl, :] = own[sl, :] * col * g_v[...]
            sl = pl.ds(row + first, SUB)
            nrm[sl, :] = own[sl, :].astype(BF16)

    for b in range(n_blk):
        reduce_block(b)

    for b in range(n_blk):
        norm_block(b)

    for q in range(len(pieces)):
        piece_copy(q).wait_send()
    for i in range(1, 2 * N_COL):
        col_copy(i % 2, i // 2).wait_send()
    sib_copy().wait_send()

    for b in range(n_blk):
        row_copy(0, b).wait_send()
        row_copy(1, b).wait_send()

    @pl.loop(0, n_blk)
    def _(b):
        for k in range(3):
            stat_copy(k, b).wait_send()


def put(hid, nrm, hid_hbm, nrm_hbm, sem):
    n = hid.shape[0] // PUT
    copies = []
    for q in range(PUT):
        sl = pl.ds(q * n, n)
        copies.append(pltpu.make_async_copy(hid.at[sl, :], hid_hbm.at[sl, :], sem.at[0, q]))
        copies.append(pltpu.make_async_copy(nrm.at[sl, :], nrm_hbm.at[sl, :], sem.at[1, q]))
    for c in copies:
        c.start()
    for c in copies:
        c.wait()


def solution(mesh):
    tp = mesh.shape["tp"]

    def local_step(a, w, r, g):
        rows, depth = a.shape
        d_loc = r.shape[1]
        per = d_loc // CW
        n_blk = len(BLOCKS)
        hbm = pl.BlockSpec(memory_space=pltpu.HBM)
        vmem = pl.BlockSpec(memory_space=pltpu.VMEM)
        dma = pltpu.SemaphoreType.DMA
        hid, nrm = pl.pallas_call(
            functools.partial(kernel, d_loc * tp),
            out_shape=(pltpu.VMEM((rows, d_loc), BF16),) * 2,
            in_specs=[hbm] * 4,
            out_specs=(vmem,) * 2,
            scratch_shapes=[
                pltpu.VMEM((rows, depth), BF16),
                pltpu.VMEM((4 * per, depth, CW), BF16),
                pltpu.VMEM((rows, d_loc), BF16),
                pltpu.VMEM((1, d_loc), F32),
                pltpu.VMEM((3, rows, d_loc), BF16),
                pltpu.VMEM((3, rows, d_loc), BF16),
                pltpu.VMEM((rows, d_loc), F32),
                pltpu.VMEM((n_blk, 1, 128), F32),
                pltpu.VMEM((3, n_blk, 1, 128), F32),
                dma((2,)), dma((2,)), dma((4 * per,)), dma, dma, dma((3,)), dma((3,)),
                dma((2, N_COL)), dma((2, N_COL)), dma((2, n_blk)), dma((2, n_blk)), dma, dma,
                dma((3, n_blk)), dma((3, n_blk)),
            ],
            compiler_params=pltpu.CompilerParams(
                collective_id=0, has_side_effects=True, vmem_limit_bytes=64946176),
            cost_estimate=pl.CostEstimate(flops=2 * rows * depth * d_loc * tp, transcendentals=0,
                                          bytes_accessed=2 * depth * d_loc * tp),
        )(a, w, r, g.reshape(1, d_loc))
        return pl.pallas_call(
            put,
            out_shape=(jax.ShapeDtypeStruct((rows, d_loc), BF16),) * 2,
            in_specs=[vmem] * 2,
            out_specs=(hbm,) * 2,
            scratch_shapes=[dma((2, PUT))],
            compiler_params=pltpu.CompilerParams(vmem_limit_bytes=1024 * 1024),
        )(hid, nrm)

    return jax.shard_map(
        local_step,
        mesh=mesh,
        in_specs=(P("data", "tp"), P("tp", None), P("data", "tp"), P("tp")),
        out_specs=(P("data", "tp"), P("data", "tp")),
        check_vma=False,
    )
```

```python
import functools

import jax
import jax.numpy as jnp
from jax import lax
from jax.experimental import pallas as pl
from jax.experimental.pallas import tpu as pltpu
from jax.sharding import PartitionSpec as P

EPS = 1e-5
MESH = pl.DeviceIdType.MESH
F32, BF16 = jnp.float32, jnp.bfloat16

CW = 256
N_COL = 2
BLOCKS = (128, 112, 16)
SUB = 16
DEPTH = 4
PUT = 1


def kernel(d_model, a_hbm, w_hbm, r_hbm, g_hbm, hid, nrm,
           a_v, w_v, r_v, g_v, part, recv, own, st_tx, st_rx,
           a_sem, w0_sem, w_sem, r_sem, g_sem, first_tx, first_rx, col_tx, col_rx, row_tx, row_rx, sib_tx, sib_rx, stat_tx, stat_rx):
    t = lax.axis_index("tp")
    rows, _ = a_v.shape
    d_loc = own.shape[1]
    per = d_loc // CW
    peers = ((t + 2) % 4, 3 - t, t + 1 - 2 * (t % 2))
    n_blk = len(BLOCKS)
    blocks = [(sum(BLOCKS[:b]), BLOCKS[b]) for b in range(n_blk)]
    c0 = N_COL * CW

    def w_copy(slot, col):
        return pltpu.make_async_copy(w_hbm.at[:, pl.ds(pl.multiple_of(col, CW), CW)], w_v.at[slot], w_sem.at[slot])

    def cross_col(i):
        k = i % 2
        return (peers[0] + (peers[1] - peers[0]) * k) * d_loc + (i // 2) * CW

    def near_col(i):
        return (peers[2] + (t - peers[2]) * (i // per)) * d_loc + (i % per) * CW

    def remote(src, dst, tx, rx, peer):
        return pltpu.make_async_remote_copy(src_ref=src, dst_ref=dst, send_sem=tx, recv_sem=rx,
                                            device_id={"tp": peer}, device_id_type=MESH)

    def col_copy(k, j):
        cols = pl.ds(j * CW, CW)
        return remote(part.at[k, :, cols], recv.at[k, :, cols], col_tx.at[k, j], col_rx.at[k, j], peers[k])

    def row_copy(k, b):
        sl = (k, pl.ds(*blocks[b]), pl.ds(c0, d_loc - c0))
        return remote(part.at[sl], recv.at[sl], row_tx.at[k, b], row_rx.at[k, b],
                      peers[0] + (peers[1] - peers[0]) * k)

    def sib_copy():
        return remote(part.at[2], recv.at[2], sib_tx, sib_rx, peers[2])

    def stat_copy(k, b):
        return remote(st_tx.at[b], st_rx.at[k, b], stat_tx.at[k, b], stat_rx.at[k, b], peers[k])

    half, lanes = rows // 2, 128

    def a_copy(q):
        sl = pl.ds(q * half, half)
        return pltpu.make_async_copy(a_hbm.at[sl, :], a_v.at[sl, :], a_sem.at[q])

    def w0_copy(q, first, n):
        src = w_hbm.at[:, pl.ds(pl.multiple_of(cross_col(0) + first, lanes), n)]
        return pltpu.make_async_copy(src, w_v.at[0, :, pl.ds(first, n)], w0_sem.at[q])

    def w_start(i):
        if isinstance(i, int):
            w_copy(i, cross_col(i) if i < 2 * per else near_col(i - 2 * per)).start()
            return

        @pl.when(i < 2 * per)
        def _():
            w_copy(i, cross_col(i)).start()

        @pl.when((i >= 2 * per) & (i < 4 * per))
        def _():
            w_copy(i, near_col(i - 2 * per)).start()

    r_copy = pltpu.make_async_copy(r_hbm, r_v, r_sem)
    g_copy = pltpu.make_async_copy(g_hbm, g_v, g_sem)
    a_copy(0).start()
    w0_copy(0, 0, lanes).start()
    a_copy(1).start()
    w0_copy(1, lanes, CW - lanes).start()
    barrier = pltpu.get_barrier_semaphore()
    for p in peers:
        pl.semaphore_signal(barrier, inc=1, device_id={"tp": p}, device_id_type=MESH)

    def dot(lhs, rhs):
        return jnp.dot(lhs, rhs, preferred_element_type=F32)

    pieces = ((pl.ds(0, half), pl.ds(0, lanes)), (pl.ds(half, half), pl.ds(0, lanes)),
              (pl.ds(0, rows), pl.ds(lanes, CW - lanes)))

    def piece_copy(q):
        sl = (0, *pieces[q])
        return remote(part.at[sl], recv.at[sl], first_tx.at[q], first_rx.at[q], peers[0])

    for q, (r_sl, c_sl) in enumerate(pieces):
        if q == 0:
            a_copy(0).wait()
            w0_copy(0, 0, lanes).wait()
            for i in range(1, DEPTH):
                w_start(i)
        elif q == 1:
            a_copy(1).wait()
        else:
            w0_copy(1, lanes, CW - lanes).wait()
            w_start(DEPTH)
        part[0, r_sl, c_sl] = dot(a_v[r_sl, :], w_v[0, :, c_sl]).astype(BF16)
        if q == 0:
            pl.semaphore_wait(barrier, 3)
        piece_copy(q).start()

    def chunk(i, col):
        w_copy(i, col).wait()
        w_start(i + DEPTH)
        return dot(a_v[...], w_v[i])

    def cross(i):
        part[i % 2, :, pl.ds(pl.multiple_of((i // 2) * CW, CW), CW)] = chunk(i, cross_col(i)).astype(BF16)

    for i in range(1, 2 * N_COL):
        cross(i)
        col_copy(i % 2, i // 2).start()

    @pl.loop(2 * N_COL, 2 * per)
    def _(i):
        cross(i)

    far, near = t % 2, 1 - t % 2
    order = ([(k, b) for b in range(n_blk - 2) for k in (far, near)]
             + [(k, b) for k in (far, near) for b in (n_blk - 2, n_blk - 1)])
    for k, b in order:
        row_copy(k, b).start()
    r_copy.start()
    g_copy.start()

    @pl.loop(0, per)
    def _(j):
        part[2, :, pl.ds(pl.multiple_of(j * CW, CW), CW)] = chunk(2 * per + j, near_col(j)).astype(BF16)

    sib_copy().start()

    @pl.loop(0, per)
    def _(j):
        own[:, pl.ds(pl.multiple_of(j * CW, CW), CW)] = chunk(3 * per + j, near_col(per + j))

    r_copy.wait()
    g_copy.wait()
    sib_copy().wait_recv()
    for q in range(len(pieces)):
        piece_copy(q).wait_recv()
    for i in range(1, 2 * N_COL):
        col_copy(i % 2, i // 2).wait_recv()

    lane = lax.broadcasted_iota(jnp.int32, (8, 128), 1)
    sub = lax.broadcasted_iota(jnp.int32, (8, 128), 0)

    def reduce_block(b):
        row_copy(0, b).wait_recv()
        row_copy(1, b).wait_recv()
        row, n = blocks[b]
        line = jnp.zeros((8, 128), F32)
        for first in range(0, n, SUB):
            sl = pl.ds(row + first, SUB)
            h = own[sl, :] + recv[0, sl, :].astype(F32) + recv[1, sl, :].astype(F32) + recv[2, sl, :].astype(F32)
            h = r_v[sl, :].astype(F32) + h
            own[sl, :] = h
            hid[sl, :] = h.astype(BF16)
            s = jnp.sum(h * h, axis=1, keepdims=True)
            for q in range(0, SUB, 8):
                line = line + jnp.where(lane == sub + (first + q), s[q:q + 8, :], 0.0)
        st_tx[b] = jnp.sum(line, axis=0, keepdims=True)
        for k in range(3):
            stat_copy(k, b).start()

    def norm_block(b):
        for k in range(3):
            stat_copy(k, b).wait_recv()
        row, n = blocks[b]
        tot = (st_tx[b] + st_rx[2, b]) + (st_rx[0, b] + st_rx[1, b])
        scale = jnp.broadcast_to(lax.rsqrt(tot / d_model + EPS), (8, 128))
        for first in range(0, n, SUB):
            for q in range(first, first + SUB, 8):
                sl = pl.ds(row + q, 8)
                col = jnp.sum(jnp.where(lane == sub + q, scale, 0.0), axis=1, keepdims=True)
                own[sl, :] = own[sl, :] * col * g_v[...]
            sl = pl.ds(row + first, SUB)
            nrm[sl, :] = own[sl, :].astype(BF16)

    for b in range(n_blk):
        reduce_block(b)

    for b in range(n_blk):
        norm_block(b)

    for q in range(len(pieces)):
        piece_copy(q).wait_send()
    for i in range(1, 2 * N_COL):
        col_copy(i % 2, i // 2).wait_send()
    sib_copy().wait_send()

    for b in range(n_blk):
        row_copy(0, b).wait_send()
        row_copy(1, b).wait_send()

    @pl.loop(0, n_blk)
    def _(b):
        for k in range(3):
            stat_copy(k, b).wait_send()


def put(hid, nrm, hid_hbm, nrm_hbm, sem):
    n = hid.shape[0] // PUT
    copies = []
    for q in range(PUT):
        sl = pl.ds(q * n, n)
        copies.append(pltpu.make_async_copy(hid.at[sl, :], hid_hbm.at[sl, :], sem.at[0, q]))
        copies.append(pltpu.make_async_copy(nrm.at[sl, :], nrm_hbm.at[sl, :], sem.at[1, q]))
    for c in copies:
        c.start()
    for c in copies:
        c.wait()


def solution(mesh):
    tp = mesh.shape["tp"]

    def local_step(a, w, r, g):
        rows, depth = a.shape
        d_loc = r.shape[1]
        per = d_loc // CW
        n_blk = len(BLOCKS)
        hbm = pl.BlockSpec(memory_space=pltpu.HBM)
        vmem = pl.BlockSpec(memory_space=pltpu.VMEM)
        dma = pltpu.SemaphoreType.DMA
        hid, nrm = pl.pallas_call(
            functools.partial(kernel, d_loc * tp),
            out_shape=(pltpu.VMEM((rows, d_loc), BF16),) * 2,
            in_specs=[hbm] * 4,
            out_specs=(vmem,) * 2,
            scratch_shapes=[
                pltpu.VMEM((rows, depth), BF16),
                pltpu.VMEM((4 * per, depth, CW), BF16),
                pltpu.VMEM((rows, d_loc), BF16),
                pltpu.VMEM((1, d_loc), F32),
                pltpu.VMEM((3, rows, d_loc), BF16),
                pltpu.VMEM((3, rows, d_loc), BF16),
                pltpu.VMEM((rows, d_loc), F32),
                pltpu.VMEM((n_blk, 1, 128), F32),
                pltpu.VMEM((3, n_blk, 1, 128), F32),
                dma((2,)), dma((2,)), dma((4 * per,)), dma, dma, dma((3,)), dma((3,)),
                dma((2, N_COL)), dma((2, N_COL)), dma((2, n_blk)), dma((2, n_blk)), dma, dma,
                dma((3, n_blk)), dma((3, n_blk)),
            ],
            compiler_params=pltpu.CompilerParams(
                collective_id=0, has_side_effects=True, vmem_limit_bytes=64946176),
            cost_estimate=pl.CostEstimate(flops=2 * rows * depth * d_loc * tp, transcendentals=0,
                                          bytes_accessed=2 * depth * d_loc * tp),
        )(a, w, r, g.reshape(1, d_loc))
        return pl.pallas_call(
            put,
            out_shape=(jax.ShapeDtypeStruct((rows, d_loc), BF16),) * 2,
            in_specs=[vmem] * 2,
            out_specs=(hbm,) * 2,
            scratch_shapes=[dma((2, PUT))],
            compiler_params=pltpu.CompilerParams(vmem_limit_bytes=1024 * 1024),
        )(hid, nrm)

    return jax.shard_map(
        local_step,
        mesh=mesh,
        in_specs=(P("data", "tp"), P("tp", None), P("data", "tp"), P("tp")),
        out_specs=(P("data", "tp"), P("data", "tp")),
        check_vma=False,
    )
```

```python
import functools

import jax
import jax.numpy as jnp
from jax import lax
from jax.experimental import pallas as pl
from jax.experimental.pallas import tpu as pltpu
from jax.sharding import PartitionSpec as P

EPS = 1e-5
MESH = pl.DeviceIdType.MESH
F32, BF16 = jnp.float32, jnp.bfloat16

CW = 256
N_COL = 2
BLOCKS = (128, 112, 16)
SUB = 16
DEPTH = 4
PUT = 1
FAR, NEAR, SIB = 0, 1, 2


def kernel(d_model, a_hbm, w_hbm, r_hbm, g_hbm, hid, nrm,
           a_v, w_v, r_v, g_v, part, recv, own, st_tx, st_rx,
           a_sem, w0_sem, w_sem, r_sem, g_sem, far_tx, far_rx, near_tx, near_rx, sib_tx, sib_rx, stat_tx, stat_rx):
    t = lax.axis_index("tp")
    core, chip = t % 2, t // 2
    rows, _ = a_v.shape
    d_loc = own.shape[1]
    per = d_loc // CW
    n_blk = len(BLOCKS)
    blocks = [(sum(BLOCKS[:b]), BLOCKS[b]) for b in range(n_blk)]
    half, lanes = rows // 2, 128
    far, near, sib = 2 - 2 * chip, 3 - 2 * chip, t + 1 - 2 * core

    def cross_col(i):
        return (far + i // per) * d_loc + (i % per) * CW

    def home_col(i):
        return (sib + (t - sib) * (i // per)) * d_loc + (i % per) * CW

    def w_copy(i, col):
        return pltpu.make_async_copy(w_hbm.at[:, pl.ds(pl.multiple_of(col, CW), CW)], w_v.at[i], w_sem.at[i])

    def w_start(i):
        if isinstance(i, int):
            w_copy(i, cross_col(i) if i < 2 * per else home_col(i - 2 * per)).start()
            return

        @pl.when(i < 2 * per)
        def _():
            w_copy(i, cross_col(i)).start()

        @pl.when((i >= 2 * per) & (i < 4 * per))
        def _():
            w_copy(i, home_col(i - 2 * per)).start()

    def a_copy(q):
        sl = pl.ds(q * half, half)
        return pltpu.make_async_copy(a_hbm.at[sl, :], a_v.at[sl, :], a_sem.at[q])

    def w0_copy(q):
        src = w_hbm.at[:, pl.ds(pl.multiple_of(far * d_loc + q * lanes, lanes), lanes)]
        return pltpu.make_async_copy(src, w_v.at[0, :, pl.ds(q * lanes, lanes)], w0_sem.at[q])

    def remote(src, dst, tx, rx, peer):
        return pltpu.make_async_remote_copy(src_ref=src, dst_ref=dst, send_sem=tx, recv_sem=rx,
                                            device_id={"tp": peer}, device_id_type=MESH)

    every = pl.ds(0, rows)
    far_parts = [(pl.ds(0, half), pl.ds(0, lanes)), (pl.ds(0, half), pl.ds(lanes, lanes)), (pl.ds(half, half), pl.ds(0, CW))]
    far_parts += [(every, pl.ds(j * CW, CW)) for j in range(1, N_COL)]
    far_parts += [(every, pl.ds(N_COL * CW, d_loc - N_COL * CW))]

    def far_copy(q, slot):
        sl = far_parts[q]
        return remote(part.at[(FAR, *sl)], recv.at[(slot, *sl)], far_tx.at[q], far_rx.at[slot, q], far)

    def near_copy(b, slot):
        sl = pl.ds(*blocks[b])
        return remote(part.at[NEAR, sl, :], recv.at[slot, sl, :], near_tx.at[b], near_rx.at[slot, b], near)

    def sib_copy():
        return remote(part.at[SIB], recv.at[SIB], sib_tx, sib_rx, sib)

    def stat_copy(k, b, slot):
        return remote(st_tx.at[b], st_rx.at[slot, b], stat_tx.at[k, b], stat_rx.at[slot, b], (far, near, sib)[k])

    a_copy(0).start()
    w0_copy(0).start()
    w0_copy(1).start()
    a_copy(1).start()
    r_copy = pltpu.make_async_copy(r_hbm, r_v, r_sem)
    g_copy = pltpu.make_async_copy(g_hbm, g_v, g_sem)
    barrier = pltpu.get_barrier_semaphore()
    for p in (far, near, sib):
        pl.semaphore_signal(barrier, inc=1, device_id={"tp": p}, device_id_type=MESH)

    def dot(lhs, rhs):
        return jnp.dot(lhs, rhs, preferred_element_type=F32)

    for q in range(3):
        if q == 0:
            a_copy(0).wait()
            w0_copy(0).wait()
            for i in range(1, DEPTH):
                w_start(i)
        elif q == 1:
            w0_copy(1).wait()
        else:
            a_copy(1).wait()
            w_start(DEPTH)
        r_sl, c_sl = far_parts[q]
        part[FAR, r_sl, c_sl] = dot(a_v[r_sl, :], w_v[0, :, c_sl]).astype(BF16)
        if q == 0:
            pl.semaphore_wait(barrier, 3)
        far_copy(q, core).start()

    def chunk(i, col):
        w_copy(i, col).wait()
        w_start(i + DEPTH)
        return dot(a_v[...], w_v[i])

    def columns(j):
        return pl.ds(pl.multiple_of(j * CW, CW), CW)

    for j in range(1, N_COL):
        part[FAR, :, columns(j)] = chunk(j, cross_col(j)).astype(BF16)
        far_copy(2 + j, core).start()

    @pl.loop(N_COL, per)
    def _(j):
        part[FAR, :, columns(j)] = chunk(j, cross_col(j)).astype(BF16)

    far_copy(len(far_parts) - 1, core).start()

    @pl.loop(0, per)
    def _(j):
        part[NEAR, :, columns(j)] = chunk(per + j, cross_col(per + j)).astype(BF16)

    for b in range(n_blk):
        near_copy(b, core).start()
    r_copy.start()
    g_copy.start()

    @pl.loop(0, per)
    def _(j):
        part[SIB, :, columns(j)] = chunk(2 * per + j, home_col(j)).astype(BF16)

    sib_copy().start()

    @pl.loop(0, per)
    def _(j):
        own[:, columns(j)] = chunk(3 * per + j, home_col(per + j))

    r_copy.wait()
    g_copy.wait()
    sib_copy().wait_recv()

    @pl.when(core == 0)
    def _():
        for q in range(len(far_parts)):
            for slot in range(2):
                far_copy(q, slot).wait_recv()

    lane = lax.broadcasted_iota(jnp.int32, (8, 128), 1)
    sub = lax.broadcasted_iota(jnp.int32, (8, 128), 0)

    def reduce_block(b):
        @pl.when(core == 1)
        def _():
            for slot in range(2):
                near_copy(b, slot).wait_recv()

        row, n = blocks[b]
        line = jnp.zeros((8, 128), F32)
        for first in range(0, n, SUB):
            sl = pl.ds(row + first, SUB)
            h = own[sl, :] + recv[SIB, sl, :].astype(F32) + recv[0, sl, :].astype(F32) + recv[1, sl, :].astype(F32)
            h = r_v[sl, :].astype(F32) + h
            own[sl, :] = h
            hid[sl, :] = h.astype(BF16)
            s = jnp.sum(h * h, axis=1, keepdims=True)
            for q in range(0, SUB, 8):
                line = line + jnp.where(lane == sub + (first + q), s[q:q + 8, :], 0.0)
        st_tx[b] = jnp.sum(line, axis=0, keepdims=True)
        for k in range(3):
            stat_copy(k, b, SIB if k == SIB else core).start()

    def norm_block(b):
        for slot in range(3):
            stat_copy(slot, b, slot).wait_recv()
        row, n = blocks[b]
        tot = (st_tx[b] + st_rx[SIB, b]) + (st_rx[0, b] + st_rx[1, b])
        scale = jnp.broadcast_to(lax.rsqrt(tot / d_model + EPS), (8, 128))
        for first in range(0, n, SUB):
            for q in range(first, first + SUB, 8):
                sl = pl.ds(row + q, 8)
                col = jnp.sum(jnp.where(lane == sub + q, scale, 0.0), axis=1, keepdims=True)
                own[sl, :] = own[sl, :] * col * g_v[...]
            sl = pl.ds(row + first, SUB)
            nrm[sl, :] = own[sl, :].astype(BF16)

    for b in range(n_blk):
        reduce_block(b)

    for b in range(n_blk):
        norm_block(b)

    for q in range(len(far_parts)):
        far_copy(q, core).wait_send()
    for b in range(n_blk):
        near_copy(b, core).wait_send()
        for k in range(3):
            stat_copy(k, b, SIB if k == SIB else core).wait_send()
    sib_copy().wait_send()


def put(hid, nrm, hid_hbm, nrm_hbm, sem):
    n = hid.shape[0] // PUT
    copies = []
    for q in range(PUT):
        sl = pl.ds(q * n, n)
        copies.append(pltpu.make_async_copy(hid.at[sl, :], hid_hbm.at[sl, :], sem.at[0, q]))
        copies.append(pltpu.make_async_copy(nrm.at[sl, :], nrm_hbm.at[sl, :], sem.at[1, q]))
    for c in copies:
        c.start()
    for c in copies:
        c.wait()


def solution(mesh):
    tp = mesh.shape["tp"]

    def local_step(a, w, r, g):
        rows, depth = a.shape
        d_loc = r.shape[1]
        per = d_loc // CW
        n_blk = len(BLOCKS)
        hbm = pl.BlockSpec(memory_space=pltpu.HBM)
        vmem = pl.BlockSpec(memory_space=pltpu.VMEM)
        dma = pltpu.SemaphoreType.DMA
        hid, nrm = pl.pallas_call(
            functools.partial(kernel, d_loc * tp),
            out_shape=(pltpu.VMEM((rows, d_loc), BF16),) * 2,
            in_specs=[hbm] * 4,
            out_specs=(vmem,) * 2,
            scratch_shapes=[
                pltpu.VMEM((rows, depth), BF16),
                pltpu.VMEM((4 * per, depth, CW), BF16),
                pltpu.VMEM((rows, d_loc), BF16),
                pltpu.VMEM((1, d_loc), F32),
                pltpu.VMEM((3, rows, d_loc), BF16),
                pltpu.VMEM((3, rows, d_loc), BF16),
                pltpu.VMEM((rows, d_loc), F32),
                pltpu.VMEM((n_blk, 1, 128), F32),
                pltpu.VMEM((3, n_blk, 1, 128), F32),
                dma((2,)), dma((2,)), dma((4 * per,)), dma, dma,
                dma((N_COL + 3,)), dma((2, N_COL + 3)), dma((n_blk,)), dma((2, n_blk)), dma, dma,
                dma((3, n_blk)), dma((3, n_blk)),
            ],
            compiler_params=pltpu.CompilerParams(
                collective_id=0, has_side_effects=True, vmem_limit_bytes=64946176),
            cost_estimate=pl.CostEstimate(flops=2 * rows * depth * d_loc * tp, transcendentals=0,
                                          bytes_accessed=2 * depth * d_loc * tp),
        )(a, w, r, g.reshape(1, d_loc))
        return pl.pallas_call(
            put,
            out_shape=(jax.ShapeDtypeStruct((rows, d_loc), BF16),) * 2,
            in_specs=[vmem] * 2,
            out_specs=(hbm,) * 2,
            scratch_shapes=[dma((2, PUT))],
            compiler_params=pltpu.CompilerParams(vmem_limit_bytes=1024 * 1024),
        )(hid, nrm)

    return jax.shard_map(
        local_step,
        mesh=mesh,
        in_specs=(P("data", "tp"), P("tp", None), P("data", "tp"), P("tp")),
        out_specs=(P("data", "tp"), P("data", "tp")),
        check_vma=False,
    )
```

```python
import functools

import jax
import jax.numpy as jnp
from jax import lax
from jax.experimental import pallas as pl
from jax.experimental.pallas import tpu as pltpu
from jax.sharding import PartitionSpec as P

EPS = 1e-5
MESH = pl.DeviceIdType.MESH
F32, BF16 = jnp.float32, jnp.bfloat16

CW = 256
N_COL = 2
BLOCKS = (128, 112, 16)
SUB = 16
DEPTH = 4
PUT = 1
FAR, NEAR, SIB = 0, 1, 2


def kernel(d_model, a_hbm, w_hbm, r_hbm, g_hbm, hid, nrm,
           a_v, w_v, r_v, g_v, part, recv, own, st_tx, st_rx,
           a_sem, w0_sem, w_sem, r_sem, g_sem, far_tx, far_rx, near_tx, near_rx, sib_tx, sib_rx, stat_tx, stat_rx):
    t = lax.axis_index("tp")
    core, chip = t % 2, t // 2
    rows, _ = a_v.shape
    d_loc = own.shape[1]
    per = d_loc // CW
    n_blk = len(BLOCKS)
    blocks = [(sum(BLOCKS[:b]), BLOCKS[b]) for b in range(n_blk)]
    half, lanes = rows // 2, 128
    far, near, sib = 2 - 2 * chip, 3 - 2 * chip, t + 1 - 2 * core

    def cross_col(i):
        return (far + i // per) * d_loc + (i % per) * CW

    def home_col(i):
        return (sib + (t - sib) * (i // per)) * d_loc + (i % per) * CW

    def w_copy(i, col):
        return pltpu.make_async_copy(w_hbm.at[:, pl.ds(pl.multiple_of(col, CW), CW)], w_v.at[i], w_sem.at[i])

    def w_start(i):
        if isinstance(i, int):
            w_copy(i, cross_col(i) if i < 2 * per else home_col(i - 2 * per)).start()
            return

        @pl.when(i < 2 * per)
        def _():
            w_copy(i, cross_col(i)).start()

        @pl.when((i >= 2 * per) & (i < 4 * per))
        def _():
            w_copy(i, home_col(i - 2 * per)).start()

    def a_copy(q):
        sl = pl.ds(q * half, half)
        return pltpu.make_async_copy(a_hbm.at[sl, :], a_v.at[sl, :], a_sem.at[q])

    def w0_copy(q):
        src = w_hbm.at[:, pl.ds(pl.multiple_of(far * d_loc + q * lanes, lanes), lanes)]
        return pltpu.make_async_copy(src, w_v.at[0, :, pl.ds(q * lanes, lanes)], w0_sem.at[q])

    def remote(src, dst, tx, rx, peer):
        return pltpu.make_async_remote_copy(src_ref=src, dst_ref=dst, send_sem=tx, recv_sem=rx,
                                            device_id={"tp": peer}, device_id_type=MESH)

    every = pl.ds(0, rows)
    far_parts = [(pl.ds(0, half), pl.ds(0, lanes)), (pl.ds(0, half), pl.ds(lanes, lanes)), (pl.ds(half, half), pl.ds(0, CW))]
    far_parts += [(every, pl.ds(j * CW, CW)) for j in range(1, N_COL)]
    far_parts += [(every, pl.ds(N_COL * CW, d_loc - N_COL * CW))]

    def far_copy(q, slot):
        sl = far_parts[q]
        return remote(part.at[(FAR, *sl)], recv.at[(slot, *sl)], far_tx.at[q], far_rx.at[slot, q], far)

    def near_copy(b, slot):
        sl = pl.ds(*blocks[b])
        return remote(part.at[NEAR, sl, :], recv.at[slot, sl, :], near_tx.at[b], near_rx.at[slot, b], near)

    def sib_copy():
        return remote(part.at[SIB], recv.at[SIB], sib_tx, sib_rx, sib)

    def stat_copy(k, b, slot):
        return remote(st_tx.at[b], st_rx.at[slot, b], stat_tx.at[k, b], stat_rx.at[slot, b], (far, near, sib)[k])

    a_copy(0).start()
    w0_copy(0).start()
    w0_copy(1).start()
    a_copy(1).start()
    r_copy = pltpu.make_async_copy(r_hbm, r_v, r_sem)
    g_copy = pltpu.make_async_copy(g_hbm, g_v, g_sem)
    barrier = pltpu.get_barrier_semaphore()
    for p in (far, near, sib):
        pl.semaphore_signal(barrier, inc=1, device_id={"tp": p}, device_id_type=MESH)

    def dot(lhs, rhs):
        return jnp.dot(lhs, rhs, preferred_element_type=F32)

    for q in range(3):
        if q == 0:
            a_copy(0).wait()
            w0_copy(0).wait()
            for i in range(1, DEPTH):
                w_start(i)
        elif q == 1:
            w0_copy(1).wait()
        else:
            a_copy(1).wait()
            w_start(DEPTH)
        r_sl, c_sl = far_parts[q]
        part[FAR, r_sl, c_sl] = dot(a_v[r_sl, :], w_v[0, :, c_sl]).astype(BF16)
        if q == 0:
            pl.semaphore_wait(barrier, 3)
        far_copy(q, core).start()

    def chunk(i, col):
        w_copy(i, col).wait()
        w_start(i + DEPTH)
        return dot(a_v[...], w_v[i])

    def columns(j):
        return pl.ds(pl.multiple_of(j * CW, CW), CW)

    for j in range(1, N_COL):
        part[FAR, :, columns(j)] = chunk(j, cross_col(j)).astype(BF16)
        far_copy(2 + j, core).start()

    @pl.loop(N_COL, per)
    def _(j):
        part[FAR, :, columns(j)] = chunk(j, cross_col(j)).astype(BF16)

    far_copy(len(far_parts) - 1, core).start()

    @pl.loop(0, per)
    def _(j):
        part[NEAR, :, columns(j)] = chunk(per + j, cross_col(per + j)).astype(BF16)

    near_copy(0, core).start()

    @pl.when(core == 0)
    def _():
        for b in range(1, n_blk):
            near_copy(b, core).start()

    r_copy.start()
    g_copy.start()

    @pl.loop(0, per)
    def _(j):
        part[SIB, :, columns(j)] = chunk(2 * per + j, home_col(j)).astype(BF16)

    sib_copy().start()

    @pl.loop(0, per)
    def _(j):
        own[:, columns(j)] = chunk(3 * per + j, home_col(per + j))

    r_copy.wait()
    g_copy.wait()
    sib_copy().wait_recv()

    @pl.when(core == 0)
    def _():
        for q in range(len(far_parts)):
            for slot in range(2):
                far_copy(q, slot).wait_recv()

    @pl.when(core == 1)
    def _():
        near_copy(0, core).wait_send()
        for b in range(1, n_blk):
            near_copy(b, core).start()

    lane = lax.broadcasted_iota(jnp.int32, (8, 128), 1)
    sub = lax.broadcasted_iota(jnp.int32, (8, 128), 0)

    def reduce_block(b):
        @pl.when(core == 1)
        def _():
            for slot in range(2):
                near_copy(b, slot).wait_recv()

        row, n = blocks[b]
        line = jnp.zeros((8, 128), F32)
        for first in range(0, n, SUB):
            sl = pl.ds(row + first, SUB)
            h = own[sl, :] + recv[SIB, sl, :].astype(F32) + recv[0, sl, :].astype(F32) + recv[1, sl, :].astype(F32)
            h = r_v[sl, :].astype(F32) + h
            own[sl, :] = h
            hid[sl, :] = h.astype(BF16)
            s = jnp.sum(h * h, axis=1, keepdims=True)
            for q in range(0, SUB, 8):
                line = line + jnp.where(lane == sub + (first + q), s[q:q + 8, :], 0.0)
        st_tx[b] = jnp.sum(line, axis=0, keepdims=True)
        for k in range(3):
            stat_copy(k, b, SIB if k == SIB else core).start()

    def norm_block(b):
        for slot in range(3):
            stat_copy(slot, b, slot).wait_recv()
        row, n = blocks[b]
        tot = (st_tx[b] + st_rx[SIB, b]) + (st_rx[0, b] + st_rx[1, b])
        scale = jnp.broadcast_to(lax.rsqrt(tot / d_model + EPS), (8, 128))
        for first in range(0, n, SUB):
            for q in range(first, first + SUB, 8):
                sl = pl.ds(row + q, 8)
                col = jnp.sum(jnp.where(lane == sub + q, scale, 0.0), axis=1, keepdims=True)
                own[sl, :] = own[sl, :] * col * g_v[...]
            sl = pl.ds(row + first, SUB)
            nrm[sl, :] = own[sl, :].astype(BF16)

    for b in range(n_blk):
        reduce_block(b)

    for b in range(n_blk):
        norm_block(b)

    for q in range(len(far_parts)):
        far_copy(q, core).wait_send()
    @pl.when(core == 0)
    def _():
        near_copy(0, core).wait_send()

    for b in range(n_blk):
        if b:
            near_copy(b, core).wait_send()
        for k in range(3):
            stat_copy(k, b, SIB if k == SIB else core).wait_send()
    sib_copy().wait_send()


def put(hid, nrm, hid_hbm, nrm_hbm, sem):
    n = hid.shape[0] // PUT
    copies = []
    for q in range(PUT):
        sl = pl.ds(q * n, n)
        copies.append(pltpu.make_async_copy(hid.at[sl, :], hid_hbm.at[sl, :], sem.at[0, q]))
        copies.append(pltpu.make_async_copy(nrm.at[sl, :], nrm_hbm.at[sl, :], sem.at[1, q]))
    for c in copies:
        c.start()
    for c in copies:
        c.wait()


def solution(mesh):
    tp = mesh.shape["tp"]

    def local_step(a, w, r, g):
        rows, depth = a.shape
        d_loc = r.shape[1]
        per = d_loc // CW
        n_blk = len(BLOCKS)
        hbm = pl.BlockSpec(memory_space=pltpu.HBM)
        vmem = pl.BlockSpec(memory_space=pltpu.VMEM)
        dma = pltpu.SemaphoreType.DMA
        hid, nrm = pl.pallas_call(
            functools.partial(kernel, d_loc * tp),
            out_shape=(pltpu.VMEM((rows, d_loc), BF16),) * 2,
            in_specs=[hbm] * 4,
            out_specs=(vmem,) * 2,
            scratch_shapes=[
                pltpu.VMEM((rows, depth), BF16),
                pltpu.VMEM((4 * per, depth, CW), BF16),
                pltpu.VMEM((rows, d_loc), BF16),
                pltpu.VMEM((1, d_loc), F32),
                pltpu.VMEM((3, rows, d_loc), BF16),
                pltpu.VMEM((3, rows, d_loc), BF16),
                pltpu.VMEM((rows, d_loc), F32),
                pltpu.VMEM((n_blk, 1, 128), F32),
                pltpu.VMEM((3, n_blk, 1, 128), F32),
                dma((2,)), dma((2,)), dma((4 * per,)), dma, dma,
                dma((N_COL + 3,)), dma((2, N_COL + 3)), dma((n_blk,)), dma((2, n_blk)), dma, dma,
                dma((3, n_blk)), dma((3, n_blk)),
            ],
            compiler_params=pltpu.CompilerParams(
                collective_id=0, has_side_effects=True, vmem_limit_bytes=64946176),
            cost_estimate=pl.CostEstimate(flops=2 * rows * depth * d_loc * tp, transcendentals=0,
                                          bytes_accessed=2 * depth * d_loc * tp),
        )(a, w, r, g.reshape(1, d_loc))
        return pl.pallas_call(
            put,
            out_shape=(jax.ShapeDtypeStruct((rows, d_loc), BF16),) * 2,
            in_specs=[vmem] * 2,
            out_specs=(hbm,) * 2,
            scratch_shapes=[dma((2, PUT))],
            compiler_params=pltpu.CompilerParams(vmem_limit_bytes=1024 * 1024),
        )(hid, nrm)

    return jax.shard_map(
        local_step,
        mesh=mesh,
        in_specs=(P("data", "tp"), P("tp", None), P("data", "tp"), P("tp")),
        out_specs=(P("data", "tp"), P("data", "tp")),
        check_vma=False,
    )
```

```python
import functools

import jax
import jax.numpy as jnp
from jax import lax
from jax.experimental import pallas as pl
from jax.experimental.pallas import tpu as pltpu
from jax.sharding import PartitionSpec as P

EPS = 1e-5
MESH = pl.DeviceIdType.MESH
F32, BF16 = jnp.float32, jnp.bfloat16

CW = 256
N_COL = 2
BLOCKS = (128, 112, 16)
SUB = 16
DEPTH = 4
PUT = 1
FAR, NEAR, SIB = 0, 1, 2


def kernel(d_model, a_hbm, w_hbm, r_hbm, g_hbm, hid, nrm,
           a_v, w_v, r_v, g_v, part, recv, own, last_sib, last_tx, last_rx, st_tx, st_rx,
           a_sem, w0_sem, w_sem, r_sem, g_sem, far_tx, far_rx, near_tx, near_rx, last_sems, sib_tx, sib_rx, stat_tx, stat_rx):
    t = lax.axis_index("tp")
    core, chip = t % 2, t // 2
    rows, _ = a_v.shape
    d_loc = own.shape[1]
    per = d_loc // CW
    n_blk = len(BLOCKS)
    blocks = [(sum(BLOCKS[:b]), BLOCKS[b]) for b in range(n_blk)]
    half, lanes = rows // 2, 128
    far, near, sib = 2 - 2 * chip, 3 - 2 * chip, t + 1 - 2 * core

    def cross_col(i):
        return (far + i // per) * d_loc + (i % per) * CW

    def home_col(i):
        return (sib + (t - sib) * (i // per)) * d_loc + (i % per) * CW

    def w_copy(i, col):
        return pltpu.make_async_copy(w_hbm.at[:, pl.ds(pl.multiple_of(col, CW), CW)], w_v.at[i], w_sem.at[i])

    def w_start(i):
        if isinstance(i, int):
            w_copy(i, cross_col(i) if i < 2 * per else home_col(i - 2 * per)).start()
            return

        @pl.when(i < 2 * per)
        def _():
            w_copy(i, cross_col(i)).start()

        @pl.when((i >= 2 * per) & (i < 4 * per))
        def _():
            w_copy(i, home_col(i - 2 * per)).start()

    def a_copy(q):
        sl = pl.ds(q * half, half)
        return pltpu.make_async_copy(a_hbm.at[sl, :], a_v.at[sl, :], a_sem.at[q])

    def w0_copy(q):
        src = w_hbm.at[:, pl.ds(pl.multiple_of(far * d_loc + q * lanes, lanes), lanes)]
        return pltpu.make_async_copy(src, w_v.at[0, :, pl.ds(q * lanes, lanes)], w0_sem.at[q])

    def remote(src, dst, tx, rx, peer):
        return pltpu.make_async_remote_copy(src_ref=src, dst_ref=dst, send_sem=tx, recv_sem=rx,
                                            device_id={"tp": peer}, device_id_type=MESH)

    every = pl.ds(0, rows)
    far_parts = [(pl.ds(0, half), pl.ds(0, lanes)), (pl.ds(0, half), pl.ds(lanes, lanes)), (pl.ds(half, half), pl.ds(0, CW))]
    far_parts += [(every, pl.ds(j * CW, CW)) for j in range(1, N_COL)]
    far_parts += [(every, pl.ds(N_COL * CW, d_loc - N_COL * CW))]

    def far_copy(q, slot):
        sl = far_parts[q]
        return remote(part.at[(FAR, *sl)], recv.at[(slot, *sl)], far_tx.at[q], far_rx.at[slot, q], far)

    def near_copy(b, slot):
        sl = pl.ds(*blocks[b])
        return remote(part.at[NEAR, sl, :], recv.at[slot, sl, :], near_tx.at[b], near_rx.at[slot, b], near)

    last = pl.ds(*blocks[-1])

    def last_sib_copy():
        return remote(part.at[NEAR, last, :], last_sib, last_sems.at[0], last_sems.at[1], sib)

    def last_copy():
        return remote(last_tx, last_rx, last_sems.at[2], last_sems.at[3], near)

    def sib_copy():
        return remote(part.at[SIB], recv.at[SIB], sib_tx, sib_rx, sib)

    def stat_copy(k, b, slot):
        return remote(st_tx.at[b], st_rx.at[slot, b], stat_tx.at[k, b], stat_rx.at[slot, b], (far, near, sib)[k])

    barrier = pltpu.get_barrier_semaphore()
    for p in (far, near, sib):
        pl.semaphore_signal(barrier, inc=1, device_id={"tp": p}, device_id_type=MESH)
    a_copy(0).start()
    w0_copy(0).start()
    w0_copy(1).start()
    a_copy(1).start()
    r_copy = pltpu.make_async_copy(r_hbm, r_v, r_sem)
    g_copy = pltpu.make_async_copy(g_hbm, g_v, g_sem)

    def dot(lhs, rhs):
        return jnp.dot(lhs, rhs, preferred_element_type=F32)

    for q in range(3):
        if q == 0:
            a_copy(0).wait()
            w0_copy(0).wait()
            for i in range(1, DEPTH):
                w_start(i)
        elif q == 1:
            w0_copy(1).wait()
        else:
            a_copy(1).wait()
            w_start(DEPTH)
        r_sl, c_sl = far_parts[q]
        part[FAR, r_sl, c_sl] = dot(a_v[r_sl, :], w_v[0, :, c_sl]).astype(BF16)
        if q == 0:
            pl.semaphore_wait(barrier, 3)
        far_copy(q, core).start()

    def chunk(i, col):
        w_copy(i, col).wait()
        w_start(i + DEPTH)
        return dot(a_v[...], w_v[i])

    def columns(j):
        return pl.ds(pl.multiple_of(j * CW, CW), CW)

    for j in range(1, N_COL):
        part[FAR, :, columns(j)] = chunk(j, cross_col(j)).astype(BF16)
        far_copy(2 + j, core).start()

    @pl.loop(N_COL, per)
    def _(j):
        part[FAR, :, columns(j)] = chunk(j, cross_col(j)).astype(BF16)

    far_copy(len(far_parts) - 1, core).start()

    @pl.loop(0, per)
    def _(j):
        part[NEAR, :, columns(j)] = chunk(per + j, cross_col(per + j)).astype(BF16)

    for b in range(n_blk - 1):
        near_copy(b, core).start()

    @pl.when(core == 0)
    def _():
        last_sib_copy().start()

    r_copy.start()
    g_copy.start()

    @pl.loop(0, per)
    def _(j):
        part[SIB, :, columns(j)] = chunk(2 * per + j, home_col(j)).astype(BF16)

    sib_copy().start()

    @pl.when(core == 1)
    def _():
        last_sib_copy().wait_recv()
        last_tx[...] = part[NEAR, last, :].astype(F32) + last_sib[...].astype(F32)
        last_copy().start()

    @pl.loop(0, per)
    def _(j):
        own[:, columns(j)] = chunk(3 * per + j, home_col(per + j))

    r_copy.wait()
    g_copy.wait()
    sib_copy().wait_recv()

    @pl.when(core == 0)
    def _():
        for q in range(len(far_parts)):
            for slot in range(2):
                far_copy(q, slot).wait_recv()
        last_rx[...] = recv[0, last, :].astype(F32) + recv[1, last, :].astype(F32)

    lane = lax.broadcasted_iota(jnp.int32, (8, 128), 1)
    sub = lax.broadcasted_iota(jnp.int32, (8, 128), 0)

    def reduce_block(b):
        @pl.when(core == 1)
        def _():
            if b == n_blk - 1:
                last_copy().wait_recv()
            else:
                for slot in range(2):
                    near_copy(b, slot).wait_recv()

        row, n = blocks[b]
        line = jnp.zeros((8, 128), F32)
        for first in range(0, n, SUB):
            sl = pl.ds(row + first, SUB)
            if b == n_blk - 1:
                off_chip = last_rx[pl.ds(first, SUB), :]
            else:
                off_chip = recv[0, sl, :].astype(F32) + recv[1, sl, :].astype(F32)
            h = r_v[sl, :].astype(F32) + ((own[sl, :] + recv[SIB, sl, :].astype(F32)) + off_chip)
            own[sl, :] = h
            hid[sl, :] = h.astype(BF16)
            s = jnp.sum(h * h, axis=1, keepdims=True)
            for q in range(0, SUB, 8):
                line = line + jnp.where(lane == sub + (first + q), s[q:q + 8, :], 0.0)
        st_tx[b] = jnp.sum(line, axis=0, keepdims=True)
        for k in range(3):
            stat_copy(k, b, SIB if k == SIB else core).start()

    def norm_block(b):
        for slot in range(3):
            stat_copy(slot, b, slot).wait_recv()
        row, n = blocks[b]
        tot = (st_tx[b] + st_rx[SIB, b]) + (st_rx[0, b] + st_rx[1, b])
        scale = jnp.broadcast_to(lax.rsqrt(tot / d_model + EPS), (8, 128))
        for first in range(0, n, SUB):
            for q in range(first, first + SUB, 8):
                sl = pl.ds(row + q, 8)
                col = jnp.sum(jnp.where(lane == sub + q, scale, 0.0), axis=1, keepdims=True)
                own[sl, :] = own[sl, :] * col * g_v[...]
            sl = pl.ds(row + first, SUB)
            nrm[sl, :] = own[sl, :].astype(BF16)

    for b in range(n_blk):
        reduce_block(b)

    for b in range(n_blk):
        norm_block(b)

    for q in range(len(far_parts)):
        far_copy(q, core).wait_send()
    for b in range(n_blk - 1):
        near_copy(b, core).wait_send()

    @pl.when(core == 0)
    def _():
        last_sib_copy().wait_send()

    @pl.when(core == 1)
    def _():
        last_copy().wait_send()

    for b in range(n_blk):
        for k in range(3):
            stat_copy(k, b, SIB if k == SIB else core).wait_send()
    sib_copy().wait_send()


def put(hid, nrm, hid_hbm, nrm_hbm, sem):
    n = hid.shape[0] // PUT
    copies = []
    for q in range(PUT):
        sl = pl.ds(q * n, n)
        copies.append(pltpu.make_async_copy(hid.at[sl, :], hid_hbm.at[sl, :], sem.at[0, q]))
        copies.append(pltpu.make_async_copy(nrm.at[sl, :], nrm_hbm.at[sl, :], sem.at[1, q]))
    for c in copies:
        c.start()
    for c in copies:
        c.wait()


def solution(mesh):
    tp = mesh.shape["tp"]

    def local_step(a, w, r, g):
        rows, depth = a.shape
        d_loc = r.shape[1]
        per = d_loc // CW
        n_blk = len(BLOCKS)
        hbm = pl.BlockSpec(memory_space=pltpu.HBM)
        vmem = pl.BlockSpec(memory_space=pltpu.VMEM)
        dma = pltpu.SemaphoreType.DMA
        hid, nrm = pl.pallas_call(
            functools.partial(kernel, d_loc * tp),
            out_shape=(pltpu.VMEM((rows, d_loc), BF16),) * 2,
            in_specs=[hbm] * 4,
            out_specs=(vmem,) * 2,
            scratch_shapes=[
                pltpu.VMEM((rows, depth), BF16),
                pltpu.VMEM((4 * per, depth, CW), BF16),
                pltpu.VMEM((rows, d_loc), BF16),
                pltpu.VMEM((1, d_loc), F32),
                pltpu.VMEM((3, rows, d_loc), BF16),
                pltpu.VMEM((3, rows, d_loc), BF16),
                pltpu.VMEM((rows, d_loc), F32),
                pltpu.VMEM((BLOCKS[-1], d_loc), BF16),
                pltpu.VMEM((BLOCKS[-1], d_loc), F32),
                pltpu.VMEM((BLOCKS[-1], d_loc), F32),
                pltpu.VMEM((n_blk, 1, 128), F32),
                pltpu.VMEM((3, n_blk, 1, 128), F32),
                dma((2,)), dma((2,)), dma((4 * per,)), dma, dma,
                dma((N_COL + 3,)), dma((2, N_COL + 3)), dma((n_blk - 1,)), dma((2, n_blk - 1)), dma((4,)), dma, dma,
                dma((3, n_blk)), dma((3, n_blk)),
            ],
            compiler_params=pltpu.CompilerParams(
                collective_id=0, has_side_effects=True, vmem_limit_bytes=64946176),
            cost_estimate=pl.CostEstimate(flops=2 * rows * depth * d_loc * tp, transcendentals=0,
                                          bytes_accessed=2 * depth * d_loc * tp),
        )(a, w, r, g.reshape(1, d_loc))
        return pl.pallas_call(
            put,
            out_shape=(jax.ShapeDtypeStruct((rows, d_loc), BF16),) * 2,
            in_specs=[vmem] * 2,
            out_specs=(hbm,) * 2,
            scratch_shapes=[dma((2, PUT))],
            compiler_params=pltpu.CompilerParams(vmem_limit_bytes=1024 * 1024),
        )(hid, nrm)

    return jax.shard_map(
        local_step,
        mesh=mesh,
        in_specs=(P("data", "tp"), P("tp", None), P("data", "tp"), P("tp")),
        out_specs=(P("data", "tp"), P("data", "tp")),
        check_vma=False,
    )
```

```python
import functools

import jax
import jax.numpy as jnp
from jax import lax
from jax.experimental import pallas as pl
from jax.experimental.pallas import tpu as pltpu
from jax.sharding import PartitionSpec as P

EPS = 1e-5
MESH = pl.DeviceIdType.MESH
F32, BF16 = jnp.float32, jnp.bfloat16

CW = 256
N_COL = 2
BLOCKS = (128, 16, 96, 16)
MID = 1
SUB = 16
DEPTH = 4
PUT = 1
FAR, NEAR, SIB = 0, 1, 2


def kernel(d_model, a_hbm, w_hbm, r_hbm, g_hbm, hid, nrm,
           a_v, w_v, r_v, g_v, part, recv, own, mid_sib, mid_tx, mid_rx, st_tx, st_rx,
           a_sem, w0_sem, w_sem, r_sem, g_sem, far_tx, far_rx, near_tx, near_rx, mid_sems, sib_tx, sib_rx, stat_tx, stat_rx):
    t = lax.axis_index("tp")
    core, chip = t % 2, t // 2
    rows, _ = a_v.shape
    d_loc = own.shape[1]
    per = d_loc // CW
    n_blk = len(BLOCKS)
    blocks = [(sum(BLOCKS[:b]), BLOCKS[b]) for b in range(n_blk)]
    half, lanes = rows // 2, 128
    far, near, sib = 2 - 2 * chip, 3 - 2 * chip, t + 1 - 2 * core

    def cross_col(i):
        return (far + i // per) * d_loc + (i % per) * CW

    def home_col(i):
        return (sib + (t - sib) * (i // per)) * d_loc + (i % per) * CW

    def w_copy(i, col):
        return pltpu.make_async_copy(w_hbm.at[:, pl.ds(pl.multiple_of(col, CW), CW)], w_v.at[i], w_sem.at[i])

    def w_start(i):
        if isinstance(i, int):
            w_copy(i, cross_col(i) if i < 2 * per else home_col(i - 2 * per)).start()
            return

        @pl.when(i < 2 * per)
        def _():
            w_copy(i, cross_col(i)).start()

        @pl.when((i >= 2 * per) & (i < 4 * per))
        def _():
            w_copy(i, home_col(i - 2 * per)).start()

    def a_copy(q):
        sl = pl.ds(q * half, half)
        return pltpu.make_async_copy(a_hbm.at[sl, :], a_v.at[sl, :], a_sem.at[q])

    def w0_copy(q):
        src = w_hbm.at[:, pl.ds(pl.multiple_of(far * d_loc + q * lanes, lanes), lanes)]
        return pltpu.make_async_copy(src, w_v.at[0, :, pl.ds(q * lanes, lanes)], w0_sem.at[q])

    def remote(src, dst, tx, rx, peer):
        return pltpu.make_async_remote_copy(src_ref=src, dst_ref=dst, send_sem=tx, recv_sem=rx,
                                            device_id={"tp": peer}, device_id_type=MESH)

    every = pl.ds(0, rows)
    far_parts = [(pl.ds(0, half), pl.ds(0, lanes)), (pl.ds(0, half), pl.ds(lanes, lanes)), (pl.ds(half, half), pl.ds(0, CW))]
    far_parts += [(every, pl.ds(j * CW, CW)) for j in range(1, N_COL)]
    far_parts += [(every, pl.ds(N_COL * CW, d_loc - N_COL * CW))]

    def far_copy(q, slot):
        sl = far_parts[q]
        return remote(part.at[(FAR, *sl)], recv.at[(slot, *sl)], far_tx.at[q], far_rx.at[slot, q], far)

    def near_copy(b, slot):
        sl = pl.ds(*blocks[b])
        return remote(part.at[NEAR, sl, :], recv.at[slot, sl, :], near_tx.at[b], near_rx.at[slot, b], near)

    mid = pl.ds(*blocks[MID])

    def mid_sib_copy():
        return remote(part.at[NEAR, mid, :], mid_sib, mid_sems.at[0], mid_sems.at[1], sib)

    def mid_copy():
        return remote(mid_tx, mid_rx, mid_sems.at[2], mid_sems.at[3], near)

    def sib_copy():
        return remote(part.at[SIB], recv.at[SIB], sib_tx, sib_rx, sib)

    def stat_copy(k, b, slot):
        return remote(st_tx.at[b], st_rx.at[slot, b], stat_tx.at[k, b], stat_rx.at[slot, b], (far, near, sib)[k])

    barrier = pltpu.get_barrier_semaphore()
    for p in (far, near, sib):
        pl.semaphore_signal(barrier, inc=1, device_id={"tp": p}, device_id_type=MESH)
    a_copy(0).start()
    w0_copy(0).start()
    w0_copy(1).start()
    a_copy(1).start()
    r_copy = pltpu.make_async_copy(r_hbm, r_v, r_sem)
    g_copy = pltpu.make_async_copy(g_hbm, g_v, g_sem)

    def dot(lhs, rhs):
        return jnp.dot(lhs, rhs, preferred_element_type=F32)

    for q in range(3):
        if q == 0:
            a_copy(0).wait()
            w0_copy(0).wait()
            for i in range(1, DEPTH):
                w_start(i)
        elif q == 1:
            w0_copy(1).wait()
        else:
            a_copy(1).wait()
            w_start(DEPTH)
        r_sl, c_sl = far_parts[q]
        part[FAR, r_sl, c_sl] = dot(a_v[r_sl, :], w_v[0, :, c_sl]).astype(BF16)
        if q == 0:
            pl.semaphore_wait(barrier, 3)
        far_copy(q, core).start()

    def chunk(i, col):
        w_copy(i, col).wait()
        w_start(i + DEPTH)
        return dot(a_v[...], w_v[i])

    def columns(j):
        return pl.ds(pl.multiple_of(j * CW, CW), CW)

    for j in range(1, N_COL):
        part[FAR, :, columns(j)] = chunk(j, cross_col(j)).astype(BF16)
        far_copy(2 + j, core).start()

    @pl.loop(N_COL, per)
    def _(j):
        part[FAR, :, columns(j)] = chunk(j, cross_col(j)).astype(BF16)

    far_copy(len(far_parts) - 1, core).start()

    @pl.loop(0, per)
    def _(j):
        part[NEAR, :, columns(j)] = chunk(per + j, cross_col(per + j)).astype(BF16)

    plain = [b for b in range(n_blk) if b != MID]

    @pl.when(core == 0)
    def _():
        for b in plain:
            near_copy(b, core).start()
        mid_sib_copy().start()

    @pl.when(core == 1)
    def _():
        near_copy(0, core).start()

    r_copy.start()
    g_copy.start()

    @pl.loop(0, per)
    def _(j):
        part[SIB, :, columns(j)] = chunk(2 * per + j, home_col(j)).astype(BF16)

    sib_copy().start()

    @pl.when(core == 1)
    def _():
        mid_sib_copy().wait_recv()
        mid_tx[...] = part[NEAR, mid, :].astype(F32) + mid_sib[...].astype(F32)
        mid_copy().start()
        for b in plain[1:]:
            near_copy(b, core).start()

    @pl.loop(0, per)
    def _(j):
        own[:, columns(j)] = chunk(3 * per + j, home_col(per + j))

    r_copy.wait()
    g_copy.wait()
    sib_copy().wait_recv()

    @pl.when(core == 0)
    def _():
        for q in range(len(far_parts)):
            for slot in range(2):
                far_copy(q, slot).wait_recv()
        mid_rx[...] = recv[0, mid, :].astype(F32) + recv[1, mid, :].astype(F32)

    lane = lax.broadcasted_iota(jnp.int32, (8, 128), 1)
    sub = lax.broadcasted_iota(jnp.int32, (8, 128), 0)

    def reduce_block(b):
        @pl.when(core == 1)
        def _():
            if b == MID:
                mid_copy().wait_recv()
            else:
                for slot in range(2):
                    near_copy(b, slot).wait_recv()

        row, n = blocks[b]
        line = jnp.zeros((8, 128), F32)
        for first in range(0, n, SUB):
            sl = pl.ds(row + first, SUB)
            if b == MID:
                off_chip = mid_rx[pl.ds(first, SUB), :]
            else:
                off_chip = recv[0, sl, :].astype(F32) + recv[1, sl, :].astype(F32)
            h = r_v[sl, :].astype(F32) + ((own[sl, :] + recv[SIB, sl, :].astype(F32)) + off_chip)
            own[sl, :] = h
            hid[sl, :] = h.astype(BF16)
            s = jnp.sum(h * h, axis=1, keepdims=True)
            for q in range(0, SUB, 8):
                line = line + jnp.where(lane == sub + (first + q), s[q:q + 8, :], 0.0)
        st_tx[b] = jnp.sum(line, axis=0, keepdims=True)
        for k in range(3):
            stat_copy(k, b, SIB if k == SIB else core).start()

    def norm_block(b):
        for slot in range(3):
            stat_copy(slot, b, slot).wait_recv()
        row, n = blocks[b]
        tot = (st_tx[b] + st_rx[SIB, b]) + (st_rx[0, b] + st_rx[1, b])
        scale = jnp.broadcast_to(lax.rsqrt(tot / d_model + EPS), (8, 128))
        for first in range(0, n, SUB):
            for q in range(first, first + SUB, 8):
                sl = pl.ds(row + q, 8)
                col = jnp.sum(jnp.where(lane == sub + q, scale, 0.0), axis=1, keepdims=True)
                own[sl, :] = own[sl, :] * col * g_v[...]
            sl = pl.ds(row + first, SUB)
            nrm[sl, :] = own[sl, :].astype(BF16)

    for b in range(n_blk):
        reduce_block(b)

    for b in range(n_blk):
        norm_block(b)

    for q in range(len(far_parts)):
        far_copy(q, core).wait_send()
    for b in plain:
        near_copy(b, core).wait_send()

    @pl.when(core == 0)
    def _():
        mid_sib_copy().wait_send()

    @pl.when(core == 1)
    def _():
        mid_copy().wait_send()

    for b in range(n_blk):
        for k in range(3):
            stat_copy(k, b, SIB if k == SIB else core).wait_send()
    sib_copy().wait_send()


def put(hid, nrm, hid_hbm, nrm_hbm, sem):
    n = hid.shape[0] // PUT
    copies = []
    for q in range(PUT):
        sl = pl.ds(q * n, n)
        copies.append(pltpu.make_async_copy(hid.at[sl, :], hid_hbm.at[sl, :], sem.at[0, q]))
        copies.append(pltpu.make_async_copy(nrm.at[sl, :], nrm_hbm.at[sl, :], sem.at[1, q]))
    for c in copies:
        c.start()
    for c in copies:
        c.wait()


def solution(mesh):
    tp = mesh.shape["tp"]

    def local_step(a, w, r, g):
        rows, depth = a.shape
        d_loc = r.shape[1]
        per = d_loc // CW
        n_blk = len(BLOCKS)
        hbm = pl.BlockSpec(memory_space=pltpu.HBM)
        vmem = pl.BlockSpec(memory_space=pltpu.VMEM)
        dma = pltpu.SemaphoreType.DMA
        hid, nrm = pl.pallas_call(
            functools.partial(kernel, d_loc * tp),
            out_shape=(pltpu.VMEM((rows, d_loc), BF16),) * 2,
            in_specs=[hbm] * 4,
            out_specs=(vmem,) * 2,
            scratch_shapes=[
                pltpu.VMEM((rows, depth), BF16),
                pltpu.VMEM((4 * per, depth, CW), BF16),
                pltpu.VMEM((rows, d_loc), BF16),
                pltpu.VMEM((1, d_loc), F32),
                pltpu.VMEM((3, rows, d_loc), BF16),
                pltpu.VMEM((3, rows, d_loc), BF16),
                pltpu.VMEM((rows, d_loc), F32),
                pltpu.VMEM((BLOCKS[MID], d_loc), BF16),
                pltpu.VMEM((BLOCKS[MID], d_loc), F32),
                pltpu.VMEM((BLOCKS[MID], d_loc), F32),
                pltpu.VMEM((n_blk, 1, 128), F32),
                pltpu.VMEM((3, n_blk, 1, 128), F32),
                dma((2,)), dma((2,)), dma((4 * per,)), dma, dma,
                dma((N_COL + 3,)), dma((2, N_COL + 3)), dma((n_blk,)), dma((2, n_blk)), dma((4,)), dma, dma,
                dma((3, n_blk)), dma((3, n_blk)),
            ],
            compiler_params=pltpu.CompilerParams(
                collective_id=0, has_side_effects=True, vmem_limit_bytes=64946176),
            cost_estimate=pl.CostEstimate(flops=2 * rows * depth * d_loc * tp, transcendentals=0,
                                          bytes_accessed=2 * depth * d_loc * tp),
        )(a, w, r, g.reshape(1, d_loc))
        return pl.pallas_call(
            put,
            out_shape=(jax.ShapeDtypeStruct((rows, d_loc), BF16),) * 2,
            in_specs=[vmem] * 2,
            out_specs=(hbm,) * 2,
            scratch_shapes=[dma((2, PUT))],
            compiler_params=pltpu.CompilerParams(vmem_limit_bytes=1024 * 1024),
        )(hid, nrm)

    return jax.shard_map(
        local_step,
        mesh=mesh,
        in_specs=(P("data", "tp"), P("tp", None), P("data", "tp"), P("tp")),
        out_specs=(P("data", "tp"), P("data", "tp")),
        check_vma=False,
    )
```

```python
import functools

import jax
import jax.numpy as jnp
from jax import lax
from jax.experimental import pallas as pl
from jax.experimental.pallas import tpu as pltpu
from jax.sharding import PartitionSpec as P

EPS = 1e-5
MESH = pl.DeviceIdType.MESH
F32, BF16 = jnp.float32, jnp.bfloat16

CW = 256
N_COL = 1
BLOCKS = (128, 112, 16)
NEAR_ROWS = (240, 16)
SUB = 16
DEPTH = 4
PUT = 1
FAR, NEAR, SIB = 0, 1, 2


def kernel(d_model, a_hbm, w_hbm, r_hbm, g_hbm, hid, nrm,
           a_v, w_v, r_v, g_v, part, recv, own, st_tx, st_rx,
           a_sem, w0_sem, w_sem, r_sem, g_sem, far_tx, far_rx, near_tx, near_rx, sib_tx, sib_rx, stat_tx, stat_rx):
    t = lax.axis_index("tp")
    core, chip = t % 2, t // 2
    rows, _ = a_v.shape
    d_loc = own.shape[1]
    per = d_loc // CW
    n_blk = len(BLOCKS)
    blocks = [(sum(BLOCKS[:b]), BLOCKS[b]) for b in range(n_blk)]
    half, lanes = rows // 2, 128
    far, near, sib = 2 - 2 * chip, 3 - 2 * chip, t + 1 - 2 * core

    def cross_col(i):
        return (far + i // per) * d_loc + (i % per) * CW

    def home_col(i):
        return (sib + (t - sib) * (i // per)) * d_loc + (i % per) * CW

    def w_copy(i, col):
        return pltpu.make_async_copy(w_hbm.at[:, pl.ds(pl.multiple_of(col, CW), CW)], w_v.at[i], w_sem.at[i])

    def w_start(i):
        if isinstance(i, int):
            w_copy(i, cross_col(i) if i < 2 * per else home_col(i - 2 * per)).start()
            return

        @pl.when(i < 2 * per)
        def _():
            w_copy(i, cross_col(i)).start()

        @pl.when((i >= 2 * per) & (i < 4 * per))
        def _():
            w_copy(i, home_col(i - 2 * per)).start()

    def a_copy(q):
        sl = pl.ds(q * half, half)
        return pltpu.make_async_copy(a_hbm.at[sl, :], a_v.at[sl, :], a_sem.at[q])

    def w0_copy(q):
        src = w_hbm.at[:, pl.ds(pl.multiple_of(far * d_loc + q * lanes, lanes), lanes)]
        return pltpu.make_async_copy(src, w_v.at[0, :, pl.ds(q * lanes, lanes)], w0_sem.at[q])

    def remote(src, dst, tx, rx, peer):
        return pltpu.make_async_remote_copy(src_ref=src, dst_ref=dst, send_sem=tx, recv_sem=rx,
                                            device_id={"tp": peer}, device_id_type=MESH)

    every = pl.ds(0, rows)
    far_parts = [(pl.ds(0, half), pl.ds(0, lanes)), (pl.ds(0, half), pl.ds(lanes, lanes)), (pl.ds(half, half), pl.ds(0, CW))]
    far_parts += [(every, pl.ds(j * CW, CW)) for j in range(1, N_COL)]
    far_parts += [(every, pl.ds(N_COL * CW, d_loc - N_COL * CW))]

    def far_copy(q, slot):
        sl = far_parts[q]
        return remote(part.at[(FAR, *sl)], recv.at[(slot, *sl)], far_tx.at[q], far_rx.at[slot, q], far)

    near_blocks = [(sum(NEAR_ROWS[:b]), NEAR_ROWS[b]) for b in range(len(NEAR_ROWS))]

    def near_copy(b, slot):
        sl = pl.ds(*near_blocks[b])
        return remote(part.at[NEAR, sl, :], recv.at[slot, sl, :], near_tx.at[b], near_rx.at[slot, b], near)

    def sib_copy():
        return remote(part.at[SIB], recv.at[SIB], sib_tx, sib_rx, sib)

    def stat_copy(k, b, slot):
        return remote(st_tx.at[b], st_rx.at[slot, b], stat_tx.at[k, b], stat_rx.at[slot, b], (far, near, sib)[k])

    barrier = pltpu.get_barrier_semaphore()
    for p in (far, near, sib):
        pl.semaphore_signal(barrier, inc=1, device_id={"tp": p}, device_id_type=MESH)
    a_copy(0).start()
    w0_copy(0).start()
    w0_copy(1).start()
    a_copy(1).start()
    r_copy = pltpu.make_async_copy(r_hbm, r_v, r_sem)
    g_copy = pltpu.make_async_copy(g_hbm, g_v, g_sem)

    def dot(lhs, rhs):
        return jnp.dot(lhs, rhs, preferred_element_type=F32)

    for q in range(3):
        if q == 0:
            a_copy(0).wait()
            w0_copy(0).wait()
            for i in range(1, DEPTH):
                w_start(i)
        elif q == 1:
            w0_copy(1).wait()
        else:
            a_copy(1).wait()
            w_start(DEPTH)
        r_sl, c_sl = far_parts[q]
        part[FAR, r_sl, c_sl] = dot(a_v[r_sl, :], w_v[0, :, c_sl]).astype(BF16)
        if q == 0:
            pl.semaphore_wait(barrier, 3)
        far_copy(q, core).start()

    def chunk(i, col):
        w_copy(i, col).wait()
        w_start(i + DEPTH)
        return dot(a_v[...], w_v[i])

    def columns(j):
        return pl.ds(pl.multiple_of(j * CW, CW), CW)

    for j in range(1, N_COL):
        part[FAR, :, columns(j)] = chunk(j, cross_col(j)).astype(BF16)
        far_copy(2 + j, core).start()

    @pl.loop(N_COL, per)
    def _(j):
        part[FAR, :, columns(j)] = chunk(j, cross_col(j)).astype(BF16)

    far_copy(len(far_parts) - 1, core).start()

    @pl.loop(0, per)
    def _(j):
        part[NEAR, :, columns(j)] = chunk(per + j, cross_col(per + j)).astype(BF16)

    for b in range(len(NEAR_ROWS)):
        near_copy(b, core).start()
    r_copy.start()
    g_copy.start()

    @pl.loop(0, per)
    def _(j):
        part[SIB, :, columns(j)] = chunk(2 * per + j, home_col(j)).astype(BF16)

    sib_copy().start()

    @pl.loop(0, per)
    def _(j):
        own[:, columns(j)] = chunk(3 * per + j, home_col(per + j))

    r_copy.wait()
    g_copy.wait()
    sib_copy().wait_recv()

    @pl.when(core == 0)
    def _():
        for q in range(len(far_parts)):
            for slot in range(2):
                far_copy(q, slot).wait_recv()

    lane = lax.broadcasted_iota(jnp.int32, (8, 128), 1)
    sub = lax.broadcasted_iota(jnp.int32, (8, 128), 0)

    def reduce_block(b):
        row, n = blocks[b]
        if row in [first for first, _ in near_blocks]:
            @pl.when(core == 1)
            def _():
                for slot in range(2):
                    near_copy([first for first, _ in near_blocks].index(row), slot).wait_recv()

        line = jnp.zeros((8, 128), F32)
        for first in range(0, n, SUB):
            sl = pl.ds(row + first, SUB)
            h = own[sl, :] + recv[SIB, sl, :].astype(F32) + recv[0, sl, :].astype(F32) + recv[1, sl, :].astype(F32)
            h = r_v[sl, :].astype(F32) + h
            own[sl, :] = h
            hid[sl, :] = h.astype(BF16)
            s = jnp.sum(h * h, axis=1, keepdims=True)
            for q in range(0, SUB, 8):
                line = line + jnp.where(lane == sub + (first + q), s[q:q + 8, :], 0.0)
        st_tx[b] = jnp.sum(line, axis=0, keepdims=True)
        for k in range(3):
            stat_copy(k, b, SIB if k == SIB else core).start()

    def norm_block(b):
        for slot in range(3):
            stat_copy(slot, b, slot).wait_recv()
        row, n = blocks[b]
        tot = (st_tx[b] + st_rx[SIB, b]) + (st_rx[0, b] + st_rx[1, b])
        scale = jnp.broadcast_to(lax.rsqrt(tot / d_model + EPS), (8, 128))
        for first in range(0, n, SUB):
            for q in range(first, first + SUB, 8):
                sl = pl.ds(row + q, 8)
                col = jnp.sum(jnp.where(lane == sub + q, scale, 0.0), axis=1, keepdims=True)
                own[sl, :] = own[sl, :] * col * g_v[...]
            sl = pl.ds(row + first, SUB)
            nrm[sl, :] = own[sl, :].astype(BF16)

    for b in range(n_blk):
        reduce_block(b)

    for b in range(n_blk):
        norm_block(b)

    for q in range(len(far_parts)):
        far_copy(q, core).wait_send()
    for b in range(len(NEAR_ROWS)):
        near_copy(b, core).wait_send()
    for b in range(n_blk):
        for k in range(3):
            stat_copy(k, b, SIB if k == SIB else core).wait_send()
    sib_copy().wait_send()


def put(hid, nrm, hid_hbm, nrm_hbm, sem):
    n = hid.shape[0] // PUT
    copies = []
    for q in range(PUT):
        sl = pl.ds(q * n, n)
        copies.append(pltpu.make_async_copy(hid.at[sl, :], hid_hbm.at[sl, :], sem.at[0, q]))
        copies.append(pltpu.make_async_copy(nrm.at[sl, :], nrm_hbm.at[sl, :], sem.at[1, q]))
    for c in copies:
        c.start()
    for c in copies:
        c.wait()


def solution(mesh):
    tp = mesh.shape["tp"]

    def local_step(a, w, r, g):
        rows, depth = a.shape
        d_loc = r.shape[1]
        per = d_loc // CW
        n_blk = len(BLOCKS)
        hbm = pl.BlockSpec(memory_space=pltpu.HBM)
        vmem = pl.BlockSpec(memory_space=pltpu.VMEM)
        dma = pltpu.SemaphoreType.DMA
        hid, nrm = pl.pallas_call(
            functools.partial(kernel, d_loc * tp),
            out_shape=(pltpu.VMEM((rows, d_loc), BF16),) * 2,
            in_specs=[hbm] * 4,
            out_specs=(vmem,) * 2,
            scratch_shapes=[
                pltpu.VMEM((rows, depth), BF16),
                pltpu.VMEM((4 * per, depth, CW), BF16),
                pltpu.VMEM((rows, d_loc), BF16),
                pltpu.VMEM((1, d_loc), F32),
                pltpu.VMEM((3, rows, d_loc), BF16),
                pltpu.VMEM((3, rows, d_loc), BF16),
                pltpu.VMEM((rows, d_loc), F32),
                pltpu.VMEM((n_blk, 1, 128), F32),
                pltpu.VMEM((3, n_blk, 1, 128), F32),
                dma((2,)), dma((2,)), dma((4 * per,)), dma, dma,
                dma((N_COL + 3,)), dma((2, N_COL + 3)), dma((len(NEAR_ROWS),)), dma((2, len(NEAR_ROWS))), dma, dma,
                dma((3, n_blk)), dma((3, n_blk)),
            ],
            compiler_params=pltpu.CompilerParams(
                collective_id=0, has_side_effects=True, vmem_limit_bytes=64946176),
            cost_estimate=pl.CostEstimate(flops=2 * rows * depth * d_loc * tp, transcendentals=0,
                                          bytes_accessed=2 * depth * d_loc * tp),
        )(a, w, r, g.reshape(1, d_loc))
        return pl.pallas_call(
            put,
            out_shape=(jax.ShapeDtypeStruct((rows, d_loc), BF16),) * 2,
            in_specs=[vmem] * 2,
            out_specs=(hbm,) * 2,
            scratch_shapes=[dma((2, PUT))],
            compiler_params=pltpu.CompilerParams(vmem_limit_bytes=1024 * 1024),
        )(hid, nrm)

    return jax.shard_map(
        local_step,
        mesh=mesh,
        in_specs=(P("data", "tp"), P("tp", None), P("data", "tp"), P("tp")),
        out_specs=(P("data", "tp"), P("data", "tp")),
        check_vma=False,
    )
```

```python
import functools

import jax
import jax.numpy as jnp
from jax import lax
from jax.experimental import pallas as pl
from jax.experimental.pallas import tpu as pltpu
from jax.sharding import PartitionSpec as P

EPS = 1e-5
MESH = pl.DeviceIdType.MESH
F32, BF16 = jnp.float32, jnp.bfloat16

CW = 256
N_COL = 2
BLOCKS = (128, 112, 16)
NEAR_ROWS = (240, 16)
SUB = 16
DEPTH = 4
PUT = 1
FAR, NEAR, SIB = 0, 1, 2


def kernel(d_model, a_hbm, w_hbm, r_hbm, g_hbm, hid, nrm,
           a_v, w_v, r_v, g_v, part, recv, own, st_tx, st_rx,
           a_sem, w0_sem, w_sem, r_sem, g_sem, far_tx, far_rx, near_tx, near_rx, sib_tx, sib_rx, stat_tx, stat_rx):
    t = lax.axis_index("tp")
    core, chip = t % 2, t // 2
    rows, _ = a_v.shape
    d_loc = own.shape[1]
    per = d_loc // CW
    n_blk = len(BLOCKS)
    blocks = [(sum(BLOCKS[:b]), BLOCKS[b]) for b in range(n_blk)]
    half, lanes = rows // 2, 128
    far, near, sib = 2 - 2 * chip, 3 - 2 * chip, t + 1 - 2 * core

    def cross_col(i):
        return (far + i // per) * d_loc + (i % per) * CW

    def home_col(i):
        return (sib + (t - sib) * (i // per)) * d_loc + (i % per) * CW

    def w_copy(i, col):
        return pltpu.make_async_copy(w_hbm.at[:, pl.ds(pl.multiple_of(col, CW), CW)], w_v.at[i], w_sem.at[i])

    def w_start(i):
        if isinstance(i, int):
            w_copy(i, cross_col(i) if i < 2 * per else home_col(i - 2 * per)).start()
            return

        @pl.when(i < 2 * per)
        def _():
            w_copy(i, cross_col(i)).start()

        @pl.when((i >= 2 * per) & (i < 4 * per))
        def _():
            w_copy(i, home_col(i - 2 * per)).start()

    def a_copy(q):
        sl = pl.ds(q * half, half)
        return pltpu.make_async_copy(a_hbm.at[sl, :], a_v.at[sl, :], a_sem.at[q])

    def w0_copy(q):
        src = w_hbm.at[:, pl.ds(pl.multiple_of(far * d_loc + q * lanes, lanes), lanes)]
        return pltpu.make_async_copy(src, w_v.at[0, :, pl.ds(q * lanes, lanes)], w0_sem.at[q])

    def remote(src, dst, tx, rx, peer):
        return pltpu.make_async_remote_copy(src_ref=src, dst_ref=dst, send_sem=tx, recv_sem=rx,
                                            device_id={"tp": peer}, device_id_type=MESH)

    every = pl.ds(0, rows)
    far_parts = [(pl.ds(0, half), pl.ds(0, lanes)), (pl.ds(0, half), pl.ds(lanes, lanes)), (pl.ds(half, half), pl.ds(0, CW))]
    far_parts += [(every, pl.ds(j * CW, CW)) for j in range(1, N_COL)]
    far_parts += [(every, pl.ds(N_COL * CW, d_loc - N_COL * CW))]

    def far_copy(q, slot):
        sl = far_parts[q]
        return remote(part.at[(FAR, *sl)], recv.at[(slot, *sl)], far_tx.at[q], far_rx.at[slot, q], far)

    near_blocks = [(sum(NEAR_ROWS[:b]), NEAR_ROWS[b]) for b in range(len(NEAR_ROWS))]

    def near_copy(b, slot):
        sl = pl.ds(*near_blocks[b])
        return remote(part.at[NEAR, sl, :], recv.at[slot, sl, :], near_tx.at[b], near_rx.at[slot, b], near)

    def sib_copy():
        return remote(part.at[SIB], recv.at[SIB], sib_tx, sib_rx, sib)

    def stat_copy(k, b, slot):
        return remote(st_tx.at[b], st_rx.at[slot, b], stat_tx.at[k, b], stat_rx.at[slot, b], (far, near, sib)[k])

    barrier = pltpu.get_barrier_semaphore()
    for p in (far, near, sib):
        pl.semaphore_signal(barrier, inc=1, device_id={"tp": p}, device_id_type=MESH)
    a_copy(0).start()
    w0_copy(0).start()
    w0_copy(1).start()
    a_copy(1).start()
    r_copy = pltpu.make_async_copy(r_hbm, r_v, r_sem)
    g_copy = pltpu.make_async_copy(g_hbm, g_v, g_sem)

    def dot(lhs, rhs):
        return jnp.dot(lhs, rhs, preferred_element_type=F32)

    for q in range(3):
        if q == 0:
            a_copy(0).wait()
            w0_copy(0).wait()
            for i in range(1, DEPTH):
                w_start(i)
        elif q == 1:
            w0_copy(1).wait()
        else:
            a_copy(1).wait()
            w_start(DEPTH)
        r_sl, c_sl = far_parts[q]
        part[FAR, r_sl, c_sl] = dot(a_v[r_sl, :], w_v[0, :, c_sl]).astype(BF16)
        if q == 0:
            pl.semaphore_wait(barrier, 3)
        far_copy(q, core).start()

    def chunk(i, col):
        w_copy(i, col).wait()
        w_start(i + DEPTH)
        return dot(a_v[...], w_v[i])

    def columns(j):
        return pl.ds(pl.multiple_of(j * CW, CW), CW)

    for j in range(1, N_COL):
        part[FAR, :, columns(j)] = chunk(j, cross_col(j)).astype(BF16)
        far_copy(2 + j, core).start()

    @pl.loop(N_COL, per)
    def _(j):
        part[FAR, :, columns(j)] = chunk(j, cross_col(j)).astype(BF16)

    far_copy(len(far_parts) - 1, core).start()

    @pl.loop(0, per)
    def _(j):
        part[NEAR, :, columns(j)] = chunk(per + j, cross_col(per + j)).astype(BF16)

    for b in range(len(NEAR_ROWS)):
        near_copy(b, core).start()
    r_copy.start()
    g_copy.start()

    @pl.loop(0, per)
    def _(j):
        part[SIB, :, columns(j)] = chunk(2 * per + j, home_col(j)).astype(BF16)

    sib_copy().start()

    @pl.loop(0, per)
    def _(j):
        own[:, columns(j)] = chunk(3 * per + j, home_col(per + j))

    r_copy.wait()
    g_copy.wait()
    sib_copy().wait_recv()

    @pl.when(core == 0)
    def _():
        for q in range(len(far_parts)):
            for slot in range(2):
                far_copy(q, slot).wait_recv()

    lane = lax.broadcasted_iota(jnp.int32, (8, 128), 1)
    sub = lax.broadcasted_iota(jnp.int32, (8, 128), 0)

    def reduce_block(b):
        row, n = blocks[b]
        if row in [first for first, _ in near_blocks]:
            @pl.when(core == 1)
            def _():
                for slot in range(2):
                    near_copy([first for first, _ in near_blocks].index(row), slot).wait_recv()

        line = jnp.zeros((8, 128), F32)
        for first in range(0, n, SUB):
            sl = pl.ds(row + first, SUB)
            h = own[sl, :] + recv[SIB, sl, :].astype(F32) + recv[0, sl, :].astype(F32) + recv[1, sl, :].astype(F32)
            h = r_v[sl, :].astype(F32) + h
            own[sl, :] = h
            hid[sl, :] = h.astype(BF16)
            s = jnp.sum(h * h, axis=1, keepdims=True)
            for q in range(0, SUB, 8):
                line = line + jnp.where(lane == sub + (first + q), s[q:q + 8, :], 0.0)
        st_tx[b] = jnp.sum(line, axis=0, keepdims=True)
        for k in range(3):
            stat_copy(k, b, SIB if k == SIB else core).start()

    def norm_block(b):
        for slot in range(3):
            stat_copy(slot, b, slot).wait_recv()
        row, n = blocks[b]
        tot = (st_tx[b] + st_rx[SIB, b]) + (st_rx[0, b] + st_rx[1, b])
        scale = jnp.broadcast_to(lax.rsqrt(tot / d_model + EPS), (8, 128))
        for first in range(0, n, SUB):
            for q in range(first, first + SUB, 8):
                sl = pl.ds(row + q, 8)
                col = jnp.sum(jnp.where(lane == sub + q, scale, 0.0), axis=1, keepdims=True)
                own[sl, :] = own[sl, :] * col * g_v[...]
            sl = pl.ds(row + first, SUB)
            nrm[sl, :] = own[sl, :].astype(BF16)

    for b in range(n_blk):
        reduce_block(b)

    for b in range(n_blk):
        norm_block(b)

    for q in range(len(far_parts)):
        far_copy(q, core).wait_send()
    for b in range(len(NEAR_ROWS)):
        near_copy(b, core).wait_send()
    for b in range(n_blk):
        for k in range(3):
            stat_copy(k, b, SIB if k == SIB else core).wait_send()
    sib_copy().wait_send()


def put(hid, nrm, hid_hbm, nrm_hbm, sem):
    n = hid.shape[0] // PUT
    copies = []
    for q in range(PUT):
        sl = pl.ds(q * n, n)
        copies.append(pltpu.make_async_copy(hid.at[sl, :], hid_hbm.at[sl, :], sem.at[0, q]))
        copies.append(pltpu.make_async_copy(nrm.at[sl, :], nrm_hbm.at[sl, :], sem.at[1, q]))
    for c in copies:
        c.start()
    for c in copies:
        c.wait()


def solution(mesh):
    tp = mesh.shape["tp"]

    def local_step(a, w, r, g):
        rows, depth = a.shape
        d_loc = r.shape[1]
        per = d_loc // CW
        n_blk = len(BLOCKS)
        hbm = pl.BlockSpec(memory_space=pltpu.HBM)
        vmem = pl.BlockSpec(memory_space=pltpu.VMEM)
        dma = pltpu.SemaphoreType.DMA
        hid, nrm = pl.pallas_call(
            functools.partial(kernel, d_loc * tp),
            out_shape=(pltpu.VMEM((rows, d_loc), BF16),) * 2,
            in_specs=[hbm] * 4,
            out_specs=(vmem,) * 2,
            scratch_shapes=[
                pltpu.VMEM((rows, depth), BF16),
                pltpu.VMEM((4 * per, depth, CW), BF16),
                pltpu.VMEM((rows, d_loc), BF16),
                pltpu.VMEM((1, d_loc), F32),
                pltpu.VMEM((3, rows, d_loc), BF16),
                pltpu.VMEM((3, rows, d_loc), BF16),
                pltpu.VMEM((rows, d_loc), F32),
                pltpu.VMEM((n_blk, 1, 128), F32),
                pltpu.VMEM((3, n_blk, 1, 128), F32),
                dma((2,)), dma((2,)), dma((4 * per,)), dma, dma,
                dma((N_COL + 3,)), dma((2, N_COL + 3)), dma((len(NEAR_ROWS),)), dma((2, len(NEAR_ROWS))), dma, dma,
                dma((3, n_blk)), dma((3, n_blk)),
            ],
            compiler_params=pltpu.CompilerParams(
                collective_id=0, has_side_effects=True, vmem_limit_bytes=64946176),
            cost_estimate=pl.CostEstimate(flops=2 * rows * depth * d_loc * tp, transcendentals=0,
                                          bytes_accessed=2 * depth * d_loc * tp),
        )(a, w, r, g.reshape(1, d_loc))
        return pl.pallas_call(
            put,
            out_shape=(jax.ShapeDtypeStruct((rows, d_loc), BF16),) * 2,
            in_specs=[vmem] * 2,
            out_specs=(hbm,) * 2,
            scratch_shapes=[dma((2, PUT))],
            compiler_params=pltpu.CompilerParams(vmem_limit_bytes=1024 * 1024),
        )(hid, nrm)

    return jax.shard_map(
        local_step,
        mesh=mesh,
        in_specs=(P("data", "tp"), P("tp", None), P("data", "tp"), P("tp")),
        out_specs=(P("data", "tp"), P("data", "tp")),
        check_vma=False,
    )
```

```python
import functools

import jax
import jax.numpy as jnp
from jax import lax
from jax.experimental import pallas as pl
from jax.experimental.pallas import tpu as pltpu
from jax.sharding import PartitionSpec as P

EPS = 1e-5
MESH = pl.DeviceIdType.MESH
F32, BF16 = jnp.float32, jnp.bfloat16

CW = 256
N_COL = 2
BLOCKS = (128, 112, 16)
NEAR_ROWS = (96, 144, 16)
MID = 128
SUB = 16
DEPTH = 4
PUT = 1
FAR, NEAR, SIB = 0, 1, 2


def kernel(d_model, a_hbm, w_hbm, r_hbm, g_hbm, hid, nrm,
           a_v, w_v, r_v, g_v, part, recv, own, mid_sib, mid_tx, mid_rx, st_tx, st_rx,
           a_sem, w0_sem, w_sem, r_sem, g_sem, far_tx, far_rx, near_tx, near_rx, mid_sems, sib_tx, sib_rx, stat_tx, stat_rx):
    t = lax.axis_index("tp")
    core, chip = t % 2, t // 2
    rows, _ = a_v.shape
    d_loc = own.shape[1]
    per = d_loc // CW
    n_blk = len(BLOCKS)
    blocks = [(sum(BLOCKS[:b]), BLOCKS[b]) for b in range(n_blk)]
    half, lanes = rows // 2, 128
    far, near, sib = 2 - 2 * chip, 3 - 2 * chip, t + 1 - 2 * core

    def cross_col(i):
        return (far + i // per) * d_loc + (i % per) * CW

    def home_col(i):
        return (sib + (t - sib) * (i // per)) * d_loc + (i % per) * CW

    def w_copy(i, col):
        return pltpu.make_async_copy(w_hbm.at[:, pl.ds(pl.multiple_of(col, CW), CW)], w_v.at[i], w_sem.at[i])

    def w_start(i):
        if isinstance(i, int):
            w_copy(i, cross_col(i) if i < 2 * per else home_col(i - 2 * per)).start()
            return

        @pl.when(i < 2 * per)
        def _():
            w_copy(i, cross_col(i)).start()

        @pl.when((i >= 2 * per) & (i < 4 * per))
        def _():
            w_copy(i, home_col(i - 2 * per)).start()

    def a_copy(q):
        sl = pl.ds(q * half, half)
        return pltpu.make_async_copy(a_hbm.at[sl, :], a_v.at[sl, :], a_sem.at[q])

    def w0_copy(q):
        src = w_hbm.at[:, pl.ds(pl.multiple_of(far * d_loc + q * lanes, lanes), lanes)]
        return pltpu.make_async_copy(src, w_v.at[0, :, pl.ds(q * lanes, lanes)], w0_sem.at[q])

    def remote(src, dst, tx, rx, peer):
        return pltpu.make_async_remote_copy(src_ref=src, dst_ref=dst, send_sem=tx, recv_sem=rx,
                                            device_id={"tp": peer}, device_id_type=MESH)

    every = pl.ds(0, rows)
    far_parts = [(pl.ds(0, half), pl.ds(0, lanes)), (pl.ds(0, half), pl.ds(lanes, lanes)), (pl.ds(half, half), pl.ds(0, CW))]
    far_parts += [(every, pl.ds(j * CW, CW)) for j in range(1, N_COL)]
    far_parts += [(every, pl.ds(N_COL * CW, d_loc - N_COL * CW))]

    def far_copy(q, slot):
        sl = far_parts[q]
        return remote(part.at[(FAR, *sl)], recv.at[(slot, *sl)], far_tx.at[q], far_rx.at[slot, q], far)

    near_blocks = [(sum(NEAR_ROWS[:b]), NEAR_ROWS[b]) for b in range(len(NEAR_ROWS))]

    def near_copy(b, slot):
        sl = (pl.ds(*near_blocks[b]), pl.ds(0, d_loc if b else d_loc - MID))
        return remote(part.at[(NEAR, *sl)], recv.at[(slot, *sl)], near_tx.at[b], near_rx.at[slot, b], near)

    mid = (pl.ds(0, NEAR_ROWS[0]), pl.ds(d_loc - MID, MID))

    def mid_sib_copy():
        return remote(part.at[(NEAR, *mid)], mid_sib, mid_sems.at[0], mid_sems.at[1], sib)

    def mid_copy():
        return remote(mid_tx, mid_rx, mid_sems.at[2], mid_sems.at[3], near)

    def sib_copy():
        return remote(part.at[SIB], recv.at[SIB], sib_tx, sib_rx, sib)

    def stat_copy(k, b, slot):
        return remote(st_tx.at[b], st_rx.at[slot, b], stat_tx.at[k, b], stat_rx.at[slot, b], (far, near, sib)[k])

    barrier = pltpu.get_barrier_semaphore()
    for p in (far, near, sib):
        pl.semaphore_signal(barrier, inc=1, device_id={"tp": p}, device_id_type=MESH)
    a_copy(0).start()
    w0_copy(0).start()
    w0_copy(1).start()
    a_copy(1).start()
    r_copy = pltpu.make_async_copy(r_hbm, r_v, r_sem)
    g_copy = pltpu.make_async_copy(g_hbm, g_v, g_sem)

    def dot(lhs, rhs):
        return jnp.dot(lhs, rhs, preferred_element_type=F32)

    for q in range(3):
        if q == 0:
            a_copy(0).wait()
            w0_copy(0).wait()
            for i in range(1, DEPTH):
                w_start(i)
        elif q == 1:
            w0_copy(1).wait()
        else:
            a_copy(1).wait()
            w_start(DEPTH)
        r_sl, c_sl = far_parts[q]
        part[FAR, r_sl, c_sl] = dot(a_v[r_sl, :], w_v[0, :, c_sl]).astype(BF16)
        if q == 0:
            pl.semaphore_wait(barrier, 3)
        far_copy(q, core).start()

    def chunk(i, col):
        w_copy(i, col).wait()
        w_start(i + DEPTH)
        return dot(a_v[...], w_v[i])

    def columns(j):
        return pl.ds(pl.multiple_of(j * CW, CW), CW)

    for j in range(1, N_COL):
        part[FAR, :, columns(j)] = chunk(j, cross_col(j)).astype(BF16)
        far_copy(2 + j, core).start()

    @pl.loop(N_COL, per)
    def _(j):
        part[FAR, :, columns(j)] = chunk(j, cross_col(j)).astype(BF16)

    far_copy(len(far_parts) - 1, core).start()

    @pl.loop(0, per)
    def _(j):
        part[NEAR, :, columns(j)] = chunk(per + j, cross_col(per + j)).astype(BF16)

    near_copy(0, core).start()

    @pl.when(core == 0)
    def _():
        for b in range(1, len(NEAR_ROWS)):
            near_copy(b, core).start()
        mid_sib_copy().start()

    r_copy.start()
    g_copy.start()

    @pl.loop(0, per)
    def _(j):
        part[SIB, :, columns(j)] = chunk(2 * per + j, home_col(j)).astype(BF16)

    sib_copy().start()

    @pl.when(core == 1)
    def _():
        mid_sib_copy().wait_recv()
        mid_tx[...] = part[(NEAR, *mid)].astype(F32) + mid_sib[...].astype(F32)
        mid_copy().start()
        for b in range(1, len(NEAR_ROWS)):
            near_copy(b, core).start()

    @pl.loop(0, per)
    def _(j):
        own[:, columns(j)] = chunk(3 * per + j, home_col(per + j))

    r_copy.wait()
    g_copy.wait()
    sib_copy().wait_recv()

    @pl.when(core == 0)
    def _():
        for q in range(len(far_parts)):
            for slot in range(2):
                far_copy(q, slot).wait_recv()

    lane = lax.broadcasted_iota(jnp.int32, (8, 128), 1)
    sub = lax.broadcasted_iota(jnp.int32, (8, 128), 0)

    use = [min(b for b in range(n_blk) if blocks[b][0] < first + m and first < sum(blocks[b])) for first, m in near_blocks]

    def reduce_block(b):
        row, n = blocks[b]

        @pl.when(core == 1)
        def _():
            if b == 0:
                mid_copy().wait_recv()
                own[mid] = own[mid] + mid_rx[...]
                for slot in range(2):
                    recv[(slot, *mid)] = jnp.zeros_like(mid_sib)
            for q in range(len(near_blocks)):
                if use[q] == b:
                    for slot in range(2):
                        near_copy(q, slot).wait_recv()

        line = jnp.zeros((8, 128), F32)
        for first in range(0, n, SUB):
            sl = pl.ds(row + first, SUB)
            h = own[sl, :] + recv[SIB, sl, :].astype(F32) + recv[0, sl, :].astype(F32) + recv[1, sl, :].astype(F32)
            h = r_v[sl, :].astype(F32) + h
            own[sl, :] = h
            hid[sl, :] = h.astype(BF16)
            s = jnp.sum(h * h, axis=1, keepdims=True)
            for q in range(0, SUB, 8):
                line = line + jnp.where(lane == sub + (first + q), s[q:q + 8, :], 0.0)
        st_tx[b] = jnp.sum(line, axis=0, keepdims=True)
        for k in range(3):
            stat_copy(k, b, SIB if k == SIB else core).start()

    def norm_block(b):
        for slot in range(3):
            stat_copy(slot, b, slot).wait_recv()
        row, n = blocks[b]
        tot = (st_tx[b] + st_rx[SIB, b]) + (st_rx[0, b] + st_rx[1, b])
        scale = jnp.broadcast_to(lax.rsqrt(tot / d_model + EPS), (8, 128))
        for first in range(0, n, SUB):
            for q in range(first, first + SUB, 8):
                sl = pl.ds(row + q, 8)
                col = jnp.sum(jnp.where(lane == sub + q, scale, 0.0), axis=1, keepdims=True)
                own[sl, :] = own[sl, :] * col * g_v[...]
            sl = pl.ds(row + first, SUB)
            nrm[sl, :] = own[sl, :].astype(BF16)

    for b in range(n_blk):
        reduce_block(b)

    for b in range(n_blk):
        norm_block(b)

    for q in range(len(far_parts)):
        far_copy(q, core).wait_send()
    for b in range(len(NEAR_ROWS)):
        near_copy(b, core).wait_send()

    @pl.when(core == 0)
    def _():
        mid_sib_copy().wait_send()

    @pl.when(core == 1)
    def _():
        mid_copy().wait_send()

    for b in range(n_blk):
        for k in range(3):
            stat_copy(k, b, SIB if k == SIB else core).wait_send()
    sib_copy().wait_send()


def put(hid, nrm, hid_hbm, nrm_hbm, sem):
    n = hid.shape[0] // PUT
    copies = []
    for q in range(PUT):
        sl = pl.ds(q * n, n)
        copies.append(pltpu.make_async_copy(hid.at[sl, :], hid_hbm.at[sl, :], sem.at[0, q]))
        copies.append(pltpu.make_async_copy(nrm.at[sl, :], nrm_hbm.at[sl, :], sem.at[1, q]))
    for c in copies:
        c.start()
    for c in copies:
        c.wait()


def solution(mesh):
    tp = mesh.shape["tp"]

    def local_step(a, w, r, g):
        rows, depth = a.shape
        d_loc = r.shape[1]
        per = d_loc // CW
        n_blk = len(BLOCKS)
        hbm = pl.BlockSpec(memory_space=pltpu.HBM)
        vmem = pl.BlockSpec(memory_space=pltpu.VMEM)
        dma = pltpu.SemaphoreType.DMA
        hid, nrm = pl.pallas_call(
            functools.partial(kernel, d_loc * tp),
            out_shape=(pltpu.VMEM((rows, d_loc), BF16),) * 2,
            in_specs=[hbm] * 4,
            out_specs=(vmem,) * 2,
            scratch_shapes=[
                pltpu.VMEM((rows, depth), BF16),
                pltpu.VMEM((4 * per, depth, CW), BF16),
                pltpu.VMEM((rows, d_loc), BF16),
                pltpu.VMEM((1, d_loc), F32),
                pltpu.VMEM((3, rows, d_loc), BF16),
                pltpu.VMEM((3, rows, d_loc), BF16),
                pltpu.VMEM((rows, d_loc), F32),
                pltpu.VMEM((NEAR_ROWS[0], MID), BF16),
                pltpu.VMEM((NEAR_ROWS[0], MID), F32),
                pltpu.VMEM((NEAR_ROWS[0], MID), F32),
                pltpu.VMEM((n_blk, 1, 128), F32),
                pltpu.VMEM((3, n_blk, 1, 128), F32),
                dma((2,)), dma((2,)), dma((4 * per,)), dma, dma,
                dma((N_COL + 3,)), dma((2, N_COL + 3)), dma((len(NEAR_ROWS),)), dma((2, len(NEAR_ROWS))), dma((4,)), dma, dma,
                dma((3, n_blk)), dma((3, n_blk)),
            ],
            compiler_params=pltpu.CompilerParams(
                collective_id=0, has_side_effects=True, vmem_limit_bytes=64946176),
            cost_estimate=pl.CostEstimate(flops=2 * rows * depth * d_loc * tp, transcendentals=0,
                                          bytes_accessed=2 * depth * d_loc * tp),
        )(a, w, r, g.reshape(1, d_loc))
        return pl.pallas_call(
            put,
            out_shape=(jax.ShapeDtypeStruct((rows, d_loc), BF16),) * 2,
            in_specs=[vmem] * 2,
            out_specs=(hbm,) * 2,
            scratch_shapes=[dma((2, PUT))],
            compiler_params=pltpu.CompilerParams(vmem_limit_bytes=1024 * 1024),
        )(hid, nrm)

    return jax.shard_map(
        local_step,
        mesh=mesh,
        in_specs=(P("data", "tp"), P("tp", None), P("data", "tp"), P("tp")),
        out_specs=(P("data", "tp"), P("data", "tp")),
        check_vma=False,
    )
```

```python
import functools

import jax
import jax.numpy as jnp
from jax import lax
from jax.experimental import pallas as pl
from jax.experimental.pallas import tpu as pltpu
from jax.sharding import PartitionSpec as P

EPS = 1e-5
MESH = pl.DeviceIdType.MESH
F32, BF16 = jnp.float32, jnp.bfloat16

CW = 256
N_COL = 2
BLOCKS = (128, 112, 16)
NEAR_ROWS = (240, 16)
SUB = 16
DEPTH = 4
PUT = 1
FAR, NEAR, SIB = 0, 1, 2


def kernel(d_model, a_hbm, w_hbm, r_hbm, g_hbm, hid, nrm,
           a_v, w_v, r_v, g_v, part, recv, own, st_tx, st_rx,
           a_sem, w_sem, r_sem, g_sem, far_tx, far_rx, near_tx, near_rx, sib_tx, sib_rx, stat_tx, stat_rx):
    t = lax.axis_index("tp")
    core, chip = t % 2, t // 2
    rows, _ = a_v.shape
    d_loc = own.shape[1]
    per = d_loc // CW
    n_blk = len(BLOCKS)
    blocks = [(sum(BLOCKS[:b]), BLOCKS[b]) for b in range(n_blk)]
    far, near, sib = 2 - 2 * chip, 3 - 2 * chip, t + 1 - 2 * core

    def cross_col(i):
        return (far + i // per) * d_loc + (i % per) * CW

    def home_col(i):
        return (sib + (t - sib) * (i // per)) * d_loc + (i % per) * CW

    def w_copy(i, col):
        return pltpu.make_async_copy(w_hbm.at[:, pl.ds(pl.multiple_of(col, CW), CW)], w_v.at[i], w_sem.at[i])

    def w_start(i):
        if isinstance(i, int):
            w_copy(i, cross_col(i) if i < 2 * per else home_col(i - 2 * per)).start()
            return

        @pl.when(i < 2 * per)
        def _():
            w_copy(i, cross_col(i)).start()

        @pl.when((i >= 2 * per) & (i < 4 * per))
        def _():
            w_copy(i, home_col(i - 2 * per)).start()

    a_copy = pltpu.make_async_copy(a_hbm, a_v, a_sem)

    def remote(src, dst, tx, rx, peer):
        return pltpu.make_async_remote_copy(src_ref=src, dst_ref=dst, send_sem=tx, recv_sem=rx,
                                            device_id={"tp": peer}, device_id_type=MESH)

    every = pl.ds(0, rows)
    far_parts = [(every, pl.ds(j * CW, CW)) for j in range(N_COL)]
    far_parts += [(every, pl.ds(N_COL * CW, d_loc - N_COL * CW))]

    def far_copy(q, slot):
        sl = far_parts[q]
        return remote(part.at[(FAR, *sl)], recv.at[(slot, *sl)], far_tx.at[q], far_rx.at[slot, q], far)

    near_blocks = [(sum(NEAR_ROWS[:b]), NEAR_ROWS[b]) for b in range(len(NEAR_ROWS))]

    def near_copy(b, slot):
        sl = pl.ds(*near_blocks[b])
        return remote(part.at[NEAR, sl, :], recv.at[slot, sl, :], near_tx.at[b], near_rx.at[slot, b], near)

    def sib_copy():
        return remote(part.at[SIB], recv.at[SIB], sib_tx, sib_rx, sib)

    def stat_copy(k, b, slot):
        return remote(st_tx.at[b], st_rx.at[slot, b], stat_tx.at[k, b], stat_rx.at[slot, b], (far, near, sib)[k])

    barrier = pltpu.get_barrier_semaphore()
    for p in (far, near, sib):
        pl.semaphore_signal(barrier, inc=1, device_id={"tp": p}, device_id_type=MESH)
    w_start(0)
    a_copy.start()
    for i in range(1, DEPTH):
        w_start(i)
    r_copy = pltpu.make_async_copy(r_hbm, r_v, r_sem)
    g_copy = pltpu.make_async_copy(g_hbm, g_v, g_sem)

    def dot(lhs, rhs):
        return jnp.dot(lhs, rhs, preferred_element_type=F32)

    def chunk(i, col):
        w_copy(i, col).wait()
        w_start(i + DEPTH)
        return dot(a_v[...], w_v[i])

    def columns(j):
        return pl.ds(pl.multiple_of(j * CW, CW), CW)

    for j in range(N_COL):
        if j == 0:
            a_copy.wait()
        part[FAR, :, columns(j)] = chunk(j, cross_col(j)).astype(BF16)
        if j == 0:
            pl.semaphore_wait(barrier, 3)
        far_copy(j, core).start()

    @pl.loop(N_COL, per)
    def _(j):
        part[FAR, :, columns(j)] = chunk(j, cross_col(j)).astype(BF16)

    far_copy(len(far_parts) - 1, core).start()

    @pl.loop(0, per)
    def _(j):
        part[NEAR, :, columns(j)] = chunk(per + j, cross_col(per + j)).astype(BF16)

    for b in range(len(NEAR_ROWS)):
        near_copy(b, core).start()
    r_copy.start()
    g_copy.start()

    @pl.loop(0, per)
    def _(j):
        part[SIB, :, columns(j)] = chunk(2 * per + j, home_col(j)).astype(BF16)

    sib_copy().start()

    @pl.loop(0, per)
    def _(j):
        own[:, columns(j)] = chunk(3 * per + j, home_col(per + j))

    r_copy.wait()
    g_copy.wait()
    sib_copy().wait_recv()

    @pl.when(core == 0)
    def _():
        for q in range(len(far_parts)):
            for slot in range(2):
                far_copy(q, slot).wait_recv()

    lane = lax.broadcasted_iota(jnp.int32, (8, 128), 1)
    sub = lax.broadcasted_iota(jnp.int32, (8, 128), 0)

    def reduce_block(b):
        row, n = blocks[b]
        if row in [first for first, _ in near_blocks]:
            @pl.when(core == 1)
            def _():
                for slot in range(2):
                    near_copy([first for first, _ in near_blocks].index(row), slot).wait_recv()

        line = jnp.zeros((8, 128), F32)
        for first in range(0, n, SUB):
            sl = pl.ds(row + first, SUB)
            h = own[sl, :] + recv[SIB, sl, :].astype(F32) + recv[0, sl, :].astype(F32) + recv[1, sl, :].astype(F32)
            h = r_v[sl, :].astype(F32) + h
            own[sl, :] = h
            hid[sl, :] = h.astype(BF16)
            s = jnp.sum(h * h, axis=1, keepdims=True)
            for q in range(0, SUB, 8):
                line = line + jnp.where(lane == sub + (first + q), s[q:q + 8, :], 0.0)
        st_tx[b] = jnp.sum(line, axis=0, keepdims=True)
        for k in range(3):
            stat_copy(k, b, SIB if k == SIB else core).start()

    def norm_block(b):
        for slot in range(3):
            stat_copy(slot, b, slot).wait_recv()
        row, n = blocks[b]
        tot = (st_tx[b] + st_rx[SIB, b]) + (st_rx[0, b] + st_rx[1, b])
        scale = jnp.broadcast_to(lax.rsqrt(tot / d_model + EPS), (8, 128))
        for first in range(0, n, SUB):
            for q in range(first, first + SUB, 8):
                sl = pl.ds(row + q, 8)
                col = jnp.sum(jnp.where(lane == sub + q, scale, 0.0), axis=1, keepdims=True)
                own[sl, :] = own[sl, :] * col * g_v[...]
            sl = pl.ds(row + first, SUB)
            nrm[sl, :] = own[sl, :].astype(BF16)

    for b in range(n_blk):
        reduce_block(b)

    for b in range(n_blk):
        norm_block(b)

    for q in range(len(far_parts)):
        far_copy(q, core).wait_send()
    for b in range(len(NEAR_ROWS)):
        near_copy(b, core).wait_send()
    for b in range(n_blk):
        for k in range(3):
            stat_copy(k, b, SIB if k == SIB else core).wait_send()
    sib_copy().wait_send()


def put(hid, nrm, hid_hbm, nrm_hbm, sem):
    n = hid.shape[0] // PUT
    copies = []
    for q in range(PUT):
        sl = pl.ds(q * n, n)
        copies.append(pltpu.make_async_copy(hid.at[sl, :], hid_hbm.at[sl, :], sem.at[0, q]))
        copies.append(pltpu.make_async_copy(nrm.at[sl, :], nrm_hbm.at[sl, :], sem.at[1, q]))
    for c in copies:
        c.start()
    for c in copies:
        c.wait()


def solution(mesh):
    tp = mesh.shape["tp"]

    def local_step(a, w, r, g):
        rows, depth = a.shape
        d_loc = r.shape[1]
        per = d_loc // CW
        n_blk = len(BLOCKS)
        hbm = pl.BlockSpec(memory_space=pltpu.HBM)
        vmem = pl.BlockSpec(memory_space=pltpu.VMEM)
        dma = pltpu.SemaphoreType.DMA
        hid, nrm = pl.pallas_call(
            functools.partial(kernel, d_loc * tp),
            out_shape=(pltpu.VMEM((rows, d_loc), BF16),) * 2,
            in_specs=[hbm] * 4,
            out_specs=(vmem,) * 2,
            scratch_shapes=[
                pltpu.VMEM((rows, depth), BF16),
                pltpu.VMEM((4 * per, depth, CW), BF16),
                pltpu.VMEM((rows, d_loc), BF16),
                pltpu.VMEM((1, d_loc), F32),
                pltpu.VMEM((3, rows, d_loc), BF16),
                pltpu.VMEM((3, rows, d_loc), BF16),
                pltpu.VMEM((rows, d_loc), F32),
                pltpu.VMEM((n_blk, 1, 128), F32),
                pltpu.VMEM((3, n_blk, 1, 128), F32),
                dma, dma((4 * per,)), dma, dma,
                dma((N_COL + 1,)), dma((2, N_COL + 1)), dma((len(NEAR_ROWS),)), dma((2, len(NEAR_ROWS))), dma, dma,
                dma((3, n_blk)), dma((3, n_blk)),
            ],
            compiler_params=pltpu.CompilerParams(
                collective_id=0, has_side_effects=True, vmem_limit_bytes=64946176),
            cost_estimate=pl.CostEstimate(flops=2 * rows * depth * d_loc * tp, transcendentals=0,
                                          bytes_accessed=2 * depth * d_loc * tp),
        )(a, w, r, g.reshape(1, d_loc))
        return pl.pallas_call(
            put,
            out_shape=(jax.ShapeDtypeStruct((rows, d_loc), BF16),) * 2,
            in_specs=[vmem] * 2,
            out_specs=(hbm,) * 2,
            scratch_shapes=[dma((2, PUT))],
            compiler_params=pltpu.CompilerParams(vmem_limit_bytes=1024 * 1024),
        )(hid, nrm)

    return jax.shard_map(
        local_step,
        mesh=mesh,
        in_specs=(P("data", "tp"), P("tp", None), P("data", "tp"), P("tp")),
        out_specs=(P("data", "tp"), P("data", "tp")),
        check_vma=False,
    )
```

```python
import functools

import jax
import jax.numpy as jnp
from jax import lax
from jax.experimental import pallas as pl
from jax.experimental.pallas import tpu as pltpu
from jax.sharding import PartitionSpec as P

EPS = 1e-5
MESH = pl.DeviceIdType.MESH
F32, BF16 = jnp.float32, jnp.bfloat16

CW = 256
FIRST = 64
N_COL = 2
BLOCKS = (128, 112, 16)
NEAR_ROWS = (240, 16)
SUB = 16
DEPTH = 4
PUT = 1
NEAR, SIB = 0, 1
FROM_SIB = 2


def kernel(d_model, a_hbm, w_hbm, r_hbm, g_hbm, hid, nrm,
           a_v, w_v, r_v, g_v, far_part, far_recv, part, recv, own, st_tx, st_rx,
           a_sem, w_sem, r_sem, g_sem, far_tx, far_rx, near_tx, near_rx, sib_tx, sib_rx, stat_tx, stat_rx):
    t = lax.axis_index("tp")
    core, chip = t % 2, t // 2
    rows, _ = a_v.shape
    d_loc = own.shape[1]
    per = d_loc // CW
    n_blk = len(BLOCKS)
    blocks = [(sum(BLOCKS[:b]), BLOCKS[b]) for b in range(n_blk)]
    far, near, sib = 2 - 2 * chip, 3 - 2 * chip, t + 1 - 2 * core

    def cross_col(i):
        return (far + i // per) * d_loc + (i % per) * CW

    def home_col(i):
        return (sib + (t - sib) * (i // per)) * d_loc + (i % per) * CW

    def w_copy(i, col):
        return pltpu.make_async_copy(w_hbm.at[:, pl.ds(pl.multiple_of(col, CW), CW)], w_v.at[i], w_sem.at[i])

    def w_start(i):
        if isinstance(i, int):
            w_copy(i, cross_col(i) if i < 2 * per else home_col(i - 2 * per)).start()
            return

        @pl.when(i < 2 * per)
        def _():
            w_copy(i, cross_col(i)).start()

        @pl.when((i >= 2 * per) & (i < 4 * per))
        def _():
            w_copy(i, home_col(i - 2 * per)).start()

    def a_copy(q):
        sl = pl.ds(*((0, FIRST), (FIRST, rows - FIRST))[q])
        return pltpu.make_async_copy(a_hbm.at[sl, :], a_v.at[sl, :], a_sem.at[q])

    def remote(src, dst, tx, rx, peer):
        return pltpu.make_async_remote_copy(src_ref=src, dst_ref=dst, send_sem=tx, recv_sem=rx,
                                            device_id={"tp": peer}, device_id_type=MESH)

    every = pl.ds(0, rows)
    far_parts = [(pl.ds(0, 1), pl.ds(0, FIRST)), (pl.ds(0, 1), pl.ds(FIRST, rows - FIRST))]
    far_parts += [(pl.ds(j, 1), every) for j in range(1, N_COL)]
    far_parts += [(pl.ds(N_COL, per - N_COL), every)]

    def far_copy(q, slot):
        sl = far_parts[q]
        return remote(far_part.at[sl], far_recv.at[(slot, *sl)], far_tx.at[q], far_rx.at[slot, q], far)

    near_blocks = [(sum(NEAR_ROWS[:b]), NEAR_ROWS[b]) for b in range(len(NEAR_ROWS))]

    def near_copy(b, slot):
        sl = pl.ds(*near_blocks[b])
        return remote(part.at[NEAR, sl, :], recv.at[slot, sl, :], near_tx.at[b], near_rx.at[slot, b], near)

    def sib_copy():
        return remote(part.at[SIB], recv.at[FROM_SIB], sib_tx, sib_rx, sib)

    def stat_copy(k, b, slot):
        return remote(st_tx.at[b], st_rx.at[slot, b], stat_tx.at[k, b], stat_rx.at[slot, b], (far, near, sib)[k])

    barrier = pltpu.get_barrier_semaphore()
    for p in (far, near, sib):
        pl.semaphore_signal(barrier, inc=1, device_id={"tp": p}, device_id_type=MESH)
    a_copy(0).start()
    w_start(0)
    a_copy(1).start()
    r_copy = pltpu.make_async_copy(r_hbm, r_v, r_sem)
    g_copy = pltpu.make_async_copy(g_hbm, g_v, g_sem)

    def dot(lhs, rhs):
        return jnp.dot(lhs, rhs, preferred_element_type=F32)

    for q in range(2):
        a_copy(q).wait()
        if q == 0:
            w_copy(0, cross_col(0)).wait()
            for i in range(1, DEPTH):
                w_start(i)
        else:
            w_start(DEPTH)
        sl = far_parts[q][1]
        far_part[0, sl, :] = dot(a_v[sl, :], w_v[0]).astype(BF16)
        if q == 0:
            pl.semaphore_wait(barrier, 3)
        far_copy(q, core).start()

    def chunk(i, col):
        w_copy(i, col).wait()
        w_start(i + DEPTH)
        return dot(a_v[...], w_v[i])

    def columns(j):
        return pl.ds(pl.multiple_of(j * CW, CW), CW)

    for j in range(1, N_COL):
        far_part[j] = chunk(j, cross_col(j)).astype(BF16)
        far_copy(1 + j, core).start()

    @pl.loop(N_COL, per)
    def _(j):
        far_part[j] = chunk(j, cross_col(j)).astype(BF16)

    far_copy(len(far_parts) - 1, core).start()

    @pl.loop(0, per)
    def _(j):
        part[NEAR, :, columns(j)] = chunk(per + j, cross_col(per + j)).astype(BF16)

    for b in range(len(NEAR_ROWS)):
        near_copy(b, core).start()
    r_copy.start()
    g_copy.start()

    @pl.loop(0, per)
    def _(j):
        part[SIB, :, columns(j)] = chunk(2 * per + j, home_col(j)).astype(BF16)

    sib_copy().start()

    @pl.loop(0, per)
    def _(j):
        own[:, columns(j)] = chunk(3 * per + j, home_col(per + j))

    r_copy.wait()
    g_copy.wait()
    sib_copy().wait_recv()

    @pl.when(core == 0)
    def _():
        for q in range(len(far_parts)):
            for slot in range(2):
                far_copy(q, slot).wait_recv()

        @pl.loop(0, per)
        def _(j):
            own[:, columns(j)] += far_recv[0, j].astype(F32) + far_recv[1, j].astype(F32)

        for slot in range(2):
            recv[slot] = jnp.zeros((rows, d_loc), BF16)

    lane = lax.broadcasted_iota(jnp.int32, (8, 128), 1)
    sub = lax.broadcasted_iota(jnp.int32, (8, 128), 0)

    def reduce_block(b):
        row, n = blocks[b]
        if row in [first for first, _ in near_blocks]:
            @pl.when(core == 1)
            def _():
                for slot in range(2):
                    near_copy([first for first, _ in near_blocks].index(row), slot).wait_recv()

        line = jnp.zeros((8, 128), F32)
        for first in range(0, n, SUB):
            sl = pl.ds(row + first, SUB)
            h = own[sl, :] + recv[FROM_SIB, sl, :].astype(F32) + recv[0, sl, :].astype(F32) + recv[1, sl, :].astype(F32)
            h = r_v[sl, :].astype(F32) + h
            own[sl, :] = h
            hid[sl, :] = h.astype(BF16)
            s = jnp.sum(h * h, axis=1, keepdims=True)
            for q in range(0, SUB, 8):
                line = line + jnp.where(lane == sub + (first + q), s[q:q + 8, :], 0.0)
        st_tx[b] = jnp.sum(line, axis=0, keepdims=True)
        for k in range(3):
            stat_copy(k, b, k if k == 2 else core).start()

    def norm_block(b):
        for slot in range(3):
            stat_copy(slot, b, slot).wait_recv()
        row, n = blocks[b]
        tot = (st_tx[b] + st_rx[2, b]) + (st_rx[0, b] + st_rx[1, b])
        scale = jnp.broadcast_to(lax.rsqrt(tot / d_model + EPS), (8, 128))
        for first in range(0, n, SUB):
            for q in range(first, first + SUB, 8):
                sl = pl.ds(row + q, 8)
                col = jnp.sum(jnp.where(lane == sub + q, scale, 0.0), axis=1, keepdims=True)
                own[sl, :] = own[sl, :] * col * g_v[...]
            sl = pl.ds(row + first, SUB)
            nrm[sl, :] = own[sl, :].astype(BF16)

    for b in range(n_blk):
        reduce_block(b)

    for b in range(n_blk):
        norm_block(b)

    for q in range(len(far_parts)):
        far_copy(q, core).wait_send()
    for b in range(len(NEAR_ROWS)):
        near_copy(b, core).wait_send()
    for b in range(n_blk):
        for k in range(3):
            stat_copy(k, b, k if k == 2 else core).wait_send()
    sib_copy().wait_send()


def put(hid, nrm, hid_hbm, nrm_hbm, sem):
    n = hid.shape[0] // PUT
    copies = []
    for q in range(PUT):
        sl = pl.ds(q * n, n)
        copies.append(pltpu.make_async_copy(hid.at[sl, :], hid_hbm.at[sl, :], sem.at[0, q]))
        copies.append(pltpu.make_async_copy(nrm.at[sl, :], nrm_hbm.at[sl, :], sem.at[1, q]))
    for c in copies:
        c.start()
    for c in copies:
        c.wait()


def solution(mesh):
    tp = mesh.shape["tp"]

    def local_step(a, w, r, g):
        rows, depth = a.shape
        d_loc = r.shape[1]
        per = d_loc // CW
        n_blk = len(BLOCKS)
        hbm = pl.BlockSpec(memory_space=pltpu.HBM)
        vmem = pl.BlockSpec(memory_space=pltpu.VMEM)
        dma = pltpu.SemaphoreType.DMA
        hid, nrm = pl.pallas_call(
            functools.partial(kernel, d_loc * tp),
            out_shape=(pltpu.VMEM((rows, d_loc), BF16),) * 2,
            in_specs=[hbm] * 4,
            out_specs=(vmem,) * 2,
            scratch_shapes=[
                pltpu.VMEM((rows, depth), BF16),
                pltpu.VMEM((4 * per, depth, CW), BF16),
                pltpu.VMEM((rows, d_loc), BF16),
                pltpu.VMEM((1, d_loc), F32),
                pltpu.VMEM((per, rows, CW), BF16),
                pltpu.VMEM((2, per, rows, CW), BF16),
                pltpu.VMEM((2, rows, d_loc), BF16),
                pltpu.VMEM((3, rows, d_loc), BF16),
                pltpu.VMEM((rows, d_loc), F32),
                pltpu.VMEM((n_blk, 1, 128), F32),
                pltpu.VMEM((3, n_blk, 1, 128), F32),
                dma((2,)), dma((4 * per,)), dma, dma,
                dma((N_COL + 2,)), dma((2, N_COL + 2)), dma((len(NEAR_ROWS),)), dma((2, len(NEAR_ROWS))), dma, dma,
                dma((3, n_blk)), dma((3, n_blk)),
            ],
            compiler_params=pltpu.CompilerParams(
                collective_id=0, has_side_effects=True, vmem_limit_bytes=64946176),
            cost_estimate=pl.CostEstimate(flops=2 * rows * depth * d_loc * tp, transcendentals=0,
                                          bytes_accessed=2 * depth * d_loc * tp),
        )(a, w, r, g.reshape(1, d_loc))
        return pl.pallas_call(
            put,
            out_shape=(jax.ShapeDtypeStruct((rows, d_loc), BF16),) * 2,
            in_specs=[vmem] * 2,
            out_specs=(hbm,) * 2,
            scratch_shapes=[dma((2, PUT))],
            compiler_params=pltpu.CompilerParams(vmem_limit_bytes=1024 * 1024),
        )(hid, nrm)

    return jax.shard_map(
        local_step,
        mesh=mesh,
        in_specs=(P("data", "tp"), P("tp", None), P("data", "tp"), P("tp")),
        out_specs=(P("data", "tp"), P("data", "tp")),
        check_vma=False,
    )
```

```python
import functools

import jax
import jax.numpy as jnp
from jax import lax
from jax.experimental import pallas as pl
from jax.experimental.pallas import tpu as pltpu
from jax.sharding import PartitionSpec as P

EPS = 1e-5
MESH = pl.DeviceIdType.MESH
F32, BF16 = jnp.float32, jnp.bfloat16

CW = 256
N_COL = 2
BLOCKS = (128, 112, 16)
NEAR_ROWS = (240, 16)
NEAR_CUTS = (1, 4)
SUB = 16
DEPTH = 4
PUT = 1
FAR, NEAR, SIB = 0, 1, 2


def kernel(d_model, a_hbm, w_hbm, r_hbm, g_hbm, hid, nrm,
           a_v, w_v, r_v, g_v, part, recv, own, st_tx, st_rx,
           a_sem, w0_sem, w_sem, r_sem, g_sem, far_tx, far_rx, near_tx, near_rx, sib_tx, sib_rx, stat_tx, stat_rx):
    t = lax.axis_index("tp")
    core, chip = t % 2, t // 2
    rows, _ = a_v.shape
    d_loc = own.shape[1]
    per = d_loc // CW
    n_blk = len(BLOCKS)
    blocks = [(sum(BLOCKS[:b]), BLOCKS[b]) for b in range(n_blk)]
    half, lanes = rows // 2, 128
    far, near, sib = 2 - 2 * chip, 3 - 2 * chip, t + 1 - 2 * core

    def cross_col(i):
        return (far + i // per) * d_loc + (i % per) * CW

    def home_col(i):
        return (sib + (t - sib) * (i // per)) * d_loc + (i % per) * CW

    def w_copy(i, col):
        return pltpu.make_async_copy(w_hbm.at[:, pl.ds(pl.multiple_of(col, CW), CW)], w_v.at[i], w_sem.at[i])

    def w_start(i):
        if isinstance(i, int):
            w_copy(i, cross_col(i) if i < 2 * per else home_col(i - 2 * per)).start()
            return

        @pl.when(i < 2 * per)
        def _():
            w_copy(i, cross_col(i)).start()

        @pl.when((i >= 2 * per) & (i < 4 * per))
        def _():
            w_copy(i, home_col(i - 2 * per)).start()

    def a_copy(q):
        sl = pl.ds(q * half, half)
        return pltpu.make_async_copy(a_hbm.at[sl, :], a_v.at[sl, :], a_sem.at[q])

    def w0_copy(q):
        src = w_hbm.at[:, pl.ds(pl.multiple_of(far * d_loc + q * lanes, lanes), lanes)]
        return pltpu.make_async_copy(src, w_v.at[0, :, pl.ds(q * lanes, lanes)], w0_sem.at[q])

    def remote(src, dst, tx, rx, peer):
        return pltpu.make_async_remote_copy(src_ref=src, dst_ref=dst, send_sem=tx, recv_sem=rx,
                                            device_id={"tp": peer}, device_id_type=MESH)

    every = pl.ds(0, rows)
    far_parts = [(pl.ds(0, half), pl.ds(0, lanes)), (pl.ds(0, half), pl.ds(lanes, lanes)), (pl.ds(half, half), pl.ds(0, CW))]
    far_parts += [(every, pl.ds(j * CW, CW)) for j in range(1, N_COL)]
    far_parts += [(every, pl.ds(N_COL * CW, d_loc - N_COL * CW))]

    def far_copy(q, slot):
        sl = far_parts[q]
        return remote(part.at[(FAR, *sl)], recv.at[(slot, *sl)], far_tx.at[q], far_rx.at[slot, q], far)

    near_parts = []
    for b, cuts in enumerate(NEAR_CUTS):
        n = d_loc // cuts
        near_parts += [(pl.ds(sum(NEAR_ROWS[:b]), NEAR_ROWS[b]), pl.ds(q * n, n)) for q in range(cuts)]

    def near_copy(q, slot):
        sl = near_parts[q]
        return remote(part.at[(NEAR, *sl)], recv.at[(slot, *sl)], near_tx.at[q], near_rx.at[slot, q], near)

    def sib_copy():
        return remote(part.at[SIB], recv.at[SIB], sib_tx, sib_rx, sib)

    def stat_copy(k, b, slot):
        return remote(st_tx.at[b], st_rx.at[slot, b], stat_tx.at[k, b], stat_rx.at[slot, b], (far, near, sib)[k])

    barrier = pltpu.get_barrier_semaphore()
    for p in (far, near, sib):
        pl.semaphore_signal(barrier, inc=1, device_id={"tp": p}, device_id_type=MESH)
    a_copy(0).start()
    w0_copy(0).start()
    w0_copy(1).start()
    a_copy(1).start()
    r_copy = pltpu.make_async_copy(r_hbm, r_v, r_sem)
    g_copy = pltpu.make_async_copy(g_hbm, g_v, g_sem)

    def dot(lhs, rhs):
        return jnp.dot(lhs, rhs, preferred_element_type=F32)

    for q in range(3):
        if q == 0:
            a_copy(0).wait()
            w0_copy(0).wait()
            for i in range(1, DEPTH):
                w_start(i)
        elif q == 1:
            w0_copy(1).wait()
        else:
            a_copy(1).wait()
            w_start(DEPTH)
        r_sl, c_sl = far_parts[q]
        part[FAR, r_sl, c_sl] = dot(a_v[r_sl, :], w_v[0, :, c_sl]).astype(BF16)
        if q == 0:
            pl.semaphore_wait(barrier, 3)
        far_copy(q, core).start()

    def chunk(i, col):
        w_copy(i, col).wait()
        w_start(i + DEPTH)
        return dot(a_v[...], w_v[i])

    def columns(j):
        return pl.ds(pl.multiple_of(j * CW, CW), CW)

    for j in range(1, N_COL):
        part[FAR, :, columns(j)] = chunk(j, cross_col(j)).astype(BF16)
        far_copy(2 + j, core).start()

    @pl.loop(N_COL, per)
    def _(j):
        part[FAR, :, columns(j)] = chunk(j, cross_col(j)).astype(BF16)

    far_copy(len(far_parts) - 1, core).start()

    @pl.loop(0, per)
    def _(j):
        part[NEAR, :, columns(j)] = chunk(per + j, cross_col(per + j)).astype(BF16)

    for q in range(len(near_parts)):
        near_copy(q, core).start()
    r_copy.start()
    g_copy.start()

    @pl.loop(0, per)
    def _(j):
        part[SIB, :, columns(j)] = chunk(2 * per + j, home_col(j)).astype(BF16)

    sib_copy().start()

    @pl.loop(0, per)
    def _(j):
        own[:, columns(j)] = chunk(3 * per + j, home_col(per + j))

    r_copy.wait()
    g_copy.wait()
    sib_copy().wait_recv()

    @pl.when(core == 0)
    def _():
        for q in range(len(far_parts)):
            for slot in range(2):
                far_copy(q, slot).wait_recv()

    lane = lax.broadcasted_iota(jnp.int32, (8, 128), 1)
    sub = lax.broadcasted_iota(jnp.int32, (8, 128), 0)

    def reduce_block(b):
        row, n = blocks[b]
        awaited = [q for q, (r_sl, _) in enumerate(near_parts) if r_sl.start == row]
        if awaited:
            @pl.when(core == 1)
            def _():
                for q in awaited:
                    for slot in range(2):
                        near_copy(q, slot).wait_recv()

        line = jnp.zeros((8, 128), F32)
        for first in range(0, n, SUB):
            sl = pl.ds(row + first, SUB)
            h = own[sl, :] + recv[SIB, sl, :].astype(F32) + recv[0, sl, :].astype(F32) + recv[1, sl, :].astype(F32)
            h = r_v[sl, :].astype(F32) + h
            own[sl, :] = h
            hid[sl, :] = h.astype(BF16)
            s = jnp.sum(h * h, axis=1, keepdims=True)
            for q in range(0, SUB, 8):
                line = line + jnp.where(lane == sub + (first + q), s[q:q + 8, :], 0.0)
        st_tx[b] = jnp.sum(line, axis=0, keepdims=True)
        for k in range(3):
            stat_copy(k, b, SIB if k == SIB else core).start()

    def norm_block(b):
        for slot in range(3):
            stat_copy(slot, b, slot).wait_recv()
        row, n = blocks[b]
        tot = (st_tx[b] + st_rx[SIB, b]) + (st_rx[0, b] + st_rx[1, b])
        scale = jnp.broadcast_to(lax.rsqrt(tot / d_model + EPS), (8, 128))
        for first in range(0, n, SUB):
            for q in range(first, first + SUB, 8):
                sl = pl.ds(row + q, 8)
                col = jnp.sum(jnp.where(lane == sub + q, scale, 0.0), axis=1, keepdims=True)
                own[sl, :] = own[sl, :] * col * g_v[...]
            sl = pl.ds(row + first, SUB)
            nrm[sl, :] = own[sl, :].astype(BF16)

    for b in range(n_blk):
        reduce_block(b)

    for b in range(n_blk):
        norm_block(b)

    for q in range(len(far_parts)):
        far_copy(q, core).wait_send()
    for q in range(len(near_parts)):
        near_copy(q, core).wait_send()
    for b in range(n_blk):
        for k in range(3):
            stat_copy(k, b, SIB if k == SIB else core).wait_send()
    sib_copy().wait_send()


def put(hid, nrm, hid_hbm, nrm_hbm, sem):
    n = hid.shape[0] // PUT
    copies = []
    for q in range(PUT):
        sl = pl.ds(q * n, n)
        copies.append(pltpu.make_async_copy(hid.at[sl, :], hid_hbm.at[sl, :], sem.at[0, q]))
        copies.append(pltpu.make_async_copy(nrm.at[sl, :], nrm_hbm.at[sl, :], sem.at[1, q]))
    for c in copies:
        c.start()
    for c in copies:
        c.wait()


def solution(mesh):
    tp = mesh.shape["tp"]

    def local_step(a, w, r, g):
        rows, depth = a.shape
        d_loc = r.shape[1]
        per = d_loc // CW
        n_blk = len(BLOCKS)
        hbm = pl.BlockSpec(memory_space=pltpu.HBM)
        vmem = pl.BlockSpec(memory_space=pltpu.VMEM)
        dma = pltpu.SemaphoreType.DMA
        hid, nrm = pl.pallas_call(
            functools.partial(kernel, d_loc * tp),
            out_shape=(pltpu.VMEM((rows, d_loc), BF16),) * 2,
            in_specs=[hbm] * 4,
            out_specs=(vmem,) * 2,
            scratch_shapes=[
                pltpu.VMEM((rows, depth), BF16),
                pltpu.VMEM((4 * per, depth, CW), BF16),
                pltpu.VMEM((rows, d_loc), BF16),
                pltpu.VMEM((1, d_loc), F32),
                pltpu.VMEM((3, rows, d_loc), BF16),
                pltpu.VMEM((3, rows, d_loc), BF16),
                pltpu.VMEM((rows, d_loc), F32),
                pltpu.VMEM((n_blk, 1, 128), F32),
                pltpu.VMEM((3, n_blk, 1, 128), F32),
                dma((2,)), dma((2,)), dma((4 * per,)), dma, dma,
                dma((N_COL + 3,)), dma((2, N_COL + 3)), dma((sum(NEAR_CUTS),)), dma((2, sum(NEAR_CUTS))), dma, dma,
                dma((3, n_blk)), dma((3, n_blk)),
            ],
            compiler_params=pltpu.CompilerParams(
                collective_id=0, has_side_effects=True, vmem_limit_bytes=64946176),
            cost_estimate=pl.CostEstimate(flops=2 * rows * depth * d_loc * tp, transcendentals=0,
                                          bytes_accessed=2 * depth * d_loc * tp),
        )(a, w, r, g.reshape(1, d_loc))
        return pl.pallas_call(
            put,
            out_shape=(jax.ShapeDtypeStruct((rows, d_loc), BF16),) * 2,
            in_specs=[vmem] * 2,
            out_specs=(hbm,) * 2,
            scratch_shapes=[dma((2, PUT))],
            compiler_params=pltpu.CompilerParams(vmem_limit_bytes=1024 * 1024),
        )(hid, nrm)

    return jax.shard_map(
        local_step,
        mesh=mesh,
        in_specs=(P("data", "tp"), P("tp", None), P("data", "tp"), P("tp")),
        out_specs=(P("data", "tp"), P("data", "tp")),
        check_vma=False,
    )
```

```python
import functools

import jax
import jax.numpy as jnp
from jax import lax
from jax.experimental import pallas as pl
from jax.experimental.pallas import tpu as pltpu
from jax.sharding import PartitionSpec as P

EPS = 1e-5
MESH = pl.DeviceIdType.MESH
F32, BF16 = jnp.float32, jnp.bfloat16

CW = 256
N_COL = 2
BLOCKS = (128, 112, 16)
SUB = 16
DEPTH = 4
PUT = 1
FAR, NEAR, SIB = 0, 1, 2


def kernel(d_model, a_hbm, w_hbm, r_hbm, g_hbm, hid, nrm,
           a_v, w_v, r_v, g_v, part, recv, own, st_tx, st_rx,
           a_sem, w0_sem, w_sem, r_sem, g_sem, far_tx, far_rx, near_tx, near_rx, sib_tx, sib_rx, stat_tx, stat_rx):
    t = lax.axis_index("tp")
    core, chip = t % 2, t // 2
    rows, _ = a_v.shape
    d_loc = own.shape[1]
    per = d_loc // CW
    n_blk = len(BLOCKS)
    blocks = [(sum(BLOCKS[:b]), BLOCKS[b]) for b in range(n_blk)]
    half, lanes = rows // 2, 128
    far, near, sib = 2 - 2 * chip, 3 - 2 * chip, t + 1 - 2 * core

    def cross_col(i):
        return (far + i // per) * d_loc + (i % per) * CW

    def home_col(i):
        return (sib + (t - sib) * (i // per)) * d_loc + (i % per) * CW

    def w_copy(i, col):
        return pltpu.make_async_copy(w_hbm.at[:, pl.ds(pl.multiple_of(col, CW), CW)], w_v.at[i], w_sem.at[i])

    def w_start(i):
        if isinstance(i, int):
            w_copy(i, cross_col(i) if i < 2 * per else home_col(i - 2 * per)).start()
            return

        @pl.when(i < 2 * per)
        def _():
            w_copy(i, cross_col(i)).start()

        @pl.when((i >= 2 * per) & (i < 4 * per))
        def _():
            w_copy(i, home_col(i - 2 * per)).start()

    def a_copy(q):
        sl = pl.ds(q * half, half)
        return pltpu.make_async_copy(a_hbm.at[sl, :], a_v.at[sl, :], a_sem.at[q])

    def w0_copy(q):
        src = w_hbm.at[:, pl.ds(pl.multiple_of(far * d_loc + q * lanes, lanes), lanes)]
        return pltpu.make_async_copy(src, w_v.at[0, :, pl.ds(q * lanes, lanes)], w0_sem.at[q])

    def remote(src, dst, tx, rx, peer):
        return pltpu.make_async_remote_copy(src_ref=src, dst_ref=dst, send_sem=tx, recv_sem=rx,
                                            device_id={"tp": peer}, device_id_type=MESH)

    every = pl.ds(0, rows)
    far_parts = [(pl.ds(0, half), pl.ds(0, lanes)), (pl.ds(0, half), pl.ds(lanes, lanes)), (pl.ds(half, half), pl.ds(0, CW))]
    far_parts += [(every, pl.ds(j * CW, CW)) for j in range(1, N_COL)]
    far_parts += [(every, pl.ds(N_COL * CW, d_loc - N_COL * CW))]

    def far_copy(q, slot):
        sl = far_parts[q]
        return remote(part.at[(FAR, *sl)], recv.at[(slot, *sl)], far_tx.at[q], far_rx.at[slot, q], far)

    def near_copy(b, slot):
        sl = pl.ds(*blocks[b])
        return remote(part.at[NEAR, sl, :], recv.at[slot, sl, :], near_tx.at[b], near_rx.at[slot, b], near)

    def sib_copy():
        return remote(part.at[SIB], recv.at[SIB], sib_tx, sib_rx, sib)

    def stat_copy(k, b, slot):
        return remote(st_tx.at[b], st_rx.at[slot, b], stat_tx.at[k, b], stat_rx.at[slot, b], (far, near, sib)[k])

    barrier = pltpu.get_barrier_semaphore()
    for p in (far, near, sib):
        pl.semaphore_signal(barrier, inc=1, device_id={"tp": p}, device_id_type=MESH)
    a_copy(0).start()
    w0_copy(0).start()
    w0_copy(1).start()
    a_copy(1).start()
    r_copy = pltpu.make_async_copy(r_hbm, r_v, r_sem)
    g_copy = pltpu.make_async_copy(g_hbm, g_v, g_sem)

    def dot(lhs, rhs):
        return jnp.dot(lhs, rhs, preferred_element_type=F32)

    for q in range(3):
        if q == 0:
            a_copy(0).wait()
            w0_copy(0).wait()
            for i in range(1, DEPTH):
                w_start(i)
        elif q == 1:
            w0_copy(1).wait()
        else:
            a_copy(1).wait()
            w_start(DEPTH)
        r_sl, c_sl = far_parts[q]
        part[FAR, r_sl, c_sl] = dot(a_v[r_sl, :], w_v[0, :, c_sl]).astype(BF16)
        if q == 0:
            pl.semaphore_wait(barrier, 3)
        far_copy(q, core).start()

    def chunk(i, col):
        w_copy(i, col).wait()
        w_start(i + DEPTH)
        return dot(a_v[...], w_v[i])

    def columns(j):
        return pl.ds(pl.multiple_of(j * CW, CW), CW)

    for j in range(1, N_COL):
        part[FAR, :, columns(j)] = chunk(j, cross_col(j)).astype(BF16)
        far_copy(2 + j, core).start()

    @pl.loop(N_COL, per)
    def _(j):
        part[FAR, :, columns(j)] = chunk(j, cross_col(j)).astype(BF16)

    far_copy(len(far_parts) - 1, core).start()

    @pl.loop(0, per)
    def _(j):
        part[NEAR, :, columns(j)] = chunk(per + j, cross_col(per + j)).astype(BF16)

    for b in range(n_blk - 1):
        near_copy(b, core).start()
    r_copy.start()
    g_copy.start()

    @pl.loop(0, per)
    def _(j):
        part[SIB, :, columns(j)] = chunk(2 * per + j, home_col(j)).astype(BF16)

    sib_copy().start()

    @pl.loop(0, per)
    def _(j):
        own[:, columns(j)] = chunk(3 * per + j, home_col(per + j))

    r_copy.wait()
    g_copy.wait()
    sib_copy().wait_recv()

    @pl.when(core == 0)
    def _():
        for q in range(len(far_parts)):
            for slot in range(2):
                far_copy(q, slot).wait_recv()

    lane = lax.broadcasted_iota(jnp.int32, (8, 128), 1)
    sub = lax.broadcasted_iota(jnp.int32, (8, 128), 0)

    def reduce_block(b):
        @pl.when(core == 1)
        def _():
            for slot in range(2):
                near_copy(b, slot).wait_recv()

        row, n = blocks[b]
        line = jnp.zeros((8, 128), F32)
        for first in range(0, n, SUB):
            sl = pl.ds(row + first, SUB)
            h = own[sl, :] + recv[SIB, sl, :].astype(F32) + recv[0, sl, :].astype(F32) + recv[1, sl, :].astype(F32)
            h = r_v[sl, :].astype(F32) + h
            own[sl, :] = h
            hid[sl, :] = h.astype(BF16)
            s = jnp.sum(h * h, axis=1, keepdims=True)
            for q in range(0, SUB, 8):
                line = line + jnp.where(lane == sub + (first + q), s[q:q + 8, :], 0.0)
        st_tx[b] = jnp.sum(line, axis=0, keepdims=True)
        for k in range(3):
            stat_copy(k, b, SIB if k == SIB else core).start()

    def norm_block(b):
        for slot in range(3):
            stat_copy(slot, b, slot).wait_recv()
        row, n = blocks[b]
        tot = (st_tx[b] + st_rx[SIB, b]) + (st_rx[0, b] + st_rx[1, b])
        scale = jnp.broadcast_to(lax.rsqrt(tot / d_model + EPS), (8, 128))
        for first in range(0, n, SUB):
            for q in range(first, first + SUB, 8):
                sl = pl.ds(row + q, 8)
                col = jnp.sum(jnp.where(lane == sub + q, scale, 0.0), axis=1, keepdims=True)
                own[sl, :] = own[sl, :] * col * g_v[...]
            sl = pl.ds(row + first, SUB)
            nrm[sl, :] = own[sl, :].astype(BF16)

    for b in range(n_blk):
        reduce_block(b)
        if b in (0, n_blk - 1):
            @pl.when(core == (1 if b == 0 else 0))
            def _():
                near_copy(n_blk - 1, core).start()

    for b in range(n_blk):
        norm_block(b)

    for q in range(len(far_parts)):
        far_copy(q, core).wait_send()
    for b in range(n_blk):
        near_copy(b, core).wait_send()
        for k in range(3):
            stat_copy(k, b, SIB if k == SIB else core).wait_send()
    sib_copy().wait_send()


def put(hid, nrm, hid_hbm, nrm_hbm, sem):
    n = hid.shape[0] // PUT
    copies = []
    for q in range(PUT):
        sl = pl.ds(q * n, n)
        copies.append(pltpu.make_async_copy(hid.at[sl, :], hid_hbm.at[sl, :], sem.at[0, q]))
        copies.append(pltpu.make_async_copy(nrm.at[sl, :], nrm_hbm.at[sl, :], sem.at[1, q]))
    for c in copies:
        c.start()
    for c in copies:
        c.wait()


def solution(mesh):
    tp = mesh.shape["tp"]

    def local_step(a, w, r, g):
        rows, depth = a.shape
        d_loc = r.shape[1]
        per = d_loc // CW
        n_blk = len(BLOCKS)
        hbm = pl.BlockSpec(memory_space=pltpu.HBM)
        vmem = pl.BlockSpec(memory_space=pltpu.VMEM)
        dma = pltpu.SemaphoreType.DMA
        hid, nrm = pl.pallas_call(
            functools.partial(kernel, d_loc * tp),
            out_shape=(pltpu.VMEM((rows, d_loc), BF16),) * 2,
            in_specs=[hbm] * 4,
            out_specs=(vmem,) * 2,
            scratch_shapes=[
                pltpu.VMEM((rows, depth), BF16),
                pltpu.VMEM((4 * per, depth, CW), BF16),
                pltpu.VMEM((rows, d_loc), BF16),
                pltpu.VMEM((1, d_loc), F32),
                pltpu.VMEM((3, rows, d_loc), BF16),
                pltpu.VMEM((3, rows, d_loc), BF16),
                pltpu.VMEM((rows, d_loc), F32),
                pltpu.VMEM((n_blk, 1, 128), F32),
                pltpu.VMEM((3, n_blk, 1, 128), F32),
                dma((2,)), dma((2,)), dma((4 * per,)), dma, dma,
                dma((N_COL + 3,)), dma((2, N_COL + 3)), dma((n_blk,)), dma((2, n_blk)), dma, dma,
                dma((3, n_blk)), dma((3, n_blk)),
            ],
            compiler_params=pltpu.CompilerParams(
                collective_id=0, has_side_effects=True, vmem_limit_bytes=64946176),
            cost_estimate=pl.CostEstimate(flops=2 * rows * depth * d_loc * tp, transcendentals=0,
                                          bytes_accessed=2 * depth * d_loc * tp),
        )(a, w, r, g.reshape(1, d_loc))
        return pl.pallas_call(
            put,
            out_shape=(jax.ShapeDtypeStruct((rows, d_loc), BF16),) * 2,
            in_specs=[vmem] * 2,
            out_specs=(hbm,) * 2,
            scratch_shapes=[dma((2, PUT))],
            compiler_params=pltpu.CompilerParams(vmem_limit_bytes=1024 * 1024),
        )(hid, nrm)

    return jax.shard_map(
        local_step,
        mesh=mesh,
        in_specs=(P("data", "tp"), P("tp", None), P("data", "tp"), P("tp")),
        out_specs=(P("data", "tp"), P("data", "tp")),
        check_vma=False,
    )
```

```python
import functools

import jax
import jax.numpy as jnp
from jax import lax
from jax.experimental import pallas as pl
from jax.experimental.pallas import tpu as pltpu
from jax.sharding import PartitionSpec as P

EPS = 1e-5
MESH = pl.DeviceIdType.MESH
F32, BF16 = jnp.float32, jnp.bfloat16

CW = 256
N_COL = 2
BLOCKS = (128, 112, 16)
SUB = 16
LAG = 2
DEPTH = 4
PUT = 1
FAR, NEAR, SIB = 0, 1, 2


def kernel(d_model, a_hbm, w_hbm, r_hbm, g_hbm, hid, nrm,
           a_v, w_v, r_v, g_v, part, recv, own, st_tx, st_rx,
           a_sem, w0_sem, w_sem, r_sem, g_sem, far_tx, far_rx, near_tx, near_rx, sib_tx, sib_rx, stat_tx, stat_rx):
    t = lax.axis_index("tp")
    core, chip = t % 2, t // 2
    rows, _ = a_v.shape
    d_loc = own.shape[1]
    per = d_loc // CW
    n_blk = len(BLOCKS)
    blocks = [(sum(BLOCKS[:b]), BLOCKS[b]) for b in range(n_blk)]
    half, lanes = rows // 2, 128
    far, near, sib = 2 - 2 * chip, 3 - 2 * chip, t + 1 - 2 * core

    def cross_col(i):
        return (far + i // per) * d_loc + (i % per) * CW

    def home_col(i):
        return (sib + (t - sib) * (i // per)) * d_loc + (i % per) * CW

    def w_copy(i, col):
        return pltpu.make_async_copy(w_hbm.at[:, pl.ds(pl.multiple_of(col, CW), CW)], w_v.at[i], w_sem.at[i])

    def w_start(i):
        if isinstance(i, int):
            w_copy(i, cross_col(i) if i < 2 * per else home_col(i - 2 * per)).start()
            return

        @pl.when(i < 2 * per)
        def _():
            w_copy(i, cross_col(i)).start()

        @pl.when((i >= 2 * per) & (i < 4 * per))
        def _():
            w_copy(i, home_col(i - 2 * per)).start()

    def a_copy(q):
        sl = pl.ds(q * half, half)
        return pltpu.make_async_copy(a_hbm.at[sl, :], a_v.at[sl, :], a_sem.at[q])

    def w0_copy(q):
        src = w_hbm.at[:, pl.ds(pl.multiple_of(far * d_loc + q * lanes, lanes), lanes)]
        return pltpu.make_async_copy(src, w_v.at[0, :, pl.ds(q * lanes, lanes)], w0_sem.at[q])

    def remote(src, dst, tx, rx, peer):
        return pltpu.make_async_remote_copy(src_ref=src, dst_ref=dst, send_sem=tx, recv_sem=rx,
                                            device_id={"tp": peer}, device_id_type=MESH)

    every = pl.ds(0, rows)
    far_parts = [(pl.ds(0, half), pl.ds(0, lanes)), (pl.ds(0, half), pl.ds(lanes, lanes)), (pl.ds(half, half), pl.ds(0, CW))]
    far_parts += [(every, pl.ds(j * CW, CW)) for j in range(1, N_COL)]
    far_parts += [(every, pl.ds(N_COL * CW, d_loc - N_COL * CW))]

    def far_copy(q, slot):
        sl = far_parts[q]
        return remote(part.at[(FAR, *sl)], recv.at[(slot, *sl)], far_tx.at[q], far_rx.at[slot, q], far)

    def near_copy(b, slot):
        sl = pl.ds(*blocks[b])
        return remote(part.at[NEAR, sl, :], recv.at[slot, sl, :], near_tx.at[b], near_rx.at[slot, b], near)

    def sib_copy():
        return remote(part.at[SIB], recv.at[SIB], sib_tx, sib_rx, sib)

    def stat_copy(k, b, slot):
        return remote(st_tx.at[b], st_rx.at[slot, b], stat_tx.at[k, b], stat_rx.at[slot, b], (far, near, sib)[k])

    barrier = pltpu.get_barrier_semaphore()
    for p in (far, near, sib):
        pl.semaphore_signal(barrier, inc=1, device_id={"tp": p}, device_id_type=MESH)
    a_copy(0).start()
    w0_copy(0).start()
    w0_copy(1).start()
    a_copy(1).start()
    r_copy = pltpu.make_async_copy(r_hbm, r_v, r_sem)
    g_copy = pltpu.make_async_copy(g_hbm, g_v, g_sem)

    def dot(lhs, rhs):
        return jnp.dot(lhs, rhs, preferred_element_type=F32)

    for q in range(3):
        if q == 0:
            a_copy(0).wait()
            w0_copy(0).wait()
            for i in range(1, DEPTH):
                w_start(i)
        elif q == 1:
            w0_copy(1).wait()
        else:
            a_copy(1).wait()
            w_start(DEPTH)
        r_sl, c_sl = far_parts[q]
        part[FAR, r_sl, c_sl] = dot(a_v[r_sl, :], w_v[0, :, c_sl]).astype(BF16)
        if q == 0:
            pl.semaphore_wait(barrier, 3)
        far_copy(q, core).start()

    def chunk(i, col):
        w_copy(i, col).wait()
        w_start(i + DEPTH)
        return dot(a_v[...], w_v[i])

    def columns(j):
        return pl.ds(pl.multiple_of(j * CW, CW), CW)

    for j in range(1, N_COL):
        part[FAR, :, columns(j)] = chunk(j, cross_col(j)).astype(BF16)
        far_copy(2 + j, core).start()

    @pl.loop(N_COL, per)
    def _(j):
        part[FAR, :, columns(j)] = chunk(j, cross_col(j)).astype(BF16)

    far_copy(len(far_parts) - 1, core).start()

    @pl.loop(0, per)
    def _(j):
        part[NEAR, :, columns(j)] = chunk(per + j, cross_col(per + j)).astype(BF16)

    for b in range(n_blk - 1):
        near_copy(b, core).start()
    r_copy.start()
    g_copy.start()

    @pl.loop(0, per)
    def _(j):
        part[SIB, :, columns(j)] = chunk(2 * per + j, home_col(j)).astype(BF16)

    sib_copy().start()

    @pl.loop(0, per)
    def _(j):
        own[:, columns(j)] = chunk(3 * per + j, home_col(per + j))

    r_copy.wait()
    g_copy.wait()
    sib_copy().wait_recv()

    @pl.when(core == 0)
    def _():
        for q in range(len(far_parts)):
            for slot in range(2):
                far_copy(q, slot).wait_recv()

    lane = lax.broadcasted_iota(jnp.int32, (8, 128), 1)
    sub = lax.broadcasted_iota(jnp.int32, (8, 128), 0)

    edges = [sum(BLOCKS[:q]) // SUB for q in range(n_blk + 1)]
    corr = [0, 0]
    for q in range(2, n_blk + 1):
        corr.append(edges[q] - edges[1] * q - sum(corr))

    def first_sub(b):
        at = b * edges[1]
        for q in range(2, n_blk + 1):
            at = at + jnp.minimum(b // q, 1) * corr[q]
        return at

    def reduce_block(b):
        for q in range(n_blk):
            @pl.when((core == 1) & (b == q))
            def _():
                for slot in range(2):
                    near_copy(q, slot).wait_recv()

        base = first_sub(b)

        def add(i, line):
            row = pl.multiple_of(i * SUB, SUB)
            sl = pl.ds(row, SUB)
            h = own[sl, :] + recv[SIB, sl, :].astype(F32) + recv[0, sl, :].astype(F32) + recv[1, sl, :].astype(F32)
            h = r_v[sl, :].astype(F32) + h
            own[sl, :] = h
            hid[sl, :] = h.astype(BF16)
            s = jnp.sum(h * h, axis=1, keepdims=True)
            for q in range(0, SUB, 8):
                line = line + jnp.where(lane == sub + ((i - base) * SUB + q), s[q:q + 8, :], 0.0)
            return line

        line = lax.fori_loop(base, first_sub(b + 1), add, jnp.zeros((8, 128), F32))
        st_tx[b] = jnp.sum(line, axis=0, keepdims=True)
        for k in range(3):
            stat_copy(k, b, SIB if k == SIB else core).start()

        @pl.when(b == (n_blk - 1) * (1 - core))
        def _():
            near_copy(n_blk - 1, core).start()

    def norm_block(b):
        for slot in range(3):
            stat_copy(slot, b, slot).wait_recv()
        base = first_sub(b)
        tot = (st_tx[b] + st_rx[SIB, b]) + (st_rx[0, b] + st_rx[1, b])
        scale = jnp.broadcast_to(lax.rsqrt(tot / d_model + EPS), (8, 128))

        def norm(i, _):
            row = pl.multiple_of(i * SUB, SUB)
            out = []
            for q in range(0, SUB, 8):
                col = jnp.sum(jnp.where(lane == sub + ((i - base) * SUB + q), scale, 0.0), axis=1, keepdims=True)
                out.append(own[pl.ds(pl.multiple_of(row + q, 8), 8), :] * col * g_v[...])
            nrm[pl.ds(row, SUB), :] = jnp.concatenate(out, axis=0).astype(BF16)
            return 0

        lax.fori_loop(base, first_sub(b + 1), norm, 0)

    @pl.loop(0, n_blk + LAG)
    def _(b):
        @pl.when(b < n_blk)
        def _():
            reduce_block(b)

        @pl.when(b >= LAG)
        def _():
            norm_block(b - LAG)

    for q in range(len(far_parts)):
        far_copy(q, core).wait_send()
    for b in range(n_blk):
        near_copy(b, core).wait_send()
        for k in range(3):
            stat_copy(k, b, SIB if k == SIB else core).wait_send()
    sib_copy().wait_send()


def put(hid, nrm, hid_hbm, nrm_hbm, sem):
    n = hid.shape[0] // PUT
    copies = []
    for q in range(PUT):
        sl = pl.ds(q * n, n)
        copies.append(pltpu.make_async_copy(hid.at[sl, :], hid_hbm.at[sl, :], sem.at[0, q]))
        copies.append(pltpu.make_async_copy(nrm.at[sl, :], nrm_hbm.at[sl, :], sem.at[1, q]))
    for c in copies:
        c.start()
    for c in copies:
        c.wait()


def solution(mesh):
    tp = mesh.shape["tp"]

    def local_step(a, w, r, g):
        rows, depth = a.shape
        d_loc = r.shape[1]
        per = d_loc // CW
        n_blk = len(BLOCKS)
        hbm = pl.BlockSpec(memory_space=pltpu.HBM)
        vmem = pl.BlockSpec(memory_space=pltpu.VMEM)
        dma = pltpu.SemaphoreType.DMA
        hid, nrm = pl.pallas_call(
            functools.partial(kernel, d_loc * tp),
            out_shape=(pltpu.VMEM((rows, d_loc), BF16),) * 2,
            in_specs=[hbm] * 4,
            out_specs=(vmem,) * 2,
            scratch_shapes=[
                pltpu.VMEM((rows, depth), BF16),
                pltpu.VMEM((4 * per, depth, CW), BF16),
                pltpu.VMEM((rows, d_loc), BF16),
                pltpu.VMEM((1, d_loc), F32),
                pltpu.VMEM((3, rows, d_loc), BF16),
                pltpu.VMEM((3, rows, d_loc), BF16),
                pltpu.VMEM((rows, d_loc), F32),
                pltpu.VMEM((n_blk, 1, 128), F32),
                pltpu.VMEM((3, n_blk, 1, 128), F32),
                dma((2,)), dma((2,)), dma((4 * per,)), dma, dma,
                dma((N_COL + 3,)), dma((2, N_COL + 3)), dma((n_blk,)), dma((2, n_blk)), dma, dma,
                dma((3, n_blk)), dma((3, n_blk)),
            ],
            compiler_params=pltpu.CompilerParams(
                collective_id=0, has_side_effects=True, vmem_limit_bytes=64946176),
            cost_estimate=pl.CostEstimate(flops=2 * rows * depth * d_loc * tp, transcendentals=0,
                                          bytes_accessed=2 * depth * d_loc * tp),
        )(a, w, r, g.reshape(1, d_loc))
        return pl.pallas_call(
            put,
            out_shape=(jax.ShapeDtypeStruct((rows, d_loc), BF16),) * 2,
            in_specs=[vmem] * 2,
            out_specs=(hbm,) * 2,
            scratch_shapes=[dma((2, PUT))],
            compiler_params=pltpu.CompilerParams(vmem_limit_bytes=1024 * 1024),
        )(hid, nrm)

    return jax.shard_map(
        local_step,
        mesh=mesh,
        in_specs=(P("data", "tp"), P("tp", None), P("data", "tp"), P("tp")),
        out_specs=(P("data", "tp"), P("data", "tp")),
        check_vma=False,
    )
```

```python
import functools

import jax
import jax.numpy as jnp
from jax import lax
from jax.experimental import pallas as pl
from jax.experimental.pallas import tpu as pltpu
from jax.sharding import PartitionSpec as P

EPS = 1e-5
MESH = pl.DeviceIdType.MESH
F32, BF16 = jnp.float32, jnp.bfloat16

CW = 256
N_COL = 2
BLOCKS = (128, 112, 16)
NEAR_ROWS = (240, 16)
SUB = 16
DEPTH = 4
PUT = 1
FAR, NEAR, SIB = 0, 1, 2


def kernel(d_model, a_hbm, w_hbm, r_hbm, g_hbm, hid, nrm,
           a_v, w_v, r_v, g_v, part, recv, own, st_tx, st_rx,
           a_sem, w0_sem, w_sem, r_sem, g_sem, far_tx, far_rx, near_tx, near_rx, sib_tx, sib_rx, stat_tx, stat_rx):
    t = lax.axis_index("tp")
    core, chip = t % 2, t // 2
    rows, _ = a_v.shape
    d_loc = own.shape[1]
    per = d_loc // CW
    n_blk = len(BLOCKS)
    blocks = [(sum(BLOCKS[:b]), BLOCKS[b]) for b in range(n_blk)]
    half, lanes = rows // 2, 128
    far, near, sib = 2 - 2 * chip, 3 - 2 * chip, t + 1 - 2 * core

    def cross_col(i):
        return (far + i // per) * d_loc + (i % per) * CW

    def home_col(i):
        return (sib + (t - sib) * (i // per)) * d_loc + (i % per) * CW

    def w_copy(i, col):
        return pltpu.make_async_copy(w_hbm.at[:, pl.ds(pl.multiple_of(col, CW), CW)], w_v.at[i], w_sem.at[i])

    def w_start(i):
        if isinstance(i, int):
            w_copy(i, cross_col(i) if i < 2 * per else home_col(i - 2 * per)).start()
            return

        @pl.when(i < 2 * per)
        def _():
            w_copy(i, cross_col(i)).start()

        @pl.when((i >= 2 * per) & (i < 4 * per))
        def _():
            w_copy(i, home_col(i - 2 * per)).start()

    def a_copy(q):
        sl = pl.ds(q * half, half)
        return pltpu.make_async_copy(a_hbm.at[sl, :], a_v.at[sl, :], a_sem.at[q])

    def w0_copy(q):
        src = w_hbm.at[:, pl.ds(pl.multiple_of(far * d_loc + q * lanes, lanes), lanes)]
        return pltpu.make_async_copy(src, w_v.at[0, :, pl.ds(q * lanes, lanes)], w0_sem.at[q])

    def remote(src, dst, tx, rx, peer):
        return pltpu.make_async_remote_copy(src_ref=src, dst_ref=dst, send_sem=tx, recv_sem=rx,
                                            device_id={"tp": peer}, device_id_type=MESH)

    every = pl.ds(0, rows)
    pieces = ((pl.ds(0, half), pl.ds(0, lanes)), (pl.ds(0, half), pl.ds(lanes, lanes)), (pl.ds(half, half), pl.ds(0, CW)))
    far_parts = [(every, pl.ds(j * CW, CW)) for j in range(N_COL)]
    far_parts += [(every, pl.ds(N_COL * CW, d_loc - N_COL * CW))]

    def far_copy(q, slot):
        sl = far_parts[q]
        return remote(part.at[(FAR, *sl)], recv.at[(slot, *sl)], far_tx.at[q], far_rx.at[slot, q], far)

    near_blocks = [(sum(NEAR_ROWS[:b]), NEAR_ROWS[b]) for b in range(len(NEAR_ROWS))]

    def near_copy(b, slot):
        sl = pl.ds(*near_blocks[b])
        return remote(part.at[NEAR, sl, :], recv.at[slot, sl, :], near_tx.at[b], near_rx.at[slot, b], near)

    def sib_copy():
        return remote(part.at[SIB], recv.at[SIB], sib_tx, sib_rx, sib)

    def stat_copy(k, b, slot):
        return remote(st_tx.at[b], st_rx.at[slot, b], stat_tx.at[k, b], stat_rx.at[slot, b], (far, near, sib)[k])

    barrier = pltpu.get_barrier_semaphore()
    for p in (far, near, sib):
        pl.semaphore_signal(barrier, inc=1, device_id={"tp": p}, device_id_type=MESH)
    a_copy(0).start()
    w0_copy(0).start()
    w0_copy(1).start()
    a_copy(1).start()
    r_copy = pltpu.make_async_copy(r_hbm, r_v, r_sem)
    g_copy = pltpu.make_async_copy(g_hbm, g_v, g_sem)

    def dot(lhs, rhs):
        return jnp.dot(lhs, rhs, preferred_element_type=F32)

    for q in range(3):
        if q == 0:
            a_copy(0).wait()
            w0_copy(0).wait()
            for i in range(1, DEPTH):
                w_start(i)
        elif q == 1:
            w0_copy(1).wait()
        else:
            a_copy(1).wait()
            w_start(DEPTH)
        r_sl, c_sl = pieces[q]
        part[FAR, r_sl, c_sl] = dot(a_v[r_sl, :], w_v[0, :, c_sl]).astype(BF16)

    pl.semaphore_wait(barrier, 3)
    far_copy(0, core).start()

    def chunk(i, col):
        w_copy(i, col).wait()
        w_start(i + DEPTH)
        return dot(a_v[...], w_v[i])

    def columns(j):
        return pl.ds(pl.multiple_of(j * CW, CW), CW)

    for j in range(1, N_COL):
        part[FAR, :, columns(j)] = chunk(j, cross_col(j)).astype(BF16)
        far_copy(j, core).start()

    @pl.loop(N_COL, per)
    def _(j):
        part[FAR, :, columns(j)] = chunk(j, cross_col(j)).astype(BF16)

    far_copy(len(far_parts) - 1, core).start()

    @pl.loop(0, per)
    def _(j):
        part[NEAR, :, columns(j)] = chunk(per + j, cross_col(per + j)).astype(BF16)

    for b in range(len(NEAR_ROWS)):
        near_copy(b, core).start()
    r_copy.start()
    g_copy.start()

    @pl.loop(0, per)
    def _(j):
        part[SIB, :, columns(j)] = chunk(2 * per + j, home_col(j)).astype(BF16)

    sib_copy().start()

    @pl.loop(0, per)
    def _(j):
        own[:, columns(j)] = chunk(3 * per + j, home_col(per + j))

    r_copy.wait()
    g_copy.wait()
    sib_copy().wait_recv()

    @pl.when(core == 0)
    def _():
        for q in range(len(far_parts)):
            for slot in range(2):
                far_copy(q, slot).wait_recv()

    lane = lax.broadcasted_iota(jnp.int32, (8, 128), 1)
    sub = lax.broadcasted_iota(jnp.int32, (8, 128), 0)

    def reduce_block(b):
        row, n = blocks[b]
        if row in [first for first, _ in near_blocks]:
            @pl.when(core == 1)
            def _():
                for slot in range(2):
                    near_copy([first for first, _ in near_blocks].index(row), slot).wait_recv()

        line = jnp.zeros((8, 128), F32)
        for first in range(0, n, SUB):
            sl = pl.ds(row + first, SUB)
            h = own[sl, :] + recv[SIB, sl, :].astype(F32) + recv[0, sl, :].astype(F32) + recv[1, sl, :].astype(F32)
            h = r_v[sl, :].astype(F32) + h
            own[sl, :] = h
            hid[sl, :] = h.astype(BF16)
            s = jnp.sum(h * h, axis=1, keepdims=True)
            for q in range(0, SUB, 8):
                line = line + jnp.where(lane == sub + (first + q), s[q:q + 8, :], 0.0)
        st_tx[b] = jnp.sum(line, axis=0, keepdims=True)
        for k in range(3):
            stat_copy(k, b, SIB if k == SIB else core).start()

    def norm_block(b):
        for slot in range(3):
            stat_copy(slot, b, slot).wait_recv()
        row, n = blocks[b]
        tot = (st_tx[b] + st_rx[SIB, b]) + (st_rx[0, b] + st_rx[1, b])
        scale = jnp.broadcast_to(lax.rsqrt(tot / d_model + EPS), (8, 128))
        for first in range(0, n, SUB):
            for q in range(first, first + SUB, 8):
                sl = pl.ds(row + q, 8)
                col = jnp.sum(jnp.where(lane == sub + q, scale, 0.0), axis=1, keepdims=True)
                own[sl, :] = own[sl, :] * col * g_v[...]
            sl = pl.ds(row + first, SUB)
            nrm[sl, :] = own[sl, :].astype(BF16)

    for b in range(n_blk):
        reduce_block(b)

    for b in range(n_blk):
        norm_block(b)

    for q in range(len(far_parts)):
        far_copy(q, core).wait_send()
    for b in range(len(NEAR_ROWS)):
        near_copy(b, core).wait_send()
    for b in range(n_blk):
        for k in range(3):
            stat_copy(k, b, SIB if k == SIB else core).wait_send()
    sib_copy().wait_send()


def put(hid, nrm, hid_hbm, nrm_hbm, sem):
    n = hid.shape[0] // PUT
    copies = []
    for q in range(PUT):
        sl = pl.ds(q * n, n)
        copies.append(pltpu.make_async_copy(hid.at[sl, :], hid_hbm.at[sl, :], sem.at[0, q]))
        copies.append(pltpu.make_async_copy(nrm.at[sl, :], nrm_hbm.at[sl, :], sem.at[1, q]))
    for c in copies:
        c.start()
    for c in copies:
        c.wait()


def solution(mesh):
    tp = mesh.shape["tp"]

    def local_step(a, w, r, g):
        rows, depth = a.shape
        d_loc = r.shape[1]
        per = d_loc // CW
        n_blk = len(BLOCKS)
        hbm = pl.BlockSpec(memory_space=pltpu.HBM)
        vmem = pl.BlockSpec(memory_space=pltpu.VMEM)
        dma = pltpu.SemaphoreType.DMA
        hid, nrm = pl.pallas_call(
            functools.partial(kernel, d_loc * tp),
            out_shape=(pltpu.VMEM((rows, d_loc), BF16),) * 2,
            in_specs=[hbm] * 4,
            out_specs=(vmem,) * 2,
            scratch_shapes=[
                pltpu.VMEM((rows, depth), BF16),
                pltpu.VMEM((4 * per, depth, CW), BF16),
                pltpu.VMEM((rows, d_loc), BF16),
                pltpu.VMEM((1, d_loc), F32),
                pltpu.VMEM((3, rows, d_loc), BF16),
                pltpu.VMEM((3, rows, d_loc), BF16),
                pltpu.VMEM((rows, d_loc), F32),
                pltpu.VMEM((n_blk, 1, 128), F32),
                pltpu.VMEM((3, n_blk, 1, 128), F32),
                dma((2,)), dma((2,)), dma((4 * per,)), dma, dma,
                dma((N_COL + 1,)), dma((2, N_COL + 1)), dma((len(NEAR_ROWS),)), dma((2, len(NEAR_ROWS))), dma, dma,
                dma((3, n_blk)), dma((3, n_blk)),
            ],
            compiler_params=pltpu.CompilerParams(
                collective_id=0, has_side_effects=True, vmem_limit_bytes=64946176),
            cost_estimate=pl.CostEstimate(flops=2 * rows * depth * d_loc * tp, transcendentals=0,
                                          bytes_accessed=2 * depth * d_loc * tp),
        )(a, w, r, g.reshape(1, d_loc))
        return pl.pallas_call(
            put,
            out_shape=(jax.ShapeDtypeStruct((rows, d_loc), BF16),) * 2,
            in_specs=[vmem] * 2,
            out_specs=(hbm,) * 2,
            scratch_shapes=[dma((2, PUT))],
            compiler_params=pltpu.CompilerParams(vmem_limit_bytes=1024 * 1024),
        )(hid, nrm)

    return jax.shard_map(
        local_step,
        mesh=mesh,
        in_specs=(P("data", "tp"), P("tp", None), P("data", "tp"), P("tp")),
        out_specs=(P("data", "tp"), P("data", "tp")),
        check_vma=False,
    )
```

```python
import functools

import jax
import jax.numpy as jnp
from jax import lax
from jax.experimental import pallas as pl
from jax.experimental.pallas import tpu as pltpu
from jax.sharding import PartitionSpec as P

EPS = 1e-5
MESH = pl.DeviceIdType.MESH
F32, BF16 = jnp.float32, jnp.bfloat16

CW = 256
N_COL = 2
BLOCKS = (128, 64, 48, 16)
NEAR_ROWS = (192, 48, 16)
SUB = 16
DEPTH = 4
PUT = 1
FAR, NEAR, SIB = 0, 1, 2


def kernel(d_model, a_hbm, w_hbm, r_hbm, g_hbm, hid, nrm,
           a_v, w_v, r_v, g_v, part, recv, own, st_tx, st_rx,
           a_sem, w0_sem, w_sem, r_sem, g_sem, far_tx, far_rx, near_tx, near_rx, sib_tx, sib_rx, stat_tx, stat_rx):
    t = lax.axis_index("tp")
    core, chip = t % 2, t // 2
    rows, _ = a_v.shape
    d_loc = own.shape[1]
    per = d_loc // CW
    n_blk = len(BLOCKS)
    blocks = [(sum(BLOCKS[:b]), BLOCKS[b]) for b in range(n_blk)]
    half, lanes = rows // 2, 128
    far, near, sib = 2 - 2 * chip, 3 - 2 * chip, t + 1 - 2 * core

    def cross_col(i):
        return (far + i // per) * d_loc + (i % per) * CW

    def home_col(i):
        return (sib + (t - sib) * (i // per)) * d_loc + (i % per) * CW

    def w_copy(i, col):
        return pltpu.make_async_copy(w_hbm.at[:, pl.ds(pl.multiple_of(col, CW), CW)], w_v.at[i], w_sem.at[i])

    def w_start(i):
        if isinstance(i, int):
            w_copy(i, cross_col(i) if i < 2 * per else home_col(i - 2 * per)).start()
            return

        @pl.when(i < 2 * per)
        def _():
            w_copy(i, cross_col(i)).start()

        @pl.when((i >= 2 * per) & (i < 4 * per))
        def _():
            w_copy(i, home_col(i - 2 * per)).start()

    def a_copy(q):
        sl = pl.ds(q * half, half)
        return pltpu.make_async_copy(a_hbm.at[sl, :], a_v.at[sl, :], a_sem.at[q])

    def w0_copy(q):
        src = w_hbm.at[:, pl.ds(pl.multiple_of(far * d_loc + q * lanes, lanes), lanes)]
        return pltpu.make_async_copy(src, w_v.at[0, :, pl.ds(q * lanes, lanes)], w0_sem.at[q])

    def remote(src, dst, tx, rx, peer):
        return pltpu.make_async_remote_copy(src_ref=src, dst_ref=dst, send_sem=tx, recv_sem=rx,
                                            device_id={"tp": peer}, device_id_type=MESH)

    every = pl.ds(0, rows)
    pieces = ((pl.ds(0, half), pl.ds(0, lanes)), (pl.ds(0, half), pl.ds(lanes, lanes)), (pl.ds(half, half), pl.ds(0, CW)))
    far_parts = [(every, pl.ds(j * CW, CW)) for j in range(N_COL)]
    far_parts += [(every, pl.ds(N_COL * CW, d_loc - N_COL * CW))]

    def far_copy(q, slot):
        sl = far_parts[q]
        return remote(part.at[(FAR, *sl)], recv.at[(slot, *sl)], far_tx.at[q], far_rx.at[slot, q], far)

    near_blocks = [(sum(NEAR_ROWS[:b]), NEAR_ROWS[b]) for b in range(len(NEAR_ROWS))]

    def near_copy(b, slot):
        sl = pl.ds(*near_blocks[b])
        return remote(part.at[NEAR, sl, :], recv.at[slot, sl, :], near_tx.at[b], near_rx.at[slot, b], near)

    def sib_copy():
        return remote(part.at[SIB], recv.at[SIB], sib_tx, sib_rx, sib)

    def stat_copy(k, b, slot):
        return remote(st_tx.at[b], st_rx.at[slot, b], stat_tx.at[k, b], stat_rx.at[slot, b], (far, near, sib)[k])

    barrier = pltpu.get_barrier_semaphore()
    for p in (far, near, sib):
        pl.semaphore_signal(barrier, inc=1, device_id={"tp": p}, device_id_type=MESH)
    a_copy(0).start()
    w0_copy(0).start()
    w0_copy(1).start()
    a_copy(1).start()
    r_copy = pltpu.make_async_copy(r_hbm, r_v, r_sem)
    g_copy = pltpu.make_async_copy(g_hbm, g_v, g_sem)

    def dot(lhs, rhs):
        return jnp.dot(lhs, rhs, preferred_element_type=F32)

    for q in range(3):
        if q == 0:
            a_copy(0).wait()
            w0_copy(0).wait()
            for i in range(1, DEPTH):
                w_start(i)
        elif q == 1:
            w0_copy(1).wait()
        else:
            a_copy(1).wait()
            w_start(DEPTH)
        r_sl, c_sl = pieces[q]
        part[FAR, r_sl, c_sl] = dot(a_v[r_sl, :], w_v[0, :, c_sl]).astype(BF16)

    pl.semaphore_wait(barrier, 3)
    far_copy(0, core).start()

    def chunk(i, col):
        w_copy(i, col).wait()
        w_start(i + DEPTH)
        return dot(a_v[...], w_v[i])

    def columns(j):
        return pl.ds(pl.multiple_of(j * CW, CW), CW)

    for j in range(1, N_COL):
        part[FAR, :, columns(j)] = chunk(j, cross_col(j)).astype(BF16)
        far_copy(j, core).start()

    @pl.loop(N_COL, per)
    def _(j):
        part[FAR, :, columns(j)] = chunk(j, cross_col(j)).astype(BF16)

    far_copy(len(far_parts) - 1, core).start()

    @pl.loop(0, per)
    def _(j):
        part[NEAR, :, columns(j)] = chunk(per + j, cross_col(per + j)).astype(BF16)

    for b in range(len(NEAR_ROWS)):
        near_copy(b, core).start()
    r_copy.start()
    g_copy.start()

    @pl.loop(0, per)
    def _(j):
        part[SIB, :, columns(j)] = chunk(2 * per + j, home_col(j)).astype(BF16)

    sib_copy().start()

    @pl.loop(0, per)
    def _(j):
        own[:, columns(j)] = chunk(3 * per + j, home_col(per + j))

    r_copy.wait()
    g_copy.wait()
    sib_copy().wait_recv()

    @pl.when(core == 0)
    def _():
        for q in range(len(far_parts)):
            for slot in range(2):
                far_copy(q, slot).wait_recv()

    lane = lax.broadcasted_iota(jnp.int32, (8, 128), 1)
    sub = lax.broadcasted_iota(jnp.int32, (8, 128), 0)

    def reduce_block(b):
        row, n = blocks[b]
        if row in [first for first, _ in near_blocks]:
            @pl.when(core == 1)
            def _():
                for slot in range(2):
                    near_copy([first for first, _ in near_blocks].index(row), slot).wait_recv()

        line = jnp.zeros((8, 128), F32)
        for first in range(0, n, SUB):
            sl = pl.ds(row + first, SUB)
            h = own[sl, :] + recv[SIB, sl, :].astype(F32) + recv[0, sl, :].astype(F32) + recv[1, sl, :].astype(F32)
            h = r_v[sl, :].astype(F32) + h
            own[sl, :] = h
            hid[sl, :] = h.astype(BF16)
            s = jnp.sum(h * h, axis=1, keepdims=True)
            for q in range(0, SUB, 8):
                line = line + jnp.where(lane == sub + (first + q), s[q:q + 8, :], 0.0)
        st_tx[b] = jnp.sum(line, axis=0, keepdims=True)
        for k in range(3):
            stat_copy(k, b, SIB if k == SIB else core).start()

    def norm_block(b):
        for slot in range(3):
            stat_copy(slot, b, slot).wait_recv()
        row, n = blocks[b]
        tot = (st_tx[b] + st_rx[SIB, b]) + (st_rx[0, b] + st_rx[1, b])
        scale = jnp.broadcast_to(lax.rsqrt(tot / d_model + EPS), (8, 128))
        for first in range(0, n, SUB):
            for q in range(first, first + SUB, 8):
                sl = pl.ds(row + q, 8)
                col = jnp.sum(jnp.where(lane == sub + q, scale, 0.0), axis=1, keepdims=True)
                own[sl, :] = own[sl, :] * col * g_v[...]
            sl = pl.ds(row + first, SUB)
            nrm[sl, :] = own[sl, :].astype(BF16)

    for b in range(n_blk):
        reduce_block(b)

    for b in range(n_blk):
        norm_block(b)

    for q in range(len(far_parts)):
        far_copy(q, core).wait_send()
    for b in range(len(NEAR_ROWS)):
        near_copy(b, core).wait_send()
    for b in range(n_blk):
        for k in range(3):
            stat_copy(k, b, SIB if k == SIB else core).wait_send()
    sib_copy().wait_send()


def put(hid, nrm, hid_hbm, nrm_hbm, sem):
    n = hid.shape[0] // PUT
    copies = []
    for q in range(PUT):
        sl = pl.ds(q * n, n)
        copies.append(pltpu.make_async_copy(hid.at[sl, :], hid_hbm.at[sl, :], sem.at[0, q]))
        copies.append(pltpu.make_async_copy(nrm.at[sl, :], nrm_hbm.at[sl, :], sem.at[1, q]))
    for c in copies:
        c.start()
    for c in copies:
        c.wait()


def solution(mesh):
    tp = mesh.shape["tp"]

    def local_step(a, w, r, g):
        rows, depth = a.shape
        d_loc = r.shape[1]
        per = d_loc // CW
        n_blk = len(BLOCKS)
        hbm = pl.BlockSpec(memory_space=pltpu.HBM)
        vmem = pl.BlockSpec(memory_space=pltpu.VMEM)
        dma = pltpu.SemaphoreType.DMA
        hid, nrm = pl.pallas_call(
            functools.partial(kernel, d_loc * tp),
            out_shape=(pltpu.VMEM((rows, d_loc), BF16),) * 2,
            in_specs=[hbm] * 4,
            out_specs=(vmem,) * 2,
            scratch_shapes=[
                pltpu.VMEM((rows, depth), BF16),
                pltpu.VMEM((4 * per, depth, CW), BF16),
                pltpu.VMEM((rows, d_loc), BF16),
                pltpu.VMEM((1, d_loc), F32),
                pltpu.VMEM((3, rows, d_loc), BF16),
                pltpu.VMEM((3, rows, d_loc), BF16),
                pltpu.VMEM((rows, d_loc), F32),
                pltpu.VMEM((n_blk, 1, 128), F32),
                pltpu.VMEM((3, n_blk, 1, 128), F32),
                dma((2,)), dma((2,)), dma((4 * per,)), dma, dma,
                dma((N_COL + 1,)), dma((2, N_COL + 1)), dma((len(NEAR_ROWS),)), dma((2, len(NEAR_ROWS))), dma, dma,
                dma((3, n_blk)), dma((3, n_blk)),
            ],
            compiler_params=pltpu.CompilerParams(
                collective_id=0, has_side_effects=True, vmem_limit_bytes=64946176),
            cost_estimate=pl.CostEstimate(flops=2 * rows * depth * d_loc * tp, transcendentals=0,
                                          bytes_accessed=2 * depth * d_loc * tp),
        )(a, w, r, g.reshape(1, d_loc))
        return pl.pallas_call(
            put,
            out_shape=(jax.ShapeDtypeStruct((rows, d_loc), BF16),) * 2,
            in_specs=[vmem] * 2,
            out_specs=(hbm,) * 2,
            scratch_shapes=[dma((2, PUT))],
            compiler_params=pltpu.CompilerParams(vmem_limit_bytes=1024 * 1024),
        )(hid, nrm)

    return jax.shard_map(
        local_step,
        mesh=mesh,
        in_specs=(P("data", "tp"), P("tp", None), P("data", "tp"), P("tp")),
        out_specs=(P("data", "tp"), P("data", "tp")),
        check_vma=False,
    )
```

```python
import functools

import jax
import jax.numpy as jnp
from jax import lax
from jax.experimental import pallas as pl
from jax.experimental.pallas import tpu as pltpu
from jax.sharding import PartitionSpec as P

EPS = 1e-5
MESH = pl.DeviceIdType.MESH
F32, BF16 = jnp.float32, jnp.bfloat16

CW = 256
N_COL = 2
BLOCKS = (128, 96, 32)
NEAR_ROWS = (224, 32)
SUB = 16
DEPTH = 4
PUT = 1
FAR, NEAR, SIB = 0, 1, 2


def kernel(d_model, a_hbm, w_hbm, r_hbm, g_hbm, hid, nrm,
           a_v, w_v, r_v, g_v, part, recv, own, st_tx, st_rx,
           a_sem, w0_sem, w_sem, r_sem, g_sem, far_tx, far_rx, near_tx, near_rx, sib_tx, sib_rx, stat_tx, stat_rx):
    t = lax.axis_index("tp")
    core, chip = t % 2, t // 2
    rows, _ = a_v.shape
    d_loc = own.shape[1]
    per = d_loc // CW
    n_blk = len(BLOCKS)
    blocks = [(sum(BLOCKS[:b]), BLOCKS[b]) for b in range(n_blk)]
    half, lanes = rows // 2, 128
    far, near, sib = 2 - 2 * chip, 3 - 2 * chip, t + 1 - 2 * core

    def cross_col(i):
        return (far + i // per) * d_loc + (i % per) * CW

    def home_col(i):
        return (sib + (t - sib) * (i // per)) * d_loc + (i % per) * CW

    def w_copy(i, col):
        return pltpu.make_async_copy(w_hbm.at[:, pl.ds(pl.multiple_of(col, CW), CW)], w_v.at[i], w_sem.at[i])

    def w_start(i):
        if isinstance(i, int):
            w_copy(i, cross_col(i) if i < 2 * per else home_col(i - 2 * per)).start()
            return

        @pl.when(i < 2 * per)
        def _():
            w_copy(i, cross_col(i)).start()

        @pl.when((i >= 2 * per) & (i < 4 * per))
        def _():
            w_copy(i, home_col(i - 2 * per)).start()

    def a_copy(q):
        sl = pl.ds(q * half, half)
        return pltpu.make_async_copy(a_hbm.at[sl, :], a_v.at[sl, :], a_sem.at[q])

    def w0_copy(q):
        src = w_hbm.at[:, pl.ds(pl.multiple_of(far * d_loc + q * lanes, lanes), lanes)]
        return pltpu.make_async_copy(src, w_v.at[0, :, pl.ds(q * lanes, lanes)], w0_sem.at[q])

    def remote(src, dst, tx, rx, peer):
        return pltpu.make_async_remote_copy(src_ref=src, dst_ref=dst, send_sem=tx, recv_sem=rx,
                                            device_id={"tp": peer}, device_id_type=MESH)

    every = pl.ds(0, rows)
    pieces = ((pl.ds(0, half), pl.ds(0, lanes)), (pl.ds(0, half), pl.ds(lanes, lanes)), (pl.ds(half, half), pl.ds(0, CW)))
    far_parts = [(every, pl.ds(j * CW, CW)) for j in range(N_COL)]
    far_parts += [(every, pl.ds(N_COL * CW, d_loc - N_COL * CW))]

    def far_copy(q, slot):
        sl = far_parts[q]
        return remote(part.at[(FAR, *sl)], recv.at[(slot, *sl)], far_tx.at[q], far_rx.at[slot, q], far)

    near_blocks = [(sum(NEAR_ROWS[:b]), NEAR_ROWS[b]) for b in range(len(NEAR_ROWS))]

    def near_copy(b, slot):
        sl = pl.ds(*near_blocks[b])
        return remote(part.at[NEAR, sl, :], recv.at[slot, sl, :], near_tx.at[b], near_rx.at[slot, b], near)

    def sib_copy():
        return remote(part.at[SIB], recv.at[SIB], sib_tx, sib_rx, sib)

    def stat_copy(k, b, slot):
        return remote(st_tx.at[b], st_rx.at[slot, b], stat_tx.at[k, b], stat_rx.at[slot, b], (far, near, sib)[k])

    barrier = pltpu.get_barrier_semaphore()
    for p in (far, near, sib):
        pl.semaphore_signal(barrier, inc=1, device_id={"tp": p}, device_id_type=MESH)
    a_copy(0).start()
    w0_copy(0).start()
    w0_copy(1).start()
    a_copy(1).start()
    r_copy = pltpu.make_async_copy(r_hbm, r_v, r_sem)
    g_copy = pltpu.make_async_copy(g_hbm, g_v, g_sem)

    def dot(lhs, rhs):
        return jnp.dot(lhs, rhs, preferred_element_type=F32)

    for q in range(3):
        if q == 0:
            a_copy(0).wait()
            w0_copy(0).wait()
            for i in range(1, DEPTH):
                w_start(i)
        elif q == 1:
            w0_copy(1).wait()
        else:
            a_copy(1).wait()
            w_start(DEPTH)
        r_sl, c_sl = pieces[q]
        part[FAR, r_sl, c_sl] = dot(a_v[r_sl, :], w_v[0, :, c_sl]).astype(BF16)

    pl.semaphore_wait(barrier, 3)
    far_copy(0, core).start()

    def chunk(i, col):
        w_copy(i, col).wait()
        w_start(i + DEPTH)
        return dot(a_v[...], w_v[i])

    def columns(j):
        return pl.ds(pl.multiple_of(j * CW, CW), CW)

    for j in range(1, N_COL):
        part[FAR, :, columns(j)] = chunk(j, cross_col(j)).astype(BF16)
        far_copy(j, core).start()

    @pl.loop(N_COL, per)
    def _(j):
        part[FAR, :, columns(j)] = chunk(j, cross_col(j)).astype(BF16)

    far_copy(len(far_parts) - 1, core).start()

    @pl.loop(0, per)
    def _(j):
        part[NEAR, :, columns(j)] = chunk(per + j, cross_col(per + j)).astype(BF16)

    for b in range(len(NEAR_ROWS)):
        near_copy(b, core).start()
    r_copy.start()
    g_copy.start()

    @pl.loop(0, per)
    def _(j):
        part[SIB, :, columns(j)] = chunk(2 * per + j, home_col(j)).astype(BF16)

    sib_copy().start()

    @pl.loop(0, per)
    def _(j):
        own[:, columns(j)] = chunk(3 * per + j, home_col(per + j))

    r_copy.wait()
    g_copy.wait()
    sib_copy().wait_recv()

    @pl.when(core == 0)
    def _():
        for q in range(len(far_parts)):
            for slot in range(2):
                far_copy(q, slot).wait_recv()

    lane = lax.broadcasted_iota(jnp.int32, (8, 128), 1)
    sub = lax.broadcasted_iota(jnp.int32, (8, 128), 0)

    def reduce_block(b):
        row, n = blocks[b]
        if row in [first for first, _ in near_blocks]:
            @pl.when(core == 1)
            def _():
                for slot in range(2):
                    near_copy([first for first, _ in near_blocks].index(row), slot).wait_recv()

        line = jnp.zeros((8, 128), F32)
        for first in range(0, n, SUB):
            sl = pl.ds(row + first, SUB)
            h = own[sl, :] + recv[SIB, sl, :].astype(F32) + recv[0, sl, :].astype(F32) + recv[1, sl, :].astype(F32)
            h = r_v[sl, :].astype(F32) + h
            own[sl, :] = h
            hid[sl, :] = h.astype(BF16)
            s = jnp.sum(h * h, axis=1, keepdims=True)
            for q in range(0, SUB, 8):
                line = line + jnp.where(lane == sub + (first + q), s[q:q + 8, :], 0.0)
        st_tx[b] = jnp.sum(line, axis=0, keepdims=True)
        for k in range(3):
            stat_copy(k, b, SIB if k == SIB else core).start()

    def norm_block(b):
        for slot in range(3):
            stat_copy(slot, b, slot).wait_recv()
        row, n = blocks[b]
        tot = (st_tx[b] + st_rx[SIB, b]) + (st_rx[0, b] + st_rx[1, b])
        scale = jnp.broadcast_to(lax.rsqrt(tot / d_model + EPS), (8, 128))
        for first in range(0, n, SUB):
            for q in range(first, first + SUB, 8):
                sl = pl.ds(row + q, 8)
                col = jnp.sum(jnp.where(lane == sub + q, scale, 0.0), axis=1, keepdims=True)
                own[sl, :] = own[sl, :] * col * g_v[...]
            sl = pl.ds(row + first, SUB)
            nrm[sl, :] = own[sl, :].astype(BF16)

    for b in range(n_blk):
        reduce_block(b)

    for b in range(n_blk):
        norm_block(b)

    for q in range(len(far_parts)):
        far_copy(q, core).wait_send()
    for b in range(len(NEAR_ROWS)):
        near_copy(b, core).wait_send()
    for b in range(n_blk):
        for k in range(3):
            stat_copy(k, b, SIB if k == SIB else core).wait_send()
    sib_copy().wait_send()


def put(hid, nrm, hid_hbm, nrm_hbm, sem):
    n = hid.shape[0] // PUT
    copies = []
    for q in range(PUT):
        sl = pl.ds(q * n, n)
        copies.append(pltpu.make_async_copy(hid.at[sl, :], hid_hbm.at[sl, :], sem.at[0, q]))
        copies.append(pltpu.make_async_copy(nrm.at[sl, :], nrm_hbm.at[sl, :], sem.at[1, q]))
    for c in copies:
        c.start()
    for c in copies:
        c.wait()


def solution(mesh):
    tp = mesh.shape["tp"]

    def local_step(a, w, r, g):
        rows, depth = a.shape
        d_loc = r.shape[1]
        per = d_loc // CW
        n_blk = len(BLOCKS)
        hbm = pl.BlockSpec(memory_space=pltpu.HBM)
        vmem = pl.BlockSpec(memory_space=pltpu.VMEM)
        dma = pltpu.SemaphoreType.DMA
        hid, nrm = pl.pallas_call(
            functools.partial(kernel, d_loc * tp),
            out_shape=(pltpu.VMEM((rows, d_loc), BF16),) * 2,
            in_specs=[hbm] * 4,
            out_specs=(vmem,) * 2,
            scratch_shapes=[
                pltpu.VMEM((rows, depth), BF16),
                pltpu.VMEM((4 * per, depth, CW), BF16),
                pltpu.VMEM((rows, d_loc), BF16),
                pltpu.VMEM((1, d_loc), F32),
                pltpu.VMEM((3, rows, d_loc), BF16),
                pltpu.VMEM((3, rows, d_loc), BF16),
                pltpu.VMEM((rows, d_loc), F32),
                pltpu.VMEM((n_blk, 1, 128), F32),
                pltpu.VMEM((3, n_blk, 1, 128), F32),
                dma((2,)), dma((2,)), dma((4 * per,)), dma, dma,
                dma((N_COL + 1,)), dma((2, N_COL + 1)), dma((len(NEAR_ROWS),)), dma((2, len(NEAR_ROWS))), dma, dma,
                dma((3, n_blk)), dma((3, n_blk)),
            ],
            compiler_params=pltpu.CompilerParams(
                collective_id=0, has_side_effects=True, vmem_limit_bytes=64946176),
            cost_estimate=pl.CostEstimate(flops=2 * rows * depth * d_loc * tp, transcendentals=0,
                                          bytes_accessed=2 * depth * d_loc * tp),
        )(a, w, r, g.reshape(1, d_loc))
        return pl.pallas_call(
            put,
            out_shape=(jax.ShapeDtypeStruct((rows, d_loc), BF16),) * 2,
            in_specs=[vmem] * 2,
            out_specs=(hbm,) * 2,
            scratch_shapes=[dma((2, PUT))],
            compiler_params=pltpu.CompilerParams(vmem_limit_bytes=1024 * 1024),
        )(hid, nrm)

    return jax.shard_map(
        local_step,
        mesh=mesh,
        in_specs=(P("data", "tp"), P("tp", None), P("data", "tp"), P("tp")),
        out_specs=(P("data", "tp"), P("data", "tp")),
        check_vma=False,
    )
```

```python
import functools

import jax
import jax.numpy as jnp
from jax import lax
from jax.experimental import pallas as pl
from jax.experimental.pallas import tpu as pltpu
from jax.sharding import PartitionSpec as P

EPS = 1e-5
MESH = pl.DeviceIdType.MESH
F32, BF16 = jnp.float32, jnp.bfloat16

CW = 256
N_COL = 2
BLOCKS = (128, 112, 16)
NEAR_ROWS = (240, 16)
SUB = 16
DEPTH = 4
PUT = 1
FAR, NEAR, SIB = 0, 1, 2


def kernel(d_model, a_hbm, w_hbm, r_hbm, g_hbm, hid, nrm,
           a_v, w_v, r_v, g_v, part, recv, own, st_tx, st_rx,
           a_sem, w0_sem, w_sem, r_sem, g_sem, far_tx, far_rx, near_tx, near_rx, sib_tx, sib_rx, stat_tx, stat_rx):
    t = lax.axis_index("tp")
    core, chip = t % 2, t // 2
    rows, _ = a_v.shape
    d_loc = own.shape[1]
    per = d_loc // CW
    n_blk = len(BLOCKS)
    blocks = [(sum(BLOCKS[:b]), BLOCKS[b]) for b in range(n_blk)]
    half, lanes = rows // 2, 128
    far, near, sib = 2 - 2 * chip, 3 - 2 * chip, t + 1 - 2 * core

    def cross_col(i):
        return (far + i // per) * d_loc + (i % per) * CW

    def home_col(i):
        return (sib + (t - sib) * (i // per)) * d_loc + (i % per) * CW

    def w_copy(i, col):
        return pltpu.make_async_copy(w_hbm.at[:, pl.ds(pl.multiple_of(col, CW), CW)], w_v.at[i], w_sem.at[i])

    def w_start(i):
        if isinstance(i, int):
            w_copy(i, cross_col(i) if i < 2 * per else home_col(i - 2 * per)).start()
            return

        @pl.when(i < 2 * per)
        def _():
            w_copy(i, cross_col(i)).start()

        @pl.when((i >= 2 * per) & (i < 4 * per))
        def _():
            w_copy(i, home_col(i - 2 * per)).start()

    def a_copy(q):
        sl = pl.ds(q * half, half)
        return pltpu.make_async_copy(a_hbm.at[sl, :], a_v.at[sl, :], a_sem.at[q])

    def w0_copy(q):
        src = w_hbm.at[:, pl.ds(pl.multiple_of(far * d_loc + q * lanes, lanes), lanes)]
        return pltpu.make_async_copy(src, w_v.at[0, :, pl.ds(q * lanes, lanes)], w0_sem.at[q])

    def remote(src, dst, tx, rx, peer):
        return pltpu.make_async_remote_copy(src_ref=src, dst_ref=dst, send_sem=tx, recv_sem=rx,
                                            device_id={"tp": peer}, device_id_type=MESH)

    every = pl.ds(0, rows)
    pieces = ((pl.ds(0, half), pl.ds(0, lanes)), (pl.ds(0, half), pl.ds(lanes, lanes)), (pl.ds(half, half), pl.ds(0, CW)))
    far_parts = [(every, pl.ds(j * CW, CW)) for j in range(N_COL)]
    far_parts += [(every, pl.ds(N_COL * CW, d_loc - N_COL * CW))]

    def far_copy(q, slot):
        sl = far_parts[q]
        return remote(part.at[(FAR, *sl)], recv.at[(slot, *sl)], far_tx.at[q], far_rx.at[slot, q], far)

    near_blocks = [(sum(NEAR_ROWS[:b]), NEAR_ROWS[b]) for b in range(len(NEAR_ROWS))]

    def near_copy(b, slot):
        sl = pl.ds(*near_blocks[b])
        return remote(part.at[NEAR, sl, :], recv.at[slot, sl, :], near_tx.at[b], near_rx.at[slot, b], near)

    def sib_copy():
        return remote(part.at[SIB], recv.at[SIB], sib_tx, sib_rx, sib)

    def stat_copy(k, b, slot):
        return remote(st_tx.at[b], st_rx.at[slot, b], stat_tx.at[k, b], stat_rx.at[slot, b], (far, near, sib)[k])

    barrier = pltpu.get_barrier_semaphore()
    for p in (far, near, sib):
        pl.semaphore_signal(barrier, inc=1, device_id={"tp": p}, device_id_type=MESH)
    a_copy(0).start()
    w0_copy(0).start()
    w0_copy(1).start()
    a_copy(1).start()
    r_copy = pltpu.make_async_copy(r_hbm, r_v, r_sem)
    g_copy = pltpu.make_async_copy(g_hbm, g_v, g_sem)

    def dot(lhs, rhs):
        return jnp.dot(lhs, rhs, preferred_element_type=F32)

    for q in range(3):
        if q == 0:
            a_copy(0).wait()
            w0_copy(0).wait()
            for i in range(1, DEPTH):
                w_start(i)
        elif q == 1:
            w0_copy(1).wait()
        else:
            a_copy(1).wait()
            w_start(DEPTH)
        r_sl, c_sl = pieces[q]
        part[FAR, r_sl, c_sl] = dot(a_v[r_sl, :], w_v[0, :, c_sl]).astype(BF16)

    pl.semaphore_wait(barrier, 3)
    far_copy(0, core).start()

    def chunk(i, col):
        w_copy(i, col).wait()
        w_start(i + DEPTH)
        return dot(a_v[...], w_v[i])

    def columns(j):
        return pl.ds(pl.multiple_of(j * CW, CW), CW)

    for j in range(1, N_COL):
        part[FAR, :, columns(j)] = chunk(j, cross_col(j)).astype(BF16)
        far_copy(j, core).start()

    @pl.loop(N_COL, per)
    def _(j):
        part[FAR, :, columns(j)] = chunk(j, cross_col(j)).astype(BF16)

    far_copy(len(far_parts) - 1, core).start()

    @pl.loop(0, per)
    def _(j):
        part[NEAR, :, columns(j)] = chunk(per + j, cross_col(per + j)).astype(BF16)

    for b in range(len(NEAR_ROWS)):
        near_copy(b, core).start()
    r_copy.start()
    g_copy.start()

    @pl.loop(0, per)
    def _(j):
        part[SIB, :, columns(j)] = chunk(2 * per + j, home_col(j)).astype(BF16)

    sib_copy().start()

    @pl.loop(0, per)
    def _(j):
        own[:, columns(j)] = chunk(3 * per + j, home_col(per + j))

    r_copy.wait()
    g_copy.wait()
    sib_copy().wait_recv()

    @pl.loop(0, rows // SUB)
    def _(i):
        sl = pl.ds(pl.multiple_of(i * SUB, SUB), SUB)
        own[sl, :] = (own[sl, :] + recv[SIB, sl, :].astype(F32)) + r_v[sl, :].astype(F32)

    @pl.when(core == 0)
    def _():
        for q in range(len(far_parts)):
            for slot in range(2):
                far_copy(q, slot).wait_recv()

    lane = lax.broadcasted_iota(jnp.int32, (8, 128), 1)
    sub = lax.broadcasted_iota(jnp.int32, (8, 128), 0)

    def reduce_block(b):
        row, n = blocks[b]
        if row in [first for first, _ in near_blocks]:
            @pl.when(core == 1)
            def _():
                for slot in range(2):
                    near_copy([first for first, _ in near_blocks].index(row), slot).wait_recv()

        line = jnp.zeros((8, 128), F32)
        for first in range(0, n, SUB):
            sl = pl.ds(row + first, SUB)
            h = own[sl, :] + (recv[0, sl, :].astype(F32) + recv[1, sl, :].astype(F32))
            own[sl, :] = h
            hid[sl, :] = h.astype(BF16)
            s = jnp.sum(h * h, axis=1, keepdims=True)
            for q in range(0, SUB, 8):
                line = line + jnp.where(lane == sub + (first + q), s[q:q + 8, :], 0.0)
        st_tx[b] = jnp.sum(line, axis=0, keepdims=True)
        for k in range(3):
            stat_copy(k, b, SIB if k == SIB else core).start()

    def norm_block(b):
        for slot in range(3):
            stat_copy(slot, b, slot).wait_recv()
        row, n = blocks[b]
        tot = (st_tx[b] + st_rx[SIB, b]) + (st_rx[0, b] + st_rx[1, b])
        scale = jnp.broadcast_to(lax.rsqrt(tot / d_model + EPS), (8, 128))
        for first in range(0, n, SUB):
            for q in range(first, first + SUB, 8):
                sl = pl.ds(row + q, 8)
                col = jnp.sum(jnp.where(lane == sub + q, scale, 0.0), axis=1, keepdims=True)
                own[sl, :] = own[sl, :] * col * g_v[...]
            sl = pl.ds(row + first, SUB)
            nrm[sl, :] = own[sl, :].astype(BF16)

    for b in range(n_blk):
        reduce_block(b)

    for b in range(n_blk):
        norm_block(b)

    for q in range(len(far_parts)):
        far_copy(q, core).wait_send()
    for b in range(len(NEAR_ROWS)):
        near_copy(b, core).wait_send()
    for b in range(n_blk):
        for k in range(3):
            stat_copy(k, b, SIB if k == SIB else core).wait_send()
    sib_copy().wait_send()


def put(hid, nrm, hid_hbm, nrm_hbm, sem):
    n = hid.shape[0] // PUT
    copies = []
    for q in range(PUT):
        sl = pl.ds(q * n, n)
        copies.append(pltpu.make_async_copy(hid.at[sl, :], hid_hbm.at[sl, :], sem.at[0, q]))
        copies.append(pltpu.make_async_copy(nrm.at[sl, :], nrm_hbm.at[sl, :], sem.at[1, q]))
    for c in copies:
        c.start()
    for c in copies:
        c.wait()


def solution(mesh):
    tp = mesh.shape["tp"]

    def local_step(a, w, r, g):
        rows, depth = a.shape
        d_loc = r.shape[1]
        per = d_loc // CW
        n_blk = len(BLOCKS)
        hbm = pl.BlockSpec(memory_space=pltpu.HBM)
        vmem = pl.BlockSpec(memory_space=pltpu.VMEM)
        dma = pltpu.SemaphoreType.DMA
        hid, nrm = pl.pallas_call(
            functools.partial(kernel, d_loc * tp),
            out_shape=(pltpu.VMEM((rows, d_loc), BF16),) * 2,
            in_specs=[hbm] * 4,
            out_specs=(vmem,) * 2,
            scratch_shapes=[
                pltpu.VMEM((rows, depth), BF16),
                pltpu.VMEM((4 * per, depth, CW), BF16),
                pltpu.VMEM((rows, d_loc), BF16),
                pltpu.VMEM((1, d_loc), F32),
                pltpu.VMEM((3, rows, d_loc), BF16),
                pltpu.VMEM((3, rows, d_loc), BF16),
                pltpu.VMEM((rows, d_loc), F32),
                pltpu.VMEM((n_blk, 1, 128), F32),
                pltpu.VMEM((3, n_blk, 1, 128), F32),
                dma((2,)), dma((2,)), dma((4 * per,)), dma, dma,
                dma((N_COL + 1,)), dma((2, N_COL + 1)), dma((len(NEAR_ROWS),)), dma((2, len(NEAR_ROWS))), dma, dma,
                dma((3, n_blk)), dma((3, n_blk)),
            ],
            compiler_params=pltpu.CompilerParams(
                collective_id=0, has_side_effects=True, vmem_limit_bytes=64946176),
            cost_estimate=pl.CostEstimate(flops=2 * rows * depth * d_loc * tp, transcendentals=0,
                                          bytes_accessed=2 * depth * d_loc * tp),
        )(a, w, r, g.reshape(1, d_loc))
        return pl.pallas_call(
            put,
            out_shape=(jax.ShapeDtypeStruct((rows, d_loc), BF16),) * 2,
            in_specs=[vmem] * 2,
            out_specs=(hbm,) * 2,
            scratch_shapes=[dma((2, PUT))],
            compiler_params=pltpu.CompilerParams(vmem_limit_bytes=1024 * 1024),
        )(hid, nrm)

    return jax.shard_map(
        local_step,
        mesh=mesh,
        in_specs=(P("data", "tp"), P("tp", None), P("data", "tp"), P("tp")),
        out_specs=(P("data", "tp"), P("data", "tp")),
        check_vma=False,
    )
```

```python
import functools

import jax
import jax.numpy as jnp
from jax import lax
from jax.experimental import pallas as pl
from jax.experimental.pallas import tpu as pltpu
from jax.sharding import PartitionSpec as P

EPS = 1e-5
MESH = pl.DeviceIdType.MESH
F32, BF16 = jnp.float32, jnp.bfloat16

CW = 256
N_COL = 2
BLOCKS = (128, 112, 16)
NEAR_ROWS = (240, 16)
SUB = 16
DEPTH = 4
PUT = 1
FAR, NEAR, SIB = 0, 1, 2


def kernel(d_model, a_hbm, w_hbm, r_hbm, g_hbm, hid, nrm,
           a_v, w_v, r_v, g_v, part, recv, own, st_tx, st_rx,
           a_sem, w0_sem, w_sem, r_sem, g_sem, far_tx, far_rx, near_tx, near_rx, sib_tx, sib_rx, stat_tx, stat_rx):
    t = lax.axis_index("tp")
    core, chip = t % 2, t // 2
    rows, _ = a_v.shape
    d_loc = own.shape[1]
    per = d_loc // CW
    n_blk = len(BLOCKS)
    blocks = [(sum(BLOCKS[:b]), BLOCKS[b]) for b in range(n_blk)]
    half, lanes = rows // 2, 128
    far, near, sib = 2 - 2 * chip, 3 - 2 * chip, t + 1 - 2 * core

    def cross_col(i):
        return (far + i // per) * d_loc + (i % per) * CW

    def home_col(i):
        return (sib + (t - sib) * (i // per)) * d_loc + (i % per) * CW

    def w_copy(i, col):
        return pltpu.make_async_copy(w_hbm.at[:, pl.ds(pl.multiple_of(col, CW), CW)], w_v.at[i], w_sem.at[i])

    def w_start(i):
        if isinstance(i, int):
            w_copy(i, cross_col(i) if i < 2 * per else home_col(i - 2 * per)).start()
            return

        @pl.when(i < 2 * per)
        def _():
            w_copy(i, cross_col(i)).start()

        @pl.when((i >= 2 * per) & (i < 4 * per))
        def _():
            w_copy(i, home_col(i - 2 * per)).start()

    def a_copy(q):
        sl = pl.ds(q * half, half)
        return pltpu.make_async_copy(a_hbm.at[sl, :], a_v.at[sl, :], a_sem.at[q])

    def w0_copy(q):
        src = w_hbm.at[:, pl.ds(pl.multiple_of(far * d_loc + q * lanes, lanes), lanes)]
        return pltpu.make_async_copy(src, w_v.at[0, :, pl.ds(q * lanes, lanes)], w0_sem.at[q])

    def remote(src, dst, tx, rx, peer):
        return pltpu.make_async_remote_copy(src_ref=src, dst_ref=dst, send_sem=tx, recv_sem=rx,
                                            device_id={"tp": peer}, device_id_type=MESH)

    every = pl.ds(0, rows)
    pieces = ((pl.ds(0, half), pl.ds(0, lanes)), (pl.ds(0, half), pl.ds(lanes, lanes)), (pl.ds(half, half), pl.ds(0, CW)))
    far_parts = [(every, pl.ds(j * CW, CW)) for j in range(N_COL)]
    far_parts += [(every, pl.ds(N_COL * CW, d_loc - N_COL * CW))]

    def far_copy(q, slot):
        sl = far_parts[q]
        return remote(part.at[(FAR, *sl)], recv.at[(slot, *sl)], far_tx.at[q], far_rx.at[slot, q], far)

    near_blocks = [(sum(NEAR_ROWS[:b]), NEAR_ROWS[b]) for b in range(len(NEAR_ROWS))]

    def near_copy(b, slot):
        sl = pl.ds(*near_blocks[b])
        return remote(part.at[NEAR, sl, :], recv.at[slot, sl, :], near_tx.at[b], near_rx.at[slot, b], near)

    def sib_copy():
        return remote(part.at[SIB], recv.at[SIB], sib_tx, sib_rx, sib)

    def stat_copy(k, b, slot):
        return remote(st_tx.at[b], st_rx.at[slot, b], stat_tx.at[k, b], stat_rx.at[slot, b], (far, near, sib)[k])

    barrier = pltpu.get_barrier_semaphore()
    for p in (far, near, sib):
        pl.semaphore_signal(barrier, inc=1, device_id={"tp": p}, device_id_type=MESH)
    a_copy(0).start()
    w0_copy(0).start()
    w0_copy(1).start()
    a_copy(1).start()
    r_copy = pltpu.make_async_copy(r_hbm, r_v, r_sem)
    g_copy = pltpu.make_async_copy(g_hbm, g_v, g_sem)

    def dot(lhs, rhs):
        return jnp.dot(lhs, rhs, preferred_element_type=F32)

    for q in range(3):
        if q == 0:
            a_copy(0).wait()
            w0_copy(0).wait()
            for i in range(1, DEPTH):
                w_start(i)
        elif q == 1:
            w0_copy(1).wait()
        else:
            a_copy(1).wait()
            w_start(DEPTH)
        r_sl, c_sl = pieces[q]
        part[FAR, r_sl, c_sl] = dot(a_v[r_sl, :], w_v[0, :, c_sl]).astype(BF16)

    pl.semaphore_wait(barrier, 3)
    far_copy(0, core).start()

    def chunk(i, col):
        w_copy(i, col).wait()
        w_start(i + DEPTH)
        return dot(a_v[...], w_v[i])

    def columns(j):
        return pl.ds(pl.multiple_of(j * CW, CW), CW)

    for j in range(1, N_COL):
        part[FAR, :, columns(j)] = chunk(j, cross_col(j)).astype(BF16)
        far_copy(j, core).start()

    @pl.loop(N_COL, per)
    def _(j):
        part[FAR, :, columns(j)] = chunk(j, cross_col(j)).astype(BF16)

    far_copy(len(far_parts) - 1, core).start()

    @pl.loop(0, per)
    def _(j):
        part[NEAR, :, columns(j)] = chunk(per + j, cross_col(per + j)).astype(BF16)

    for b in range(len(NEAR_ROWS)):
        near_copy(b, core).start()
    r_copy.start()
    g_copy.start()

    @pl.loop(0, per)
    def _(j):
        part[SIB, :, columns(j)] = chunk(2 * per + j, home_col(j)).astype(BF16)

    sib_copy().start()

    @pl.loop(0, per)
    def _(j):
        own[:, columns(j)] = chunk(3 * per + j, home_col(per + j))

    r_copy.wait()
    g_copy.wait()
    sib_copy().wait_recv()

    @pl.loop(0, rows // SUB)
    def _(i):
        sl = pl.ds(pl.multiple_of(i * SUB, SUB), SUB)
        own[sl, :] = (own[sl, :] + recv[SIB, sl, :].astype(F32)) + r_v[sl, :].astype(F32)

    @pl.when(core == 0)
    def _():
        for q in range(len(far_parts)):
            for slot in range(2):
                far_copy(q, slot).wait_recv()

    lane = lax.broadcasted_iota(jnp.int32, (8, 128), 1)
    sub = lax.broadcasted_iota(jnp.int32, (8, 128), 0)

    def reduce_block(b):
        row, n = blocks[b]
        if row in [first for first, _ in near_blocks]:
            @pl.when(core == 1)
            def _():
                for slot in range(2):
                    near_copy([first for first, _ in near_blocks].index(row), slot).wait_recv()

        line = jnp.zeros((8, 128), F32)
        for first in range(0, n, SUB):
            sl = pl.ds(row + first, SUB)
            h = own[sl, :] + (recv[0, sl, :].astype(F32) + recv[1, sl, :].astype(F32))
            own[sl, :] = h
            hid[sl, :] = h.astype(BF16)
            s = jnp.sum(h * h, axis=1, keepdims=True)
            for q in range(0, SUB, 8):
                line = line + jnp.where(lane == sub + (first + q), s[q:q + 8, :], 0.0)
        st_tx[b] = jnp.sum(line, axis=0, keepdims=True)
        for k in range(3):
            stat_copy(k, b, SIB if k == SIB else core).start()

    def norm_block(b):
        for slot in range(3):
            stat_copy(slot, b, slot).wait_recv()
        row, n = blocks[b]
        tot = (st_tx[b] + st_rx[SIB, b]) + (st_rx[0, b] + st_rx[1, b])
        scale = jnp.broadcast_to(lax.rsqrt(tot / d_model + EPS), (8, 128))
        for first in range(0, n, SUB):
            out = []
            for q in range(first, first + SUB, 8):
                col = jnp.sum(jnp.where(lane == sub + q, scale, 0.0), axis=1, keepdims=True)
                out.append(own[pl.ds(row + q, 8), :] * col * g_v[...])
            nrm[pl.ds(row + first, SUB), :] = jnp.concatenate(out, axis=0).astype(BF16)

    for b in range(n_blk):
        reduce_block(b)

    for b in range(n_blk):
        norm_block(b)

    for q in range(len(far_parts)):
        far_copy(q, core).wait_send()
    for b in range(len(NEAR_ROWS)):
        near_copy(b, core).wait_send()
    for b in range(n_blk):
        for k in range(3):
            stat_copy(k, b, SIB if k == SIB else core).wait_send()
    sib_copy().wait_send()


def put(hid, nrm, hid_hbm, nrm_hbm, sem):
    n = hid.shape[0] // PUT
    copies = []
    for q in range(PUT):
        sl = pl.ds(q * n, n)
        copies.append(pltpu.make_async_copy(hid.at[sl, :], hid_hbm.at[sl, :], sem.at[0, q]))
        copies.append(pltpu.make_async_copy(nrm.at[sl, :], nrm_hbm.at[sl, :], sem.at[1, q]))
    for c in copies:
        c.start()
    for c in copies:
        c.wait()


def solution(mesh):
    tp = mesh.shape["tp"]

    def local_step(a, w, r, g):
        rows, depth = a.shape
        d_loc = r.shape[1]
        per = d_loc // CW
        n_blk = len(BLOCKS)
        hbm = pl.BlockSpec(memory_space=pltpu.HBM)
        vmem = pl.BlockSpec(memory_space=pltpu.VMEM)
        dma = pltpu.SemaphoreType.DMA
        hid, nrm = pl.pallas_call(
            functools.partial(kernel, d_loc * tp),
            out_shape=(pltpu.VMEM((rows, d_loc), BF16),) * 2,
            in_specs=[hbm] * 4,
            out_specs=(vmem,) * 2,
            scratch_shapes=[
                pltpu.VMEM((rows, depth), BF16),
                pltpu.VMEM((4 * per, depth, CW), BF16),
                pltpu.VMEM((rows, d_loc), BF16),
                pltpu.VMEM((1, d_loc), F32),
                pltpu.VMEM((3, rows, d_loc), BF16),
                pltpu.VMEM((3, rows, d_loc), BF16),
                pltpu.VMEM((rows, d_loc), F32),
                pltpu.VMEM((n_blk, 1, 128), F32),
                pltpu.VMEM((3, n_blk, 1, 128), F32),
                dma((2,)), dma((2,)), dma((4 * per,)), dma, dma,
                dma((N_COL + 1,)), dma((2, N_COL + 1)), dma((len(NEAR_ROWS),)), dma((2, len(NEAR_ROWS))), dma, dma,
                dma((3, n_blk)), dma((3, n_blk)),
            ],
            compiler_params=pltpu.CompilerParams(
                collective_id=0, has_side_effects=True, vmem_limit_bytes=64946176),
            cost_estimate=pl.CostEstimate(flops=2 * rows * depth * d_loc * tp, transcendentals=0,
                                          bytes_accessed=2 * depth * d_loc * tp),
        )(a, w, r, g.reshape(1, d_loc))
        return pl.pallas_call(
            put,
            out_shape=(jax.ShapeDtypeStruct((rows, d_loc), BF16),) * 2,
            in_specs=[vmem] * 2,
            out_specs=(hbm,) * 2,
            scratch_shapes=[dma((2, PUT))],
            compiler_params=pltpu.CompilerParams(vmem_limit_bytes=1024 * 1024),
        )(hid, nrm)

    return jax.shard_map(
        local_step,
        mesh=mesh,
        in_specs=(P("data", "tp"), P("tp", None), P("data", "tp"), P("tp")),
        out_specs=(P("data", "tp"), P("data", "tp")),
        check_vma=False,
    )
```

```python
import functools

import jax
import jax.numpy as jnp
from jax import lax
from jax.experimental import pallas as pl
from jax.experimental.pallas import tpu as pltpu
from jax.sharding import PartitionSpec as P

EPS = 1e-5
MESH = pl.DeviceIdType.MESH
F32, BF16 = jnp.float32, jnp.bfloat16

CW = 256
N_COL = 2
BLOCKS = (128, 112, 16)
NEAR_ROWS = (240, 16)
SUB = 16
DEPTH = 4
PUT = 1
FAR, NEAR, SIB = 0, 1, 2


def kernel(d_model, a_hbm, w_hbm, r_hbm, g_hbm, hid, nrm,
           a_v, w_v, r_v, g_v, part, recv, own, st_tx, st_rx,
           a_sem, w0_sem, w_sem, r_sem, g_sem, far_tx, far_rx, near_tx, near_rx, sib_tx, sib_rx, stat_tx, stat_rx):
    t = lax.axis_index("tp")
    core, chip = t % 2, t // 2
    rows, _ = a_v.shape
    d_loc = own.shape[1]
    per = d_loc // CW
    n_blk = len(BLOCKS)
    blocks = [(sum(BLOCKS[:b]), BLOCKS[b]) for b in range(n_blk)]
    half, lanes = rows // 2, 128
    far, near, sib = 2 - 2 * chip, 3 - 2 * chip, t + 1 - 2 * core

    def cross_col(i):
        return (far + i // per) * d_loc + (i % per) * CW

    def home_col(i):
        return (sib + (t - sib) * (i // per)) * d_loc + (i % per) * CW

    def w_copy(i, col):
        return pltpu.make_async_copy(w_hbm.at[:, pl.ds(pl.multiple_of(col, CW), CW)], w_v.at[i], w_sem.at[i])

    def w_start(i):
        if isinstance(i, int):
            w_copy(i, cross_col(i) if i < 2 * per else home_col(i - 2 * per)).start()
            return

        @pl.when(i < 2 * per)
        def _():
            w_copy(i, cross_col(i)).start()

        @pl.when((i >= 2 * per) & (i < 4 * per))
        def _():
            w_copy(i, home_col(i - 2 * per)).start()

    def a_copy(q):
        sl = pl.ds(q * half, half)
        return pltpu.make_async_copy(a_hbm.at[sl, :], a_v.at[sl, :], a_sem.at[q])

    def w0_copy(q):
        src = w_hbm.at[:, pl.ds(pl.multiple_of(far * d_loc + q * lanes, lanes), lanes)]
        return pltpu.make_async_copy(src, w_v.at[0, :, pl.ds(q * lanes, lanes)], w0_sem.at[q])

    def remote(src, dst, tx, rx, peer):
        return pltpu.make_async_remote_copy(src_ref=src, dst_ref=dst, send_sem=tx, recv_sem=rx,
                                            device_id={"tp": peer}, device_id_type=MESH)

    every = pl.ds(0, rows)
    pieces = ((pl.ds(0, half), pl.ds(0, lanes)), (pl.ds(0, half), pl.ds(lanes, lanes)), (pl.ds(half, half), pl.ds(0, CW)))
    far_parts = [(every, pl.ds(0, N_COL * CW))]
    far_parts += [(every, pl.ds(N_COL * CW, d_loc - N_COL * CW))]

    def far_copy(q, slot):
        sl = far_parts[q]
        return remote(part.at[(FAR, *sl)], recv.at[(slot, *sl)], far_tx.at[q], far_rx.at[slot, q], far)

    near_blocks = [(sum(NEAR_ROWS[:b]), NEAR_ROWS[b]) for b in range(len(NEAR_ROWS))]

    def near_copy(b, slot):
        sl = pl.ds(*near_blocks[b])
        return remote(part.at[NEAR, sl, :], recv.at[slot, sl, :], near_tx.at[b], near_rx.at[slot, b], near)

    def sib_copy():
        return remote(part.at[SIB], recv.at[SIB], sib_tx, sib_rx, sib)

    def stat_copy(k, b, slot):
        return remote(st_tx.at[b], st_rx.at[slot, b], stat_tx.at[k, b], stat_rx.at[slot, b], (far, near, sib)[k])

    barrier = pltpu.get_barrier_semaphore()
    for p in (far, near, sib):
        pl.semaphore_signal(barrier, inc=1, device_id={"tp": p}, device_id_type=MESH)
    a_copy(0).start()
    w0_copy(0).start()
    w0_copy(1).start()
    a_copy(1).start()
    r_copy = pltpu.make_async_copy(r_hbm, r_v, r_sem)
    g_copy = pltpu.make_async_copy(g_hbm, g_v, g_sem)

    def dot(lhs, rhs):
        return jnp.dot(lhs, rhs, preferred_element_type=F32)

    for q in range(3):
        if q == 0:
            a_copy(0).wait()
            w0_copy(0).wait()
            for i in range(1, DEPTH):
                w_start(i)
        elif q == 1:
            w0_copy(1).wait()
        else:
            a_copy(1).wait()
            w_start(DEPTH)
        r_sl, c_sl = pieces[q]
        part[FAR, r_sl, c_sl] = dot(a_v[r_sl, :], w_v[0, :, c_sl]).astype(BF16)


    def chunk(i, col):
        w_copy(i, col).wait()
        w_start(i + DEPTH)
        return dot(a_v[...], w_v[i])

    def columns(j):
        return pl.ds(pl.multiple_of(j * CW, CW), CW)

    for j in range(1, N_COL):
        part[FAR, :, columns(j)] = chunk(j, cross_col(j)).astype(BF16)

    pl.semaphore_wait(barrier, 3)
    far_copy(0, core).start()

    @pl.loop(N_COL, per)
    def _(j):
        part[FAR, :, columns(j)] = chunk(j, cross_col(j)).astype(BF16)

    far_copy(len(far_parts) - 1, core).start()

    @pl.loop(0, per)
    def _(j):
        part[NEAR, :, columns(j)] = chunk(per + j, cross_col(per + j)).astype(BF16)

    for b in range(len(NEAR_ROWS)):
        near_copy(b, core).start()
    r_copy.start()
    g_copy.start()

    @pl.loop(0, per)
    def _(j):
        part[SIB, :, columns(j)] = chunk(2 * per + j, home_col(j)).astype(BF16)

    sib_copy().start()

    @pl.loop(0, per)
    def _(j):
        own[:, columns(j)] = chunk(3 * per + j, home_col(per + j))

    r_copy.wait()
    g_copy.wait()
    sib_copy().wait_recv()

    @pl.loop(0, rows // SUB)
    def _(i):
        sl = pl.ds(pl.multiple_of(i * SUB, SUB), SUB)
        own[sl, :] = (own[sl, :] + recv[SIB, sl, :].astype(F32)) + r_v[sl, :].astype(F32)

    @pl.when(core == 0)
    def _():
        for q in range(len(far_parts)):
            for slot in range(2):
                far_copy(q, slot).wait_recv()

    lane = lax.broadcasted_iota(jnp.int32, (8, 128), 1)
    sub = lax.broadcasted_iota(jnp.int32, (8, 128), 0)

    def reduce_block(b):
        row, n = blocks[b]
        if row in [first for first, _ in near_blocks]:
            @pl.when(core == 1)
            def _():
                for slot in range(2):
                    near_copy([first for first, _ in near_blocks].index(row), slot).wait_recv()

        line = jnp.zeros((8, 128), F32)
        for first in range(0, n, SUB):
            sl = pl.ds(row + first, SUB)
            h = own[sl, :] + (recv[0, sl, :].astype(F32) + recv[1, sl, :].astype(F32))
            own[sl, :] = h
            hid[sl, :] = h.astype(BF16)
            s = jnp.sum(h * h, axis=1, keepdims=True)
            for q in range(0, SUB, 8):
                line = line + jnp.where(lane == sub + (first + q), s[q:q + 8, :], 0.0)
        st_tx[b] = jnp.sum(line, axis=0, keepdims=True)
        for k in range(3):
            stat_copy(k, b, SIB if k == SIB else core).start()

    def norm_block(b):
        for slot in range(3):
            stat_copy(slot, b, slot).wait_recv()
        row, n = blocks[b]
        tot = (st_tx[b] + st_rx[SIB, b]) + (st_rx[0, b] + st_rx[1, b])
        scale = jnp.broadcast_to(lax.rsqrt(tot / d_model + EPS), (8, 128))
        for first in range(0, n, SUB):
            out = []
            for q in range(first, first + SUB, 8):
                col = jnp.sum(jnp.where(lane == sub + q, scale, 0.0), axis=1, keepdims=True)
                out.append(own[pl.ds(row + q, 8), :] * col * g_v[...])
            nrm[pl.ds(row + first, SUB), :] = jnp.concatenate(out, axis=0).astype(BF16)

    for b in range(n_blk):
        reduce_block(b)

    for b in range(n_blk):
        norm_block(b)

    for q in range(len(far_parts)):
        far_copy(q, core).wait_send()
    for b in range(len(NEAR_ROWS)):
        near_copy(b, core).wait_send()
    for b in range(n_blk):
        for k in range(3):
            stat_copy(k, b, SIB if k == SIB else core).wait_send()
    sib_copy().wait_send()


def put(hid, nrm, hid_hbm, nrm_hbm, sem):
    n = hid.shape[0] // PUT
    copies = []
    for q in range(PUT):
        sl = pl.ds(q * n, n)
        copies.append(pltpu.make_async_copy(hid.at[sl, :], hid_hbm.at[sl, :], sem.at[0, q]))
        copies.append(pltpu.make_async_copy(nrm.at[sl, :], nrm_hbm.at[sl, :], sem.at[1, q]))
    for c in copies:
        c.start()
    for c in copies:
        c.wait()


def solution(mesh):
    tp = mesh.shape["tp"]

    def local_step(a, w, r, g):
        rows, depth = a.shape
        d_loc = r.shape[1]
        per = d_loc // CW
        n_blk = len(BLOCKS)
        hbm = pl.BlockSpec(memory_space=pltpu.HBM)
        vmem = pl.BlockSpec(memory_space=pltpu.VMEM)
        dma = pltpu.SemaphoreType.DMA
        hid, nrm = pl.pallas_call(
            functools.partial(kernel, d_loc * tp),
            out_shape=(pltpu.VMEM((rows, d_loc), BF16),) * 2,
            in_specs=[hbm] * 4,
            out_specs=(vmem,) * 2,
            scratch_shapes=[
                pltpu.VMEM((rows, depth), BF16),
                pltpu.VMEM((4 * per, depth, CW), BF16),
                pltpu.VMEM((rows, d_loc), BF16),
                pltpu.VMEM((1, d_loc), F32),
                pltpu.VMEM((3, rows, d_loc), BF16),
                pltpu.VMEM((3, rows, d_loc), BF16),
                pltpu.VMEM((rows, d_loc), F32),
                pltpu.VMEM((n_blk, 1, 128), F32),
                pltpu.VMEM((3, n_blk, 1, 128), F32),
                dma((2,)), dma((2,)), dma((4 * per,)), dma, dma,
                dma((2,)), dma((2, 2)), dma((len(NEAR_ROWS),)), dma((2, len(NEAR_ROWS))), dma, dma,
                dma((3, n_blk)), dma((3, n_blk)),
            ],
            compiler_params=pltpu.CompilerParams(
                collective_id=0, has_side_effects=True, vmem_limit_bytes=64946176),
            cost_estimate=pl.CostEstimate(flops=2 * rows * depth * d_loc * tp, transcendentals=0,
                                          bytes_accessed=2 * depth * d_loc * tp),
        )(a, w, r, g.reshape(1, d_loc))
        return pl.pallas_call(
            put,
            out_shape=(jax.ShapeDtypeStruct((rows, d_loc), BF16),) * 2,
            in_specs=[vmem] * 2,
            out_specs=(hbm,) * 2,
            scratch_shapes=[dma((2, PUT))],
            compiler_params=pltpu.CompilerParams(vmem_limit_bytes=1024 * 1024),
        )(hid, nrm)

    return jax.shard_map(
        local_step,
        mesh=mesh,
        in_specs=(P("data", "tp"), P("tp", None), P("data", "tp"), P("tp")),
        out_specs=(P("data", "tp"), P("data", "tp")),
        check_vma=False,
    )
```
